32 devices in a mesh: gx: 4 (over z), gy: 4 (over y, x), gz: 2 (over core).
Axes of the slice: x: 2, y: 2, z: 4, core: 2. Of those that a mesh axis runs over, the one named last changes fastest.
Arguments:
- potential: float32 [16, 96, 512], P('gz', 'gx', 'gy'), may hold values from -6 to 6
- tissue_mask: int32 [16, 96, 512], P('gz', 'gx', 'gy'), may hold values from 0 to 2, as said below
- layer_index: int32 [16], P('gz'), may hold values from 0 to 15
- source: float32 [16, 96, 512], P('gz', 'gx', 'gy'), may hold values from -6 to 6
Outputs:
- phi_e: float32 [16, 96, 512], P('gz', 'gx', 'gy')
- residual: float32 [16, 96, 512], P('gz', 'gx', 'gy')
The draws below stay inside these ranges and needn't reach their ends.
Inputs may be any that keep to these rules, and one draw needn't show every extreme that they name: `tissue_mask`: 0 marks cells outside every medium, 1 bath, 2 tissue.
All inputs are finite; a program needn't handle non-finite values.
Results may differ from the reference program's by a relative error of at most 0.0003.
Values sent between devices are 32-bit elements; how exact they have to be, the bound alone decides.
A program may use at most 128 MiB of HBM per device.

```python
import math
import jax
import jax.numpy as jnp

ITERS = 8
LAYERS = 16
NZ = 16
NX = 96
NY = 512


def cell_axes():
    plane_z = jnp.arange(NZ, dtype=jnp.float32)[:, None, None] + 0.5
    row_x = jnp.arange(NX, dtype=jnp.float32)[None, :, None] + 0.5
    column_y = jnp.arange(NY, dtype=jnp.float32)[None, None, :] + 0.5
    return (plane_z, row_x, column_y)


def draw_tissue_mask(key, part):
    centre_key = jax.random.fold_in(key, 101)
    radius_key = jax.random.fold_in(key, 103)
    jitter_key = jax.random.fold_in(key, 107)
    shift = jax.random.randint(centre_key, (3,), -8, 9)
    centre_z = NZ // 2 + shift[0] * NZ // 64
    centre_x = NX // 2 + shift[1] * NX // 64
    centre_y = NY // 2 + shift[2] * NY // 64
    plane_z = jnp.arange(NZ, dtype=jnp.int32)[:, None, None]
    row_x = jnp.arange(NX, dtype=jnp.int32)[None, :, None]
    column_y = jnp.arange(NY, dtype=jnp.int32)[None, None, :]
    scaled_z = 128 * (plane_z - centre_z) // NZ
    scaled_x = 128 * (row_x - centre_x) // NX
    scaled_y = 128 * (column_y - centre_y) // NY
    reach = scaled_z * scaled_z + scaled_x * scaled_x + scaled_y * scaled_y
    reach = reach + jax.random.randint(jitter_key, (NZ, NX, NY), -150, 151)
    inner_key, outer_key, bath_key = jax.random.split(radius_key, 3)
    inner_edge = jax.random.randint(inner_key, (), 600, 1001)
    outer_edge = jax.random.randint(outer_key, (), 1900, 2501)
    bath_edge = jax.random.randint(bath_key, (), 3200, 4201)
    labels = jnp.where(reach < inner_edge, 1, jnp.where(reach < outer_edge, 2, jnp.where(reach < bath_edge, 1, 0)))
    return labels.astype(jnp.int32)


def draw_potential(key, part):
    normal_key = jax.random.fold_in(key, 201)
    anchor_key = jax.random.fold_in(key, 203)
    shape_key = jax.random.fold_in(key, 207)
    noise_key = jax.random.fold_in(key, 211)
    plane_z, row_x, column_y = cell_axes()
    sizes = jnp.array([NZ, NX, NY], jnp.float32)
    anchor = jax.random.uniform(anchor_key, (3,), jnp.float32, 0.3, 0.7) * sizes
    amp_key, width_key = jax.random.split(shape_key, 2)
    width = jax.random.uniform(width_key, (), jnp.float32, 2.0, 5.0)
    direction = jax.random.normal(normal_key, (3,), jnp.float32)
    direction = direction / jnp.sqrt(jnp.sum(direction * direction) + 1e-06)
    signed = direction[0] * (plane_z - anchor[0]) + direction[1] * (row_x - anchor[1]) + direction[2] * (column_y - anchor[2])
    amplitude = jax.random.uniform(amp_key, (), jnp.float32, 2.0, 4.0)
    noise = jnp.clip(0.5 * jax.random.normal(noise_key, (NZ, NX, NY), jnp.float32), -2.0, 2.0)
    return (amplitude * jnp.tanh(signed / width) + noise).astype(jnp.float32)


def draw_source(key, part):
    sign_key = jax.random.fold_in(key, 301)
    level_key = jax.random.fold_in(key, 303)
    mode_key = jax.random.fold_in(key, 307)
    weight_key = jax.random.fold_in(key, 311)
    noise_key = jax.random.fold_in(key, 313)
    plane_z, row_x, column_y = cell_axes()
    sign = jnp.where(jax.random.bernoulli(sign_key), 1.0, -1.0).astype(jnp.float32)
    orders = jax.random.randint(mode_key, (3, 3), 0, 3).astype(jnp.float32)
    level = jax.random.uniform(level_key, (), jnp.float32, 0.5, 1.0)
    weights = jax.random.uniform(weight_key, (3,), jnp.float32, -0.5, 0.5)
    noise = jnp.clip(jax.random.normal(noise_key, (NZ, NX, NY), jnp.float32), -3.0, 3.0)
    smooth = jnp.zeros((NZ, NX, NY), jnp.float32)
    for mode in range(3):
        wave = jnp.cos(math.pi * orders[mode, 0] * plane_z / NZ) * jnp.cos(math.pi * orders[mode, 1] * row_x / NX)
        wave = wave * jnp.cos(math.pi * orders[mode, 2] * column_y / NY)
        smooth = smooth + weights[mode] * wave
    return (sign * level + smooth + noise).astype(jnp.float32)


def with_ends(result, key, smallest, largest):
    place = [jax.random.randint(jax.random.fold_in(key, axis), (), 0, length) for axis, length in enumerate(result.shape)]
    main_axis = result.shape.index(max(result.shape))
    next_to = place[:main_axis] + [(place[main_axis] + 1) % result.shape[main_axis]] + place[main_axis + 1:]
    return result.at[tuple(place)].set(smallest).at[tuple(next_to)].set(largest)


def setup_inputs(seed: int = 0) -> dict:
    arg_keys = jax.random.split(jax.random.key(seed), 5)
    potential = draw_potential(jax.random.fold_in(arg_keys[4], 71), 0)
    tissue_mask = draw_tissue_mask(jax.random.fold_in(arg_keys[4], 71), 0)
    layer_index = with_ends(jax.random.randint(arg_keys[2], (NZ,), 0, LAYERS), jax.random.fold_in(arg_keys[2], 1), 0, LAYERS - 1).astype(jnp.int32)
    source = draw_source(jax.random.fold_in(arg_keys[4], 71), 0)
    return dict(potential=potential, tissue_mask=tissue_mask, layer_index=layer_index, source=source)


OFFSETS = [(0, 1, 0), (0, 0, 1), (1, 0, 0), (0, 1, 1), (0, 1, -1), (1, 1, 0), (-1, 1, 0), (1, 0, 1), (-1, 0, 1)]
bulk_long = 7.99
bulk_trans = 2.55
intra_long = 1.74
intra_trans = 0.19
bath_sigma = 5.0


def tensor_table(layers, longitudinal, transverse):
    depth = jnp.arange(layers, dtype=jnp.float32) / (layers - 1)
    helix = (math.pi / 3.0) * (1.0 - 2.0 * depth)
    tilted = 0.35 * jnp.cos(math.pi * depth)
    fiber_x = jnp.cos(tilted) * jnp.cos(helix)
    fiber_y = jnp.cos(tilted) * jnp.sin(helix)
    fiber_z = jnp.sin(tilted)
    spread = longitudinal - transverse
    s_xx = transverse + spread * fiber_x * fiber_x
    s_yy = transverse + spread * fiber_y * fiber_y
    s_zz = transverse + spread * fiber_z * fiber_z
    s_xy = spread * fiber_x * fiber_y
    s_xz = spread * fiber_x * fiber_z
    s_yz = spread * fiber_y * fiber_z
    columns = [s_xx - jnp.abs(s_xy) - jnp.abs(s_xz), s_yy - jnp.abs(s_xy) - jnp.abs(s_yz),
               s_zz - jnp.abs(s_xz) - jnp.abs(s_yz), jnp.maximum(s_xy, 0.0), jnp.maximum(-s_xy, 0.0),
               jnp.maximum(s_xz, 0.0), jnp.maximum(-s_xz, 0.0), jnp.maximum(s_yz, 0.0), jnp.maximum(-s_yz, 0.0)]
    return jnp.stack(columns, axis=1).astype(jnp.float32)


def window(array, offset, extent):
    return array[1 + offset[0]:1 + offset[0] + extent[0], 1 + offset[1]:1 + offset[1] + extent[1],
                 1 + offset[2]:1 + offset[2] + extent[2]]


def cell_weight(planes, column, tissue_pad, bath_pad):
    weight = tissue_pad * planes[:, column][:, None, None]
    if bath_pad is not None and column < 3:
        weight = weight + bath_sigma * bath_pad
    return weight


def edge_pair(weight, medium_pad, offset, extent):
    backward = (-offset[0], -offset[1], -offset[2])
    centre = window(medium_pad, (0, 0, 0), extent)
    own_weight = window(weight, (0, 0, 0), extent)
    forward_edge = centre * window(medium_pad, offset, extent) * (0.5 * (own_weight + window(weight, offset, extent)))
    backward_edge = centre * window(medium_pad, backward, extent) * (0.5 * (own_weight + window(weight, backward, extent)))
    return forward_edge, backward_edge


def operate(field, planes, tissue_pad, bath_pad, medium_pad):
    extent = field.shape
    field_pad = jnp.pad(field, 1)
    summed = jnp.zeros(extent, jnp.float32)
    for column, offset in enumerate(OFFSETS):
        backward = (-offset[0], -offset[1], -offset[2])
        weight = cell_weight(planes, column, tissue_pad, bath_pad)
        forward_edge, backward_edge = edge_pair(weight, medium_pad, offset, extent)
        summed = summed + forward_edge * (field - window(field_pad, offset, extent)) + backward_edge * (field - window(field_pad, backward, extent))
    return summed


def reference(potential, tissue_mask, layer_index, source):
    extent = tissue_mask.shape
    mask_pad = jnp.pad(tissue_mask, 1)
    layer_pad = jnp.pad(layer_index, 1)
    tissue_pad = (mask_pad == 2).astype(jnp.float32)
    bath_pad = (mask_pad == 1).astype(jnp.float32)
    inside_pad = (mask_pad > 0).astype(jnp.float32)
    inside = window(inside_pad, (0, 0, 0), extent)
    bulk_planes = tensor_table(LAYERS, bulk_long, bulk_trans)[layer_pad]
    intra_planes = tensor_table(LAYERS, intra_long, intra_trans)[layer_pad]
    diagonal = jnp.zeros(extent, jnp.float32)
    for column, offset in enumerate(OFFSETS):
        weight = cell_weight(bulk_planes, column, tissue_pad, bath_pad)
        forward_edge, backward_edge = edge_pair(weight, inside_pad, offset, extent)
        diagonal = diagonal + forward_edge + backward_edge
    jacobi = inside / jnp.maximum(diagonal, 1.0)
    rhs = -operate(potential, intra_planes, tissue_pad, None, tissue_pad) + inside * source
    count = jnp.sum(inside)
    residual = rhs - inside * (jnp.sum(rhs) / count)

    def precondition(current):
        scaled = jacobi * current
        return scaled - inside * (jnp.sum(scaled) / count)

    solution = jnp.zeros(extent, jnp.float32)
    precond = precondition(residual)
    direction = precond
    rz_now = jnp.sum(residual * precond)
    for step in range(ITERS):
        image = operate(direction, bulk_planes, tissue_pad, bath_pad, inside_pad)
        alpha = rz_now / jnp.sum(direction * image)
        solution = solution + alpha * direction
        residual = residual - alpha * image
        if step + 1 < ITERS:
            precond = precondition(residual)
            rz_next = jnp.sum(residual * precond)
            direction = precond + (rz_next / rz_now) * direction
            rz_now = rz_next
    return solution, residual
```

```python
import functools
import math

import jax
import jax.numpy as jnp
from jax import lax
from jax.experimental import pallas as pl
from jax.experimental.pallas import tpu as pltpu
from jax.sharding import PartitionSpec as P
import numpy as np

ITERS = 8
DEPTH = ITERS + 1
LAYERS = 16
AXES = ("gx", "gy", "gz")

OFFSETS = [
    (0, 1, 0),
    (0, 0, 1),
    (1, 0, 0),
    (0, 1, 1),
    (0, 1, -1),
    (1, 1, 0),
    (-1, 1, 0),
    (1, 0, 1),
    (-1, 0, 1),
]
bulk_long = 7.99
bulk_trans = 2.55
intra_long = 1.74
intra_trans = 0.19
bath_sigma = 5.0


def tensor_table(layers, longitudinal, transverse):
    depth = jnp.arange(layers, dtype=jnp.float32) / (layers - 1)
    helix = math.pi / 3.0 * (1.0 - 2.0 * depth)
    tilted = 0.35 * jnp.cos(math.pi * depth)
    fiber_x = jnp.cos(tilted) * jnp.cos(helix)
    fiber_y = jnp.cos(tilted) * jnp.sin(helix)
    fiber_z = jnp.sin(tilted)
    spread = longitudinal - transverse
    s_xx = transverse + spread * fiber_x * fiber_x
    s_yy = transverse + spread * fiber_y * fiber_y
    s_zz = transverse + spread * fiber_z * fiber_z
    s_xy = spread * fiber_x * fiber_y
    s_xz = spread * fiber_x * fiber_z
    s_yz = spread * fiber_y * fiber_z
    columns = [
        s_xx - jnp.abs(s_xy) - jnp.abs(s_xz),
        s_yy - jnp.abs(s_xy) - jnp.abs(s_yz),
        s_zz - jnp.abs(s_xz) - jnp.abs(s_yz),
        jnp.maximum(s_xy, 0.0),
        jnp.maximum(-s_xy, 0.0),
        jnp.maximum(s_xz, 0.0),
        jnp.maximum(-s_xz, 0.0),
        jnp.maximum(s_yz, 0.0),
        jnp.maximum(-s_yz, 0.0),
    ]
    return jnp.stack(columns, axis=1)


def shifted(value, axis, hop):
    count = lax.axis_size(axis)
    pairs = [(i + hop, i) for i in range(count) if 0 <= i + hop < count]
    return lax.ppermute(value, axis, pairs)


def framed(value, axis, dim, multiple):
    count, length = lax.axis_size(axis), value.shape[dim]
    if count == 1:
        return value
    if count == 2 and 2 * length <= length + 2 * DEPTH and multiple == 1:
        other = lax.ppermute(value, axis, [(0, 1), (1, 0)])
        return jnp.concatenate([value, other], axis=dim)
    after, before = [], []
    left, hop = DEPTH, 1
    while left > 0:
        width = min(left, length)
        if hop < count:
            after.append(
                shifted(lax.slice_in_dim(value, 0, width, axis=dim), axis, hop)
            )
            before.insert(
                0, shifted(lax.slice_in_dim(value, length - width, length, axis=dim), axis, -hop)
            )
        else:
            shape = list(value.shape)
            shape[dim] = width
            after.append(jnp.zeros(shape, value.dtype))
            before.insert(0, jnp.zeros(shape, value.dtype))
        left, hop = left - width, hop + 1
    gap = -(length + 2 * DEPTH) % multiple
    shape = list(value.shape)
    shape[dim] = gap
    middle = [jnp.zeros(shape, value.dtype)] if gap else []
    return jnp.concatenate([value] + after + middle + before, axis=dim)


def fields_around(ref, here, above, below, rows, lanes):
    def along_x(value, step):
        return pltpu.roll(value, (-step) % rows, 0)

    def along_y(value, step):
        return pltpu.roll(value, (-step) % lanes, 1)

    for dz, plane in ((0, here), (1, above), (-1, below)):
        value = ref[plane]
        if dz:
            yield (dz, 0, 0), value
        for step in (1, -1):
            yield (dz, step, 0), along_x(value, step)
        for step in (1, -1):
            moved = along_y(value, step)
            yield (dz, 0, step), moved
            if dz == 0:
                for other in (1, -1):
                    yield (0, other, step), along_x(moved, other)


SLOT = {}
for _column, _offset in enumerate(OFFSETS):
    SLOT[_offset] = (_column, 2 * _column)
    SLOT[tuple(-o for o in _offset)] = (_column, 2 * _column + 1)


def grid_kernel(extent, sizes, table, mask_in, potential_in, source_in, phi, residual,
                basis, scale, dots, weights, spare, first, second, jac,
                own_row, early, final_row, late, sends, early_recv, late_recv):
    mask, potential, source = mask_in, potential_in, source_in
    planes, rows, lanes = mask.shape
    nz, nx, ny = extent
    held = jac.shape[1]
    keep = nx + ITERS
    peers = math.prod(sizes)
    me = 0
    for axis, size in zip(AXES, sizes):
        me = me * size + lax.axis_index(axis)

    def device(index):
        return (index // (sizes[1] * sizes[2]), index // sizes[2] % sizes[1], index % sizes[2])

    def peer(k):
        return lax.rem(me + k, peers)

    barrier = pltpu.get_barrier_semaphore()

    def greet(k, carry):
        pl.semaphore_signal(
            barrier, inc=1, device_id=device(peer(k)), device_id_type=pl.DeviceIdType.MESH
        )
        return carry

    lax.fori_loop(1, peers, greet, 0)

    def spread(row, gathered, recv):
        def one(k, carry):
            pltpu.make_async_remote_copy(
                src_ref=row, dst_ref=gathered.at[me], send_sem=sends.at[k],
                recv_sem=recv.at[me], device_id=device(peer(k)),
                device_id_type=pl.DeviceIdType.MESH,
            ).start()
            return carry

        lax.fori_loop(1, peers, one, 0)

    def collect(row, gathered, recv):
        def one(k, carry):
            other = peer(k)
            copy = pltpu.make_async_remote_copy(
                src_ref=row, dst_ref=gathered.at[other], send_sem=sends.at[k],
                recv_sem=recv.at[other], device_id=device(other),
                device_id_type=pl.DeviceIdType.MESH,
            )
            copy.wait_recv()
            copy.wait_send()
            return carry

        lax.fori_loop(1, peers, one, 0)
        gathered[me] = row[...]
        return jnp.sum(gathered[...], axis=0)

    lane = lax.broadcasted_iota(jnp.int32, (1, 128), 1)

    def pick(vector, index):
        return jnp.sum(jnp.where(lane == index, vector, 0.0), axis=1, keepdims=True)

    cells = jnp.zeros((1, ny), jnp.float32)
    injected = jnp.zeros((1, ny), jnp.float32)
    for plane in range(nz):
        own_inside = jnp.where(mask_in[plane, 0:nx, 0:ny] > 0.0, 1.0, 0.0)
        cells = cells + jnp.sum(own_inside, axis=0, keepdims=True)
        injected = injected + jnp.sum(
            own_inside * source_in[plane, 0:nx, 0:ny], axis=0, keepdims=True
        )
    cells = jnp.sum(cells, axis=1, keepdims=True)
    injected = jnp.sum(injected, axis=1, keepdims=True)
    own_row[...] = jnp.where(lane == 0, cells, jnp.where(lane == 1, injected, 0.0))

    def neighbours(plane):
        above = jnp.where(plane + 1 == planes, 0, plane + 1)
        below = jnp.where(plane == 0, planes - 1, plane - 1)
        return above, below

    def store(ref, index, value):
        if held == rows:
            ref[index] = value
        else:
            ref[(*index, slice(0, keep))] = value[:keep]
            ref[(*index, slice(keep, held))] = value[rows - held + keep :]

    def setup(plane, carry):
        above, below = neighbours(plane)
        labels = mask[plane]
        tissue = jnp.where(labels == 2.0, 1.0, 0.0)
        bath = jnp.where(labels == 1.0, 1.0, 0.0)
        inside = tissue + bath
        volts = potential[plane]
        total = jnp.zeros((rows, lanes), jnp.float32)
        image = jnp.zeros((rows, lanes), jnp.float32)
        pairs = zip(
            fields_around(mask, plane, above, below, rows, lanes),
            fields_around(potential, plane, above, below, rows, lanes),
        )
        for (offset, label), (_, volt) in pairs:
            column, slot = SLOT[offset]
            beyond = {0: plane, 1: above, -1: below}[offset[0]]
            link = 0.5
            if offset[0] == 1:
                link = 0.5 * table[plane, 18]
            if offset[0] == -1:
                link = 0.5 * table[below, 18]
            their_tissue = jnp.where(label == 2.0, 1.0, 0.0)
            g_here, g_there = table[plane, column] * link, table[beyond, column] * link
            weight = tissue * g_here
            if column < 3:
                their_bath = jnp.where(label == 1.0, 1.0, 0.0)
                sigma = bath_sigma * link
                weight = inside * (
                    jnp.where(label > 0.0, weight + bath * sigma, 0.0)
                    + (their_tissue * g_there + their_bath * sigma)
                )
            else:
                weight = inside * (jnp.where(label > 0.0, weight, 0.0) + their_tissue * g_there)
            store(weights, (slot, plane), weight)
            total = total + weight
            intra = (table[plane, 9 + column] + table[beyond, 9 + column]) * link
            image = image + (tissue * their_tissue * intra) * (volts - volt)
        bounded = jnp.maximum(total, 1.0)
        jacobi = inside / bounded
        store(jac, (plane,), jacobi + jacobi)
        store(spare, (plane,), inside * (1.0 - jacobi * total))
        store(first, (plane,), jacobi * (inside * source[plane] - image))

        @pl.when(plane < nz)
        def _():
            scale[plane] = (inside * bounded)[:nx, :ny]

        return carry

    lax.fori_loop(0, planes // 2, setup, 0)
    pl.semaphore_wait(barrier, peers - 1)
    spread(own_row, early, early_recv)
    lax.fori_loop(planes // 2, planes, setup, 0)
    totals = collect(own_row, early, early_recv)
    count = pick(totals, 0)
    mean_rhs = pick(totals, 1) / count

    def centre(plane, carry):
        first[plane] = first[plane] - 0.5 * jac[plane] * mean_rhs
        return carry

    lax.fori_loop(0, planes, centre, 0)

    def record(step, now, before):
        rowsum = jnp.zeros((1, ny), jnp.float32)
        square, cross, plain = rowsum, rowsum, rowsum
        for plane in range(nz):
            value = now[plane, 0:nx, 0:ny]
            basis[step, plane] = value
            weighted = value * scale[plane]
            square = square + jnp.sum(weighted * value, axis=0, keepdims=True)
            if step:
                past = basis[step - 1, plane]
                cross = cross + jnp.sum(weighted * past, axis=0, keepdims=True)
            plain = plain + jnp.sum(value, axis=0, keepdims=True)
        if step < ITERS:
            dots[pl.ds(2 * step, 1)] = square
            dots[pl.ds(2 * ITERS + step, 1)] = plain
        if step:
            dots[pl.ds(2 * step - 1, 1)] = cross

    record(0, first, None)

    def apply(now, old, step):
        reach = ITERS - step
        if planes == nz:
            begin, span = 0, nz
        elif planes == sizes[2] * nz:
            begin = planes - lax.axis_index("gz") * reach
            span = min(planes, nz + reach)
        else:
            begin, span = planes - reach, nz + 2 * reach

        def one(index, carry):
            plane = lax.rem(begin + index, planes)
            above, below = neighbours(plane)
            total = jnp.zeros((held, lanes), jnp.float32)
            for offset, value in fields_around(now, plane, above, below, held, lanes):
                total = total + weights[SLOT[offset][1], plane] * value
            if step == 1:
                old[plane] = 0.5 * jac[plane] * total + spare[plane] * now[plane]
            else:
                old[plane] = (
                    jac[plane] * total + 2.0 * spare[plane] * now[plane] - old[plane]
                )
            return carry

        lax.fori_loop(0, span, one, 0)

    now, old = first, second
    for step in range(1, ITERS + 1):
        apply(now, old, step)
        now, old = old, now
        record(step, now, old)

    partial = jnp.sum(dots[...], axis=1, keepdims=True)
    diagonal = lax.broadcasted_iota(jnp.int32, (3 * ITERS, 128), 0) == lax.broadcasted_iota(
        jnp.int32, (3 * ITERS, 128), 1
    )
    final_row[...] = jnp.sum(jnp.where(diagonal, partial, 0.0), axis=0, keepdims=True)
    spread(final_row, late, late_recv)
    sums = collect(final_row, late, late_recv)

    def left(vector):
        return pltpu.roll(vector, 127, 1)

    def right(vector):
        return pltpu.roll(vector, 1, 1)

    mu0, mu1 = pick(sums, 0), pick(sums, 1)
    mu = jnp.where(lane < 2, sums, 2.0 * sums - jnp.where(lane % 2 == 0, mu0, mu1))
    mu = jnp.where(lane < 2 * ITERS, mu, 0.0)
    ones = pltpu.roll(sums, 128 - 2 * ITERS, 1)
    y = jnp.where(lane == 0, 1.0, 0.0)
    p = y
    m_y, m_p = mu, mu
    x = jnp.zeros((1, 128), jnp.float32)
    rz = mu0
    for step in range(ITERS):
        h_p = p - 0.5 * (left(p) + jnp.where(lane == 1, 2.0, 1.0) * right(p))
        h_p = jnp.where(lane <= ITERS, h_p, 0.0)
        before = jnp.where(lane == 0, left(m_p), right(m_p))
        m_h = m_p - 0.5 * (left(m_p) + before)
        alpha = rz / jnp.sum(jnp.where(lane < ITERS, p * m_h, 0.0), axis=1, keepdims=True)
        x = x + alpha * p
        y = y - alpha * h_p
        m_y = m_y - alpha * m_h
        if step + 1 < ITERS:
            rz_next = jnp.sum(jnp.where(lane < ITERS, y * m_y, 0.0), axis=1, keepdims=True)
            beta = rz_next / rz
            p = y + beta * p
            m_p = m_y + beta * m_p
            rz = rz_next
    mean = jnp.sum(jnp.where(lane < ITERS, x * ones, 0.0), axis=1, keepdims=True) / count
    xs = [pick(x, j) for j in range(ITERS)]
    ys = [pick(y, j) for j in range(ITERS + 1)]

    def one(plane, carry):
        weight = scale[plane]
        total = jnp.where(weight > 0.0, -mean, 0.0)
        rest = ys[ITERS] * basis[ITERS, plane]
        for j in range(ITERS):
            value = basis[j, plane]
            total = total + xs[j] * value
            rest = rest + ys[j] * value
        phi[plane] = total
        residual[plane] = weight * rest
        return carry

    lax.fori_loop(0, nz, one, 0)


def general_body(potential, tissue_mask, layer_index, source):
    extent = tissue_mask.shape
    nz = extent[0]
    labels = tissue_mask.astype(jnp.float32)
    sizes = tuple(lax.axis_size(axis) for axis in AXES)
    packed = jnp.stack([labels, potential, source], axis=1)
    packed = framed(packed, "gz", 0, 1)
    packed = framed(packed, "gx", 2, 8)
    packed = framed(packed, "gy", 3, 128)
    operands = (packed[:, 0], packed[:, 1], packed[:, 2])
    frame = operands[0].shape
    layers = framed(layer_index, "gz", 0, 1)
    planes = layers.shape[0]
    selector = (layers[:, None] == jnp.arange(LAYERS, dtype=jnp.int32)[None, :]).astype(
        jnp.float32
    )
    tables = jnp.concatenate(
        [
            tensor_table(LAYERS, bulk_long, bulk_trans),
            tensor_table(LAYERS, intra_long, intra_trans),
        ],
        axis=1,
    )
    table = jnp.dot(selector, tables, precision=lax.Precision.HIGHEST)
    size = lax.axis_size("gz")
    link = jnp.ones((planes, 1), jnp.float32)
    if planes == size * nz:
        place = (lax.axis_index("gz") * nz + jnp.arange(planes)) % planes
        link = (place + 1 < planes).astype(jnp.float32)[:, None]
    table = jnp.concatenate([table, link], axis=1)
    smem = pl.BlockSpec(memory_space=pltpu.SMEM)
    vmem = pl.BlockSpec(memory_space=pltpu.VMEM)
    compact = frame
    if extent[1] % 8 == 0 and ITERS % 8 == 0 and frame[1] > extent[1] + 2 * ITERS:
        compact = (planes, extent[1] + 2 * ITERS, frame[2])
    peers = math.prod(sizes)
    row = pltpu.VMEM((1, 128), jnp.float32)
    gathered = pltpu.VMEM((peers, 1, 128), jnp.float32)
    return tuple(
        pl.pallas_call(
            functools.partial(grid_kernel, extent, sizes),
            out_shape=(jax.ShapeDtypeStruct(extent, jnp.float32),) * 2,
            in_specs=[smem, vmem, vmem, vmem],
            out_specs=(vmem, vmem),
            scratch_shapes=[
                pltpu.VMEM((ITERS + 1,) + extent, jnp.float32),
                pltpu.VMEM(extent, jnp.float32),
                pltpu.VMEM((3 * ITERS, extent[2]), jnp.float32),
                pltpu.VMEM((18,) + compact, jnp.float32),
            ]
            + [pltpu.VMEM(compact, jnp.float32)] * 4
            + [row, gathered, row, gathered]
            + [pltpu.SemaphoreType.DMA((peers,))] * 3,
            compiler_params=pltpu.CompilerParams(
                vmem_limit_bytes=60 * 1024 * 1024, collective_id=0, has_side_effects=True
            ),
        )(table, *operands)
    )


GROUP = 16
TERMS_SAME = [(0, 1), (0, -1), (1, 0), (-1, 0), (1, 1), (1, -1), (-1, 1), (-1, -1)]
TERMS_SIDE = [(0, 0), (0, 1), (0, -1), (1, 0), (-1, 0)]
LEVEL = [0, 1, 3, 4]
STEEP = [(0, 0), (1, 0), (-1, 0), (0, 1), (0, -1)]
COEFS = 2 * len(LEVEL) + 2 * (1 + 3 * len(STEEP))


def numpy_table(longitudinal, transverse):
    depth = np.arange(LAYERS, dtype=np.float64) / (LAYERS - 1)
    helix = math.pi / 3.0 * (1.0 - 2.0 * depth)
    tilted = 0.35 * np.cos(math.pi * depth)
    fiber = (np.cos(tilted) * np.cos(helix), np.cos(tilted) * np.sin(helix), np.sin(tilted))
    spread = longitudinal - transverse
    s_xx, s_yy, s_zz = (transverse + spread * f * f for f in fiber)
    s_xy = spread * fiber[0] * fiber[1]
    s_xz = spread * fiber[0] * fiber[2]
    s_yz = spread * fiber[1] * fiber[2]
    columns = [s_xx - abs(s_xy) - abs(s_xz), s_yy - abs(s_xy) - abs(s_yz), s_zz - abs(s_xz) - abs(s_yz)]
    for value in (s_xy, s_xz, s_yz):
        columns += [np.maximum(value, 0.0), np.maximum(-value, 0.0)]
    return np.stack(columns, axis=1)


HALF_TABLE = 0.5 * np.concatenate(
    [numpy_table(bulk_long, bulk_trans), numpy_table(intra_long, intra_trans)], axis=1
)


def lane_roll(value, step):
    return pltpu.roll(value, step % value.shape[1], 1)


def row_roll(value, step):
    return pltpu.roll(value, step % value.shape[0], 0)


def tiled(value, rows):
    return jnp.concatenate([value] * (rows // value.shape[0]), axis=0)


def column_of(dz, dx, dy, side):
    same, flipped = SLOT[(dz, dx, dy)][0], SLOT[(-dz, dx, dy)][0]
    return same if same == flipped else same + side * (flipped - same)


def fast_kernel(extent, sizes, potential_in, mask_in, layers_in, source_in, phi, residual,
                fields, labels, packs, edge_send, edge_recv, from_after, from_before, strips,
                derived, weights, basis, moved, beside, jac, spare, scale, coef_lanes, dots,
                early_row, early_all, line_row, line_all, final_row, final_all,
                table, coefs, layers_own, layers_far, layers,
                loads, halo_send, halo_recv, sum_send, sum_recv):
    nz, nx, ny = extent
    planes, held, deep = 2 * nz, nx + 16, nx + 32
    own = slice(8, 8 + nx)
    place = tuple(lax.axis_index(axis) for axis in AXES)
    gx, gy, side = place
    first_x, last_x = gx == 0, gx == sizes[0] - 1
    first_y, last_y = gy == 0, gy == sizes[1] - 1

    def exists(dx, dy):
        return (gx + dx >= 0) & (gx + dx < sizes[0]) & (gy + dy >= 0) & (gy + dy < sizes[1])

    def around(a, b, c):
        return tuple(
            lax.rem(here + step, size) if step else here
            for here, step, size in zip(place, (a, b, c), sizes)
        )

    slab = [(0, b, c) for b in range(sizes[1]) for c in range(sizes[2])]
    line = [(a, 0, 0) for a in range(sizes[0])]
    everyone = [(a, b, c) for a, _, _ in line for _, b, c in slab]
    corners = [(dx, dy) for dx in (1, -1) for dy in (1, -1)]

    def flip(slot, turned):
        return slot + turned * (nz - 1 - 2 * slot)

    barrier = pltpu.get_barrier_semaphore()

    def greet(target):
        pl.semaphore_signal(
            barrier, inc=1, device_id=target, device_id_type=pl.DeviceIdType.MESH
        )

    expected = len(slab) + len(line) - 2
    for step in slab[1:] + line[1:]:
        greet(around(*step))
    for dx, dy in corners:
        pl.when(exists(dx, dy))(lambda: greet((gx + dx, gy + dy, side)))
        expected = expected + jnp.where(exists(dx, dy), 1, 0)

    get_layers = pltpu.make_async_copy(layers_in, layers_own, loads.at[0])
    get_mask = pltpu.make_async_copy(mask_in, labels, loads.at[1])
    get_layers.start()
    get_mask.start()
    whole = []
    for index, ref in ((1, potential_in), (2, source_in)):
        for plane in range(nz):
            pltpu.make_async_copy(
                ref.at[plane], fields.at[index, flip(plane, side), own], loads.at[1 + index]
            ).start()
        whole.append(pltpu.make_async_copy(ref, fields.at[index, 0:nz, own], loads.at[1 + index]))

    def clear(when, ref, index):
        @pl.when(when)
        def _():
            ref[index] = jnp.zeros(ref.at[index].shape, jnp.float32)

    every = slice(None)
    clear(first_x, fields, (every, slice(0, nz), slice(0, 8)))
    clear(last_x, fields, (every, slice(0, nz), slice(8 + nx, held)))
    clear(first_x, edge_recv, (0, 0))
    clear(last_x, edge_recv, (0, 1))
    for ref, edge in ((from_after, last_y), (from_before, first_y)):
        clear(edge, ref, (every,))
        clear(first_x, ref, (every, slice(0, 16)))
        clear(last_x, ref, (every, slice(16 + nx, deep)))
    for layer in range(LAYERS):
        for column in range(18):
            table[layer, column] = jnp.float32(HALF_TABLE[layer, column])

    def lanes_of(rows):
        lane = lax.broadcasted_iota(jnp.int32, (rows, ny), 1)
        return lane, lane // GROUP, lane % GROUP

    get_layers.wait()
    get_mask.wait()
    for plane in range(nz):
        fields[0, flip(plane, side), own] = labels[plane].astype(jnp.float32)
    for copy in whole:
        copy.wait()

    _, group, inner = lanes_of(nx)

    def packed(values, shift):
        total = values[0]
        total = lane_roll(total, shift)
        for g in range(1, nz):
            total = jnp.where(group == g, lane_roll(values[g], GROUP * g + shift), total)
        return total

    for index in range(3):
        values = [fields[index, slot, own] for slot in range(nz)]
        packs[index] = packed(values, 8)
        if index < 2:
            packs[3 + index] = jnp.where(inner == 15, packed(values, 7), packed(values, 9))
            for slot in range(nz):
                edge_send[0, index, slot : slot + 1] = values[slot][8:9]
                edge_send[1, index, slot : slot + 1] = values[slot][nx - 9 : nx - 8]

    pl.semaphore_wait(barrier, expected)

    def link(number, src, dst, target):
        return pltpu.make_async_remote_copy(
            src_ref=src, dst_ref=dst, send_sem=halo_send.at[number],
            recv_sem=halo_recv.at[number], device_id=target,
            device_id_type=pl.DeviceIdType.MESH,
        )

    moves = []

    def move(dx, dy, src, dst):
        copy = link(len(moves), src, dst, (gx + dx, gy + dy, side))
        pl.when(exists(dx, dy))(copy.start)
        moves.append((exists(-dx, -dy), exists(dx, dy), copy))

    for dx, dy in corners:
        into = from_before if dy == 1 else from_after
        if dx == 1:
            move(dx, dy, packs.at[:, nx - 16 : nx], into.at[:, 0:16])
        else:
            move(dx, dy, packs.at[:, 0:16], into.at[:, 16 + nx : deep])
    move(0, 1, packs, from_before.at[:, 16 : 16 + nx])
    move(0, -1, packs, from_after.at[:, 16 : 16 + nx])
    move(1, 0, edge_send.at[1], edge_recv.at[0, 0])
    move(-1, 0, edge_send.at[0], edge_recv.at[0, 1])
    move(1, 0, fields.at[:, 0:nz, nx : nx + 8], fields.at[:, 0:nz, 0:8])
    move(-1, 0, fields.at[:, 0:nz, 8:16], fields.at[:, 0:nz, 8 + nx : held])
    other = (gx, gy, 1 - side)
    base = len(moves)
    swaps = [
        link(base, layers_own, layers_far, other),
        link(base + 1, fields.at[:, 0:nz, own], fields.at[:, nz:planes, own], other),
    ]
    for copy in swaps:
        copy.start()

    def spread(number, row, gathered, targets):
        for index, step in enumerate(targets):
            if index:
                pltpu.make_async_remote_copy(
                    src_ref=row, dst_ref=gathered.at[index], send_sem=sum_send.at[number],
                    recv_sem=sum_recv.at[number], device_id=around(*step),
                    device_id_type=pl.DeviceIdType.MESH,
                ).start()

    def collect(number, row, gathered, targets):
        arrived = gathered.at[pl.ds(1, len(targets) - 1)]
        pltpu.make_async_copy(arrived, arrived, sum_recv.at[number]).wait()
        pltpu.make_async_copy(arrived, arrived, sum_send.at[number]).wait()
        gathered[0] = row[...]
        return jnp.sum(gathered[...], axis=0)

    lane = lax.broadcasted_iota(jnp.int32, (1, ny), 1)

    def pick(vector, index):
        return jnp.sum(jnp.where(lane == index, vector, 0.0), axis=1, keepdims=True)

    cells = jnp.zeros((8, ny), jnp.float32)
    injected = cells
    for slot in range(nz):
        for row in range(8, 8 + nx, 8):
            inside = jnp.where(fields[0, slot, row : row + 8] > 0.0, 1.0, 0.0)
            cells = cells + inside
            injected = injected + inside * fields[2, slot, row : row + 8]
    cells = jnp.sum(jnp.sum(cells, axis=0, keepdims=True), axis=1, keepdims=True)
    injected = jnp.sum(jnp.sum(injected, axis=0, keepdims=True), axis=1, keepdims=True)
    early_row[...] = jnp.where(lane == 0, cells, jnp.where(lane == 1, injected, 0.0))
    spread(0, early_row, early_all, slab)

    swaps[0].wait()
    for slot in range(nz):
        layers[slot] = layers_own[flip(slot, side)]
        layers[nz + slot] = layers_far[flip(slot, 1 - side)]

    def slot_of(j):
        return jnp.where(j < nz, j, 3 * nz - 1 - j)

    def coefficients(slot, carry):
        j = slot_of(slot)
        layer = layers[slot]
        for n, k in enumerate(LEVEL):
            coefs[slot, 2 * n] = table[layer, k]
            coefs[slot, 2 * n + 1] = 2.0 * table[layer, 9 + k]
        for half, dz in enumerate((1, -1)):
            near = (j + dz >= 0) & (j + dz < planes)
            there = layers[slot_of(jnp.where(near, j + dz, j))]
            open_ = jnp.where(near, 1.0, 0.0).astype(jnp.float32)
            start = 2 * len(LEVEL) + half * (1 + 3 * len(STEEP))
            coefs[slot, start] = 0.5 * bath_sigma * open_
            for n, (dx, dy) in enumerate(STEEP):
                k = column_of(dz, dx, dy, side)
                coefs[slot, start + 1 + 3 * n] = table[layer, k] * open_
                coefs[slot, start + 2 + 3 * n] = table[there, k] * open_
                coefs[slot, start + 3 + 3 * n] = (table[layer, 9 + k] + table[there, 9 + k]) * open_
        return carry

    lax.fori_loop(0, planes, coefficients, 0)
    _, group8, _ = lanes_of(8)

    def widen(n, carry):
        for q in range(2):
            value = jnp.full((8, ny), coefs[q * nz, n], jnp.float32)
            for g in range(1, nz):
                value = jnp.where(group8 == g, coefs[q * nz + g, n], value)
            coef_lanes[q, n] = value
        return carry

    lax.fori_loop(0, COEFS, widen, 0)

    line_row[...] = collect(0, early_row, early_all, slab)
    spread(1, line_row, line_all, line)

    for receives, _, copy in moves:
        pl.when(receives)(copy.wait_recv)
    _, _, inner_deep = lanes_of(deep)
    for index in range(5):
        strips[index, 0] = jnp.where(inner_deep < 8, from_before[index], from_after[index])
    late = [
        (strips.at[:, 0], strips.at[:, 1]),
        (edge_recv.at[0], edge_recv.at[1]),
        (fields.at[:, 0:nz, 0:8], fields.at[:, nz:planes, 0:8]),
        (fields.at[:, 0:nz, 8 + nx : held], fields.at[:, nz:planes, 8 + nx : held]),
    ]
    for number, (src, dst) in enumerate(late):
        swaps.append(link(base + 2 + number, src, dst, other))
        swaps[-1].start()

    lane_deep, group_deep, inner_deep = lanes_of(deep)

    def sides(value, strip, g):
        ring = lane_roll(strip, -(GROUP * g + 8))
        after = lane_roll(jnp.where(lane_of == 0, ring, value), -1)
        before = lane_roll(jnp.where(lane_of == ny - 1, ring, value), 1)
        return after, before

    def inserted(values):
        total = lane_roll(values[0], 8)
        for g in range(1, len(values)):
            total = jnp.where(group_of == g, lane_roll(values[g], GROUP * g + 8), total)
        return total

    def stored(number, slot, label, volts):
        derived[3 * number, slot] = jnp.where(label == 2.0, 1.0, 0.0)
        derived[3 * number + 1, slot] = jnp.where(label > 0.0, 1.0, 0.0)
        derived[3 * number + 2, slot] = volts

    lane_of, group_of = lane_deep, group_deep

    def framed_plane(index, q, g):
        before = jnp.broadcast_to(edge_recv[q, 0, index, g : g + 1], (8, ny))
        after = jnp.broadcast_to(edge_recv[q, 1, index, g : g + 1], (8, ny))
        return jnp.concatenate([before, fields[index, q * nz + g], after], axis=0)

    for q in range(2):
        if q:
            for copy in swaps[1:]:
                copy.wait_recv()
        found = [[], []]
        for g in range(nz):
            parts = []
            for index in range(2):
                value = framed_plane(index, q, g)
                found[index].append(value)
                parts.append((value,) + sides(value, strips[index, q], g))
            for number in range(3):
                stored(number, q * nz + g, parts[0][number], parts[1][number])
        parts = []
        for index in range(2):
            value, edge = strips[index, q], strips[3 + index, q]
            mixed = inserted(found[index])
            after = lane_roll(jnp.where(inner_deep == 8, mixed, value), -1)
            before = lane_roll(jnp.where(inner_deep == 7, mixed, value), 1)
            after = jnp.where(inner_deep == 15, edge, after)
            before = jnp.where(inner_deep == 0, edge, before)
            parts.append((value, after, before))
        for number in range(3):
            stored(number, planes + q, parts[0][number], parts[1][number])

    def across(lower, upper):
        up0 = jnp.where(group_of == nz - 1, upper, lane_roll(lower, -GROUP))
        up1 = lane_roll(upper, GROUP)
        down0 = lane_roll(lower, GROUP)
        down1 = jnp.where(group_of == nz - 1, lower, lane_roll(upper, -GROUP))
        return up0, up1, down0, down1

    for index in range(9):
        found = across(derived[index, planes], derived[index, planes + 1])
        for number, value in enumerate(found):
            derived[index, planes + 2 + number] = value

    totals = collect(1, line_row, line_all, line)
    count = pick(totals, 0)
    mean_rhs = pick(totals, 1) / count

    def setup(slot, above, below, coef, source):
        level = {k: (coef(2 * n), coef(2 * n + 1)) for n, k in enumerate(LEVEL)}
        base_bath = 0.5 * bath_sigma
        neighbour = {0: slot, 1: above, -1: below}

        def steep(dz):
            start = 2 * len(LEVEL) + (0 if dz == 1 else 1 + 3 * len(STEEP))
            entries = {}
            for n, key in enumerate(STEEP):
                entries[key] = tuple(coef(start + 1 + 3 * n + m) for m in range(3))
            return coef(start), entries

        slopes = {1: steep(1), -1: steep(-1)}

        def fetch(dz, dy, rows):
            number = {0: 0, 1: 1, -1: 2}[dy]
            return tuple(derived[3 * number + m, neighbour[dz], rows] for m in range(3))

        def edges(centre, rows, dx, terms, first):
            t, i, v = centre
            size = t.shape[0]

            def by(value, factor):
                if isinstance(factor, float) or factor.ndim == 0:
                    return value * factor
                return value * tiled(factor, size)

            total = jnp.zeros((size, ny), jnp.float32)
            image = total
            keep = {0: slice(0, held), 1: slice(0, held), -1: slice(8, 8 + held)}[dx]
            for number, (dz, dy) in enumerate(terms):
                tn, i_n, vn = fetch(dz, dy, rows)
                axis = (dz != 0) + (dx != 0) + (dy != 0) == 1
                if dz == 0:
                    k = SLOT[(0, dx, dy)][0]
                    g_here, intra = level[k]
                    g_there, bath = g_here, base_bath
                else:
                    bath, entries = slopes[dz]
                    g_here, g_there, intra = entries[(dx, dy)]
                if axis:
                    ours = by(t, g_here - bath) + by(i, bath)
                    theirs = by(tn, g_there - bath) + by(i_n, bath)
                else:
                    ours, theirs = by(t, g_here), by(tn, g_there)
                weight = i_n * ours + i * theirs
                weights[first + number, slot] = weight[keep]
                total = total + weight
                image = image + by(tn * (v - vn), intra)
            return total, image

        middle = slice(8, 8 + held)
        full = fetch(0, 0, slice(0, deep))
        centre = tuple(value[middle] for value in full)
        total, image = edges(centre, middle, 0, TERMS_SAME, 0)
        high = tuple(row_roll(value, 1)[8:deep] for value in full)
        part = edges(high, slice(8, deep), 1, TERMS_SIDE, 8)
        total = total + row_roll(part[0], -1)[0:held]
        image = image + row_roll(part[1], -1)[0:held]
        low = tuple(row_roll(value, -1)[0 : 8 + held] for value in full)
        part = edges(low, slice(0, 8 + held), -1, TERMS_SIDE, 13)
        total = total + row_roll(part[0], 1)[middle]
        image = image + row_roll(part[1], 1)[middle]
        tissue, inside, _ = centre
        bounded = jnp.maximum(total, 1.0)
        jacobi = inside / bounded
        jac[slot] = jacobi + jacobi
        spare[slot] = 2.0 * (inside - inside * (jacobi * total))
        basis[0, slot] = jacobi * (inside * (source - mean_rhs) - tissue * image)
        return (inside * bounded)[own]

    def own_setup(slot, carry):
        above = slot_of(slot + 1)
        below = jnp.maximum(slot - 1, 0)
        scale[slot] = setup(slot, above, below, lambda n: coefs[slot, n], fields[2, slot])
        return carry

    def far_setup(slot, carry):
        j = slot_of(slot)
        above = slot_of(jnp.minimum(j + 1, planes - 1))
        below = slot_of(j - 1)
        setup(slot, above, below, lambda n: coefs[slot, n], fields[2, slot])
        return carry

    def strip_setup(q, carry):
        slot = planes + q
        setup(slot, slot + 2, slot + 4, lambda n: coef_lanes[q, n], strips[2, q, 8 : 8 + held])
        return carry

    lax.fori_loop(0, nz, own_setup, 0)
    lax.fori_loop(nz, planes, far_setup, 0)
    lax.fori_loop(0, 2, strip_setup, 0)

    def folded(value):
        total = value[0:8]
        for row in range(8, value.shape[0], 8):
            total = total + value[row : row + 8]
        return total

    zero8 = jnp.zeros((8, ny), jnp.float32)

    def record(step, sums):
        square, cross, plain = (jnp.sum(value, axis=0, keepdims=True) for value in sums)
        if step < ITERS:
            dots[2 * step : 2 * step + 1] = square
            dots[2 * ITERS + step : 2 * ITERS + step + 1] = plain
        if step:
            dots[2 * step - 1 : 2 * step] = cross

    sums = [zero8, zero8, zero8]
    for slot in range(nz):
        value = basis[0, slot, own]
        sums[0] = sums[0] + folded(value * value * scale[slot])
        sums[2] = sums[2] + folded(value)
    record(0, sums)

    lane_of, group_of, inner_held = lanes_of(held)

    def at(j):
        return j if j < nz else 3 * nz - 1 - j

    def advance(step, slot, up, down, near, rows):
        same = None
        for number, (dz, dy) in enumerate(TERMS_SAME):
            value = near(dz, dy)
            if value is None:
                continue
            term = weights[number, slot, rows] * value[rows]
            same = term if same is None else same + term
        for dx, first in ((1, 8), (-1, 13)):
            part = None
            for number, (dz, dy) in enumerate(TERMS_SIDE):
                value = near(dz, dy)
                if value is None:
                    continue
                term = weights[first + number, slot] * value[...]
                part = term if part is None else part + term
            same = same + row_roll(part, -dx)[rows]
        value = basis[step - 1, slot, rows]
        fresh = jac[slot, rows] * same + spare[slot, rows] * value
        if step == 1:
            fresh = 0.5 * fresh
        else:
            fresh = fresh - basis[step - 2, slot, rows]
        basis[step, slot, rows] = fresh
        return fresh, value

    for step in range(1, ITERS + 1):
        reach = ITERS - step
        last = nz + reach
        now = basis.at[step - 1]
        for j in range(min(last + 1, planes)):
            slot = at(j)
            found = sides(now[slot], now[planes + slot // nz], slot % nz)
            moved[0, slot], moved[1, slot] = found
        if reach:
            triples = []
            for q in range(2):
                values = [now[slot] for slot in range(q * nz, q * nz + nz)]
                if q:
                    values = [v for s, v in zip(range(nz, planes), values) if 3 * nz - 1 - s <= last]
                strip = now[planes + q]
                mixed = strip
                for g in range(nz):
                    slot = q * nz + g
                    j = slot if q == 0 else 3 * nz - 1 - slot
                    if j <= last:
                        mixed = jnp.where(
                            group_of == g, lane_roll(now[slot], GROUP * g + 8), mixed
                        )
                after = lane_roll(jnp.where(inner_held == 8, mixed, strip), -1)
                before = lane_roll(jnp.where(inner_held == 7, mixed, strip), 1)
                moved[0, planes + q], moved[1, planes + q] = after, before
                triples.append((strip, after, before))
            for number in range(3):
                found = across(triples[0][number], triples[1][number])
                for which, value in enumerate(found):
                    beside[which, number] = value
            for q in range(2):
                slot = planes + q

                def near(dz, dy):
                    number = {0: 0, 1: 1, -1: 2}[dy]
                    if dz:
                        return beside.at[q if dz == 1 else 2 + q, number]
                    return now.at[slot] if dy == 0 else moved.at[number - 1, slot]

                advance(step, slot, None, None, near, slice(0, held))
        sums = [zero8, zero8, zero8]
        for j in range(last):
            slot = at(j)

            def near(dz, dy):
                if j + dz < 0:
                    return None
                spot = at(j + dz)
                return now.at[spot] if dy == 0 else moved.at[0 if dy == 1 else 1, spot]

            rows = slice(0, held) if reach else own
            fresh, value = advance(step, slot, None, None, near, rows)
            if j < nz:
                if reach:
                    fresh, value = fresh[own], value[own]
                weighted = fresh * scale[slot]
                sums[0] = sums[0] + folded(weighted * fresh)
                sums[1] = sums[1] + folded(weighted * value)
                sums[2] = sums[2] + folded(fresh)
        record(step, sums)

    partial = jnp.sum(dots[...], axis=1, keepdims=True)
    diagonal = lax.broadcasted_iota(jnp.int32, (3 * ITERS, ny), 0) == lax.broadcasted_iota(
        jnp.int32, (3 * ITERS, ny), 1
    )
    final_row[...] = jnp.sum(jnp.where(diagonal, partial, 0.0), axis=0, keepdims=True)
    spread(2, final_row, final_all, everyone)
    for _, sends, copy in moves:
        pl.when(sends)(copy.wait_send)
    for copy in swaps[1:]:
        copy.wait_send()
    sums = collect(2, final_row, final_all, everyone)

    mu = [pick(sums, n) for n in range(2 * ITERS)]
    ones = [pick(sums, 2 * ITERS + n) for n in range(ITERS)]
    for n in range(2, 2 * ITERS):
        mu[n] = 2.0 * mu[n] - mu[n % 2]
    one = jnp.ones((1, 1), jnp.float32)
    y, p = [one], [one]
    m_y, m_p = list(mu), list(mu)
    x = []
    rz = mu[0]

    def plus(first, second):
        if first is None or second is None:
            return second if first is None else first
        return first + second

    def get(values, n):
        return values[n] if 0 <= n < len(values) else None

    for step in range(ITERS):
        h_p = []
        for n in range(step + 2):
            right = get(p, n - 1)
            if n == 1:
                right = right + right
            around_n = plus(get(p, n + 1), right)
            here = get(p, n)
            drop = None if around_n is None else -0.5 * around_n
            h_p.append(plus(here, drop))
        m_h = [m_p[0] - m_p[1]]
        for n in range(1, 2 * ITERS - 1 - step):
            m_h.append(m_p[n] - 0.5 * (m_p[n + 1] + m_p[n - 1]))
        bottom = p[0] * m_h[0]
        for n in range(1, step + 1):
            bottom = bottom + p[n] * m_h[n]
        alpha = rz / bottom
        x = [plus(get(x, n), alpha * p[n]) for n in range(step + 1)]
        y = [plus(get(y, n), -(alpha * h_p[n])) for n in range(step + 2)]
        if step + 1 < ITERS:
            m_y = [m_y[n] - alpha * m_h[n] for n in range(len(m_h))]
            rz_next = y[0] * m_y[0]
            for n in range(1, step + 2):
                rz_next = rz_next + y[n] * m_y[n]
            beta = rz_next / rz
            p = [plus(y[n], None if n > step else beta * p[n]) for n in range(step + 2)]
            m_p = [m_y[n] + beta * m_p[n] for n in range(len(m_y))]
            rz = rz_next
    mean = x[0] * ones[0]
    for n in range(1, ITERS):
        mean = mean + x[n] * ones[n]
    mean = mean / count
    xs = [jnp.broadcast_to(value, (8, ny)) for value in x]
    ys = [jnp.broadcast_to(value, (8, ny)) for value in y]
    mean = jnp.broadcast_to(mean, (8, ny))
    for slot in range(nz):
        target = flip(slot, side)
        for row in range(0, nx, 8):
            spot = slice(8 + row, 16 + row)
            weight = scale[slot, row : row + 8]
            total = jnp.where(weight > 0.0, -mean, 0.0)
            rest = ys[ITERS] * basis[ITERS, slot, spot]
            for n in range(ITERS):
                value = basis[n, slot, spot]
                total = total + xs[n] * value
                rest = rest + ys[n] * value
            phi[target, row : row + 8] = total
            residual[target, row : row + 8] = weight * rest


def fast_body(potential, tissue_mask, layer_index, source):
    extent = tissue_mask.shape
    nz, nx, ny = extent
    sizes = tuple(lax.axis_size(axis) for axis in AXES)
    planes, held, deep = 2 * nz, nx + 16, nx + 32
    peers = math.prod(sizes)
    vmem = pl.BlockSpec(memory_space=pltpu.VMEM)
    hbm = pl.BlockSpec(memory_space=pltpu.HBM)

    def real(*shape):
        return pltpu.VMEM(shape + (ny,), jnp.float32)

    moves = 16
    scratch = [
        real(3, planes, held), pltpu.VMEM(extent, jnp.int32), real(5, nx), real(2, 2, nz),
        real(2, 2, 2, nz), real(5, deep), real(5, deep), real(5, 2, deep),
        real(9, planes + 6, deep), real(18, planes + 2, held), real(ITERS + 1, planes + 2, held),
        real(2, planes + 2, held), real(4, 3, held), real(planes + 2, held),
        real(planes + 2, held), real(nz, nx), real(2, COEFS, 8), real(3 * ITERS),
        real(1), real(sizes[1] * sizes[2], 1), real(1), real(sizes[0], 1), real(1), real(peers, 1),
        pltpu.SMEM((LAYERS, 18), jnp.float32), pltpu.SMEM((planes, COEFS), jnp.float32),
        pltpu.SMEM((nz,), jnp.int32), pltpu.SMEM((nz,), jnp.int32), pltpu.SMEM((planes,), jnp.int32),
        pltpu.SemaphoreType.DMA((4,)), pltpu.SemaphoreType.DMA((moves,)),
        pltpu.SemaphoreType.DMA((moves,)), pltpu.SemaphoreType.DMA((3,)),
        pltpu.SemaphoreType.DMA((3,)),
    ]
    return tuple(
        pl.pallas_call(
            functools.partial(fast_kernel, extent, sizes),
            out_shape=(jax.ShapeDtypeStruct(extent, jnp.float32),) * 2,
            in_specs=[hbm] * 4,
            out_specs=(vmem, vmem),
            scratch_shapes=scratch,
            compiler_params=pltpu.CompilerParams(
                vmem_limit_bytes=32 * 1024 * 1024, collective_id=0, has_side_effects=True
            ),
        )(potential, tissue_mask, layer_index, source)
    )


def body(potential, tissue_mask, layer_index, source):
    nz, nx, ny = tissue_mask.shape
    fits = (
        lax.axis_size("gz") == 2 and nz == 8 and ITERS == 8 and nx % 8 == 0 and nx >= 16
        and ny == nz * GROUP and lax.axis_size("gx") > 1 and lax.axis_size("gy") > 1
    )
    return (fast_body if fits else general_body)(potential, tissue_mask, layer_index, source)


def solution(mesh):
    placed = (P("gz", "gx", "gy"), P("gz", "gx", "gy"), P("gz"), P("gz", "gx", "gy"))
    return jax.shard_map(
        body,
        mesh=mesh,
        in_specs=placed,
        out_specs=(P("gz", "gx", "gy"), P("gz", "gx", "gy")),
        check_vma=False,
    )
```

```python
import functools
import math

import jax
import jax.numpy as jnp
from jax import lax
from jax.experimental import pallas as pl
from jax.experimental.pallas import tpu as pltpu
from jax.sharding import PartitionSpec as P
import numpy as np

ITERS = 8
DEPTH = ITERS + 1
LAYERS = 16
AXES = ("gx", "gy", "gz")

OFFSETS = [
    (0, 1, 0),
    (0, 0, 1),
    (1, 0, 0),
    (0, 1, 1),
    (0, 1, -1),
    (1, 1, 0),
    (-1, 1, 0),
    (1, 0, 1),
    (-1, 0, 1),
]
bulk_long = 7.99
bulk_trans = 2.55
intra_long = 1.74
intra_trans = 0.19
bath_sigma = 5.0


def tensor_table(layers, longitudinal, transverse):
    depth = jnp.arange(layers, dtype=jnp.float32) / (layers - 1)
    helix = math.pi / 3.0 * (1.0 - 2.0 * depth)
    tilted = 0.35 * jnp.cos(math.pi * depth)
    fiber_x = jnp.cos(tilted) * jnp.cos(helix)
    fiber_y = jnp.cos(tilted) * jnp.sin(helix)
    fiber_z = jnp.sin(tilted)
    spread = longitudinal - transverse
    s_xx = transverse + spread * fiber_x * fiber_x
    s_yy = transverse + spread * fiber_y * fiber_y
    s_zz = transverse + spread * fiber_z * fiber_z
    s_xy = spread * fiber_x * fiber_y
    s_xz = spread * fiber_x * fiber_z
    s_yz = spread * fiber_y * fiber_z
    columns = [
        s_xx - jnp.abs(s_xy) - jnp.abs(s_xz),
        s_yy - jnp.abs(s_xy) - jnp.abs(s_yz),
        s_zz - jnp.abs(s_xz) - jnp.abs(s_yz),
        jnp.maximum(s_xy, 0.0),
        jnp.maximum(-s_xy, 0.0),
        jnp.maximum(s_xz, 0.0),
        jnp.maximum(-s_xz, 0.0),
        jnp.maximum(s_yz, 0.0),
        jnp.maximum(-s_yz, 0.0),
    ]
    return jnp.stack(columns, axis=1)


def shifted(value, axis, hop):
    count = lax.axis_size(axis)
    pairs = [(i + hop, i) for i in range(count) if 0 <= i + hop < count]
    return lax.ppermute(value, axis, pairs)


def framed(value, axis, dim, multiple):
    count, length = lax.axis_size(axis), value.shape[dim]
    if count == 1:
        return value
    if count == 2 and 2 * length <= length + 2 * DEPTH and multiple == 1:
        other = lax.ppermute(value, axis, [(0, 1), (1, 0)])
        return jnp.concatenate([value, other], axis=dim)
    after, before = [], []
    left, hop = DEPTH, 1
    while left > 0:
        width = min(left, length)
        if hop < count:
            after.append(
                shifted(lax.slice_in_dim(value, 0, width, axis=dim), axis, hop)
            )
            before.insert(
                0, shifted(lax.slice_in_dim(value, length - width, length, axis=dim), axis, -hop)
            )
        else:
            shape = list(value.shape)
            shape[dim] = width
            after.append(jnp.zeros(shape, value.dtype))
            before.insert(0, jnp.zeros(shape, value.dtype))
        left, hop = left - width, hop + 1
    gap = -(length + 2 * DEPTH) % multiple
    shape = list(value.shape)
    shape[dim] = gap
    middle = [jnp.zeros(shape, value.dtype)] if gap else []
    return jnp.concatenate([value] + after + middle + before, axis=dim)


def fields_around(ref, here, above, below, rows, lanes):
    def along_x(value, step):
        return pltpu.roll(value, (-step) % rows, 0)

    def along_y(value, step):
        return pltpu.roll(value, (-step) % lanes, 1)

    for dz, plane in ((0, here), (1, above), (-1, below)):
        value = ref[plane]
        if dz:
            yield (dz, 0, 0), value
        for step in (1, -1):
            yield (dz, step, 0), along_x(value, step)
        for step in (1, -1):
            moved = along_y(value, step)
            yield (dz, 0, step), moved
            if dz == 0:
                for other in (1, -1):
                    yield (0, other, step), along_x(moved, other)


SLOT = {}
for _column, _offset in enumerate(OFFSETS):
    SLOT[_offset] = (_column, 2 * _column)
    SLOT[tuple(-o for o in _offset)] = (_column, 2 * _column + 1)


def grid_kernel(extent, sizes, table, mask_in, potential_in, source_in, phi, residual,
                basis, scale, dots, weights, spare, first, second, jac,
                own_row, early, final_row, late, sends, early_recv, late_recv):
    mask, potential, source = mask_in, potential_in, source_in
    planes, rows, lanes = mask.shape
    nz, nx, ny = extent
    held = jac.shape[1]
    keep = nx + ITERS
    peers = math.prod(sizes)
    me = 0
    for axis, size in zip(AXES, sizes):
        me = me * size + lax.axis_index(axis)

    def device(index):
        return (index // (sizes[1] * sizes[2]), index // sizes[2] % sizes[1], index % sizes[2])

    def peer(k):
        return lax.rem(me + k, peers)

    barrier = pltpu.get_barrier_semaphore()

    def greet(k, carry):
        pl.semaphore_signal(
            barrier, inc=1, device_id=device(peer(k)), device_id_type=pl.DeviceIdType.MESH
        )
        return carry

    lax.fori_loop(1, peers, greet, 0)

    def spread(row, gathered, recv):
        def one(k, carry):
            pltpu.make_async_remote_copy(
                src_ref=row, dst_ref=gathered.at[me], send_sem=sends.at[k],
                recv_sem=recv.at[me], device_id=device(peer(k)),
                device_id_type=pl.DeviceIdType.MESH,
            ).start()
            return carry

        lax.fori_loop(1, peers, one, 0)

    def collect(row, gathered, recv):
        def one(k, carry):
            other = peer(k)
            copy = pltpu.make_async_remote_copy(
                src_ref=row, dst_ref=gathered.at[other], send_sem=sends.at[k],
                recv_sem=recv.at[other], device_id=device(other),
                device_id_type=pl.DeviceIdType.MESH,
            )
            copy.wait_recv()
            copy.wait_send()
            return carry

        lax.fori_loop(1, peers, one, 0)
        gathered[me] = row[...]
        return jnp.sum(gathered[...], axis=0)

    lane = lax.broadcasted_iota(jnp.int32, (1, 128), 1)

    def pick(vector, index):
        return jnp.sum(jnp.where(lane == index, vector, 0.0), axis=1, keepdims=True)

    cells = jnp.zeros((1, ny), jnp.float32)
    injected = jnp.zeros((1, ny), jnp.float32)
    for plane in range(nz):
        own_inside = jnp.where(mask_in[plane, 0:nx, 0:ny] > 0.0, 1.0, 0.0)
        cells = cells + jnp.sum(own_inside, axis=0, keepdims=True)
        injected = injected + jnp.sum(
            own_inside * source_in[plane, 0:nx, 0:ny], axis=0, keepdims=True
        )
    cells = jnp.sum(cells, axis=1, keepdims=True)
    injected = jnp.sum(injected, axis=1, keepdims=True)
    own_row[...] = jnp.where(lane == 0, cells, jnp.where(lane == 1, injected, 0.0))

    def neighbours(plane):
        above = jnp.where(plane + 1 == planes, 0, plane + 1)
        below = jnp.where(plane == 0, planes - 1, plane - 1)
        return above, below

    def store(ref, index, value):
        if held == rows:
            ref[index] = value
        else:
            ref[(*index, slice(0, keep))] = value[:keep]
            ref[(*index, slice(keep, held))] = value[rows - held + keep :]

    def setup(plane, carry):
        above, below = neighbours(plane)
        labels = mask[plane]
        tissue = jnp.where(labels == 2.0, 1.0, 0.0)
        bath = jnp.where(labels == 1.0, 1.0, 0.0)
        inside = tissue + bath
        volts = potential[plane]
        total = jnp.zeros((rows, lanes), jnp.float32)
        image = jnp.zeros((rows, lanes), jnp.float32)
        pairs = zip(
            fields_around(mask, plane, above, below, rows, lanes),
            fields_around(potential, plane, above, below, rows, lanes),
        )
        for (offset, label), (_, volt) in pairs:
            column, slot = SLOT[offset]
            beyond = {0: plane, 1: above, -1: below}[offset[0]]
            link = 0.5
            if offset[0] == 1:
                link = 0.5 * table[plane, 18]
            if offset[0] == -1:
                link = 0.5 * table[below, 18]
            their_tissue = jnp.where(label == 2.0, 1.0, 0.0)
            g_here, g_there = table[plane, column] * link, table[beyond, column] * link
            weight = tissue * g_here
            if column < 3:
                their_bath = jnp.where(label == 1.0, 1.0, 0.0)
                sigma = bath_sigma * link
                weight = inside * (
                    jnp.where(label > 0.0, weight + bath * sigma, 0.0)
                    + (their_tissue * g_there + their_bath * sigma)
                )
            else:
                weight = inside * (jnp.where(label > 0.0, weight, 0.0) + their_tissue * g_there)
            store(weights, (slot, plane), weight)
            total = total + weight
            intra = (table[plane, 9 + column] + table[beyond, 9 + column]) * link
            image = image + (tissue * their_tissue * intra) * (volts - volt)
        bounded = jnp.maximum(total, 1.0)
        jacobi = inside / bounded
        store(jac, (plane,), jacobi + jacobi)
        store(spare, (plane,), inside * (1.0 - jacobi * total))
        store(first, (plane,), jacobi * (inside * source[plane] - image))

        @pl.when(plane < nz)
        def _():
            scale[plane] = (inside * bounded)[:nx, :ny]

        return carry

    lax.fori_loop(0, planes // 2, setup, 0)
    pl.semaphore_wait(barrier, peers - 1)
    spread(own_row, early, early_recv)
    lax.fori_loop(planes // 2, planes, setup, 0)
    totals = collect(own_row, early, early_recv)
    count = pick(totals, 0)
    mean_rhs = pick(totals, 1) / count

    def centre(plane, carry):
        first[plane] = first[plane] - 0.5 * jac[plane] * mean_rhs
        return carry

    lax.fori_loop(0, planes, centre, 0)

    def record(step, now, before):
        rowsum = jnp.zeros((1, ny), jnp.float32)
        square, cross, plain = rowsum, rowsum, rowsum
        for plane in range(nz):
            value = now[plane, 0:nx, 0:ny]
            basis[step, plane] = value
            weighted = value * scale[plane]
            square = square + jnp.sum(weighted * value, axis=0, keepdims=True)
            if step:
                past = basis[step - 1, plane]
                cross = cross + jnp.sum(weighted * past, axis=0, keepdims=True)
            plain = plain + jnp.sum(value, axis=0, keepdims=True)
        if step < ITERS:
            dots[pl.ds(2 * step, 1)] = square
            dots[pl.ds(2 * ITERS + step, 1)] = plain
        if step:
            dots[pl.ds(2 * step - 1, 1)] = cross

    record(0, first, None)

    def apply(now, old, step):
        reach = ITERS - step
        if planes == nz:
            begin, span = 0, nz
        elif planes == sizes[2] * nz:
            begin = planes - lax.axis_index("gz") * reach
            span = min(planes, nz + reach)
        else:
            begin, span = planes - reach, nz + 2 * reach

        def one(index, carry):
            plane = lax.rem(begin + index, planes)
            above, below = neighbours(plane)
            total = jnp.zeros((held, lanes), jnp.float32)
            for offset, value in fields_around(now, plane, above, below, held, lanes):
                total = total + weights[SLOT[offset][1], plane] * value
            if step == 1:
                old[plane] = 0.5 * jac[plane] * total + spare[plane] * now[plane]
            else:
                old[plane] = (
                    jac[plane] * total + 2.0 * spare[plane] * now[plane] - old[plane]
                )
            return carry

        lax.fori_loop(0, span, one, 0)

    now, old = first, second
    for step in range(1, ITERS + 1):
        apply(now, old, step)
        now, old = old, now
        record(step, now, old)

    partial = jnp.sum(dots[...], axis=1, keepdims=True)
    diagonal = lax.broadcasted_iota(jnp.int32, (3 * ITERS, 128), 0) == lax.broadcasted_iota(
        jnp.int32, (3 * ITERS, 128), 1
    )
    final_row[...] = jnp.sum(jnp.where(diagonal, partial, 0.0), axis=0, keepdims=True)
    spread(final_row, late, late_recv)
    sums = collect(final_row, late, late_recv)

    def left(vector):
        return pltpu.roll(vector, 127, 1)

    def right(vector):
        return pltpu.roll(vector, 1, 1)

    mu0, mu1 = pick(sums, 0), pick(sums, 1)
    mu = jnp.where(lane < 2, sums, 2.0 * sums - jnp.where(lane % 2 == 0, mu0, mu1))
    mu = jnp.where(lane < 2 * ITERS, mu, 0.0)
    ones = pltpu.roll(sums, 128 - 2 * ITERS, 1)
    y = jnp.where(lane == 0, 1.0, 0.0)
    p = y
    m_y, m_p = mu, mu
    x = jnp.zeros((1, 128), jnp.float32)
    rz = mu0
    for step in range(ITERS):
        h_p = p - 0.5 * (left(p) + jnp.where(lane == 1, 2.0, 1.0) * right(p))
        h_p = jnp.where(lane <= ITERS, h_p, 0.0)
        before = jnp.where(lane == 0, left(m_p), right(m_p))
        m_h = m_p - 0.5 * (left(m_p) + before)
        alpha = rz / jnp.sum(jnp.where(lane < ITERS, p * m_h, 0.0), axis=1, keepdims=True)
        x = x + alpha * p
        y = y - alpha * h_p
        m_y = m_y - alpha * m_h
        if step + 1 < ITERS:
            rz_next = jnp.sum(jnp.where(lane < ITERS, y * m_y, 0.0), axis=1, keepdims=True)
            beta = rz_next / rz
            p = y + beta * p
            m_p = m_y + beta * m_p
            rz = rz_next
    mean = jnp.sum(jnp.where(lane < ITERS, x * ones, 0.0), axis=1, keepdims=True) / count
    xs = [pick(x, j) for j in range(ITERS)]
    ys = [pick(y, j) for j in range(ITERS + 1)]

    def one(plane, carry):
        weight = scale[plane]
        total = jnp.where(weight > 0.0, -mean, 0.0)
        rest = ys[ITERS] * basis[ITERS, plane]
        for j in range(ITERS):
            value = basis[j, plane]
            total = total + xs[j] * value
            rest = rest + ys[j] * value
        phi[plane] = total
        residual[plane] = weight * rest
        return carry

    lax.fori_loop(0, nz, one, 0)


def general_body(potential, tissue_mask, layer_index, source):
    extent = tissue_mask.shape
    nz = extent[0]
    labels = tissue_mask.astype(jnp.float32)
    sizes = tuple(lax.axis_size(axis) for axis in AXES)
    packed = jnp.stack([labels, potential, source], axis=1)
    packed = framed(packed, "gz", 0, 1)
    packed = framed(packed, "gx", 2, 8)
    packed = framed(packed, "gy", 3, 128)
    operands = (packed[:, 0], packed[:, 1], packed[:, 2])
    frame = operands[0].shape
    layers = framed(layer_index, "gz", 0, 1)
    planes = layers.shape[0]
    selector = (layers[:, None] == jnp.arange(LAYERS, dtype=jnp.int32)[None, :]).astype(
        jnp.float32
    )
    tables = jnp.concatenate(
        [
            tensor_table(LAYERS, bulk_long, bulk_trans),
            tensor_table(LAYERS, intra_long, intra_trans),
        ],
        axis=1,
    )
    table = jnp.dot(selector, tables, precision=lax.Precision.HIGHEST)
    size = lax.axis_size("gz")
    link = jnp.ones((planes, 1), jnp.float32)
    if planes == size * nz:
        place = (lax.axis_index("gz") * nz + jnp.arange(planes)) % planes
        link = (place + 1 < planes).astype(jnp.float32)[:, None]
    table = jnp.concatenate([table, link], axis=1)
    smem = pl.BlockSpec(memory_space=pltpu.SMEM)
    vmem = pl.BlockSpec(memory_space=pltpu.VMEM)
    compact = frame
    if extent[1] % 8 == 0 and ITERS % 8 == 0 and frame[1] > extent[1] + 2 * ITERS:
        compact = (planes, extent[1] + 2 * ITERS, frame[2])
    peers = math.prod(sizes)
    row = pltpu.VMEM((1, 128), jnp.float32)
    gathered = pltpu.VMEM((peers, 1, 128), jnp.float32)
    return tuple(
        pl.pallas_call(
            functools.partial(grid_kernel, extent, sizes),
            out_shape=(jax.ShapeDtypeStruct(extent, jnp.float32),) * 2,
            in_specs=[smem, vmem, vmem, vmem],
            out_specs=(vmem, vmem),
            scratch_shapes=[
                pltpu.VMEM((ITERS + 1,) + extent, jnp.float32),
                pltpu.VMEM(extent, jnp.float32),
                pltpu.VMEM((3 * ITERS, extent[2]), jnp.float32),
                pltpu.VMEM((18,) + compact, jnp.float32),
            ]
            + [pltpu.VMEM(compact, jnp.float32)] * 4
            + [row, gathered, row, gathered]
            + [pltpu.SemaphoreType.DMA((peers,))] * 3,
            compiler_params=pltpu.CompilerParams(
                vmem_limit_bytes=60 * 1024 * 1024, collective_id=0, has_side_effects=True
            ),
        )(table, *operands)
    )


GROUP = 16
TERMS_SAME = [(0, 1), (0, -1), (1, 0), (-1, 0), (1, 1), (1, -1), (-1, 1), (-1, -1)]
TERMS_SIDE = [(0, 0), (0, 1), (0, -1), (1, 0), (-1, 0)]
LEVEL = [0, 1, 3, 4]
STEEP = [(0, 0), (1, 0), (-1, 0), (0, 1), (0, -1)]
COEFS = 2 * len(LEVEL) + 2 * (1 + 3 * len(STEEP))


def numpy_table(longitudinal, transverse):
    depth = np.arange(LAYERS, dtype=np.float64) / (LAYERS - 1)
    helix = math.pi / 3.0 * (1.0 - 2.0 * depth)
    tilted = 0.35 * np.cos(math.pi * depth)
    fiber = (np.cos(tilted) * np.cos(helix), np.cos(tilted) * np.sin(helix), np.sin(tilted))
    spread = longitudinal - transverse
    s_xx, s_yy, s_zz = (transverse + spread * f * f for f in fiber)
    s_xy = spread * fiber[0] * fiber[1]
    s_xz = spread * fiber[0] * fiber[2]
    s_yz = spread * fiber[1] * fiber[2]
    columns = [s_xx - abs(s_xy) - abs(s_xz), s_yy - abs(s_xy) - abs(s_yz), s_zz - abs(s_xz) - abs(s_yz)]
    for value in (s_xy, s_xz, s_yz):
        columns += [np.maximum(value, 0.0), np.maximum(-value, 0.0)]
    return np.stack(columns, axis=1)


HALF_TABLE = 0.5 * np.concatenate(
    [numpy_table(bulk_long, bulk_trans), numpy_table(intra_long, intra_trans)], axis=1
)


def lane_roll(value, step):
    return pltpu.roll(value, step % value.shape[1], 1)


def row_roll(value, step):
    return pltpu.roll(value, step % value.shape[0], 0)


def tiled(value, rows):
    return jnp.concatenate([value] * (rows // value.shape[0]), axis=0)


def column_of(dz, dx, dy, side):
    same, flipped = SLOT[(dz, dx, dy)][0], SLOT[(-dz, dx, dy)][0]
    return same if same == flipped else same + side * (flipped - same)


def fast_kernel(extent, sizes, potential_in, mask_in, layers_in, source_in, phi, residual,
                fields, labels, packs, edge_send, edge_recv, from_after, from_before, strips,
                derived, weights, basis, moved, beside, jac, spare, scale, coef_lanes, dots,
                early_row, early_all, line_row, line_all, final_row, final_all,
                table, coefs, layers_own, layers_far, layers,
                loads, halo_send, halo_recv, sum_send, sum_recv):
    nz, nx, ny = extent
    planes, held, deep = 2 * nz, nx + 16, nx + 32
    own = slice(8, 8 + nx)
    place = tuple(lax.axis_index(axis) for axis in AXES)
    gx, gy, side = place
    first_x, last_x = gx == 0, gx == sizes[0] - 1
    first_y, last_y = gy == 0, gy == sizes[1] - 1

    def exists(dx, dy):
        return (gx + dx >= 0) & (gx + dx < sizes[0]) & (gy + dy >= 0) & (gy + dy < sizes[1])

    def around(a, b, c):
        return tuple(
            lax.rem(here + step, size) if step else here
            for here, step, size in zip(place, (a, b, c), sizes)
        )

    slab = [(0, b, c) for b in range(sizes[1]) for c in range(sizes[2])]
    line = [(a, 0, 0) for a in range(sizes[0])]
    everyone = [(a, b, c) for a, _, _ in line for _, b, c in slab]
    corners = [(dx, dy) for dx in (1, -1) for dy in (1, -1)]

    def flip(slot, turned):
        return slot + turned * (nz - 1 - 2 * slot)

    get_layers = pltpu.make_async_copy(layers_in, layers_own, loads.at[0])
    get_mask = pltpu.make_async_copy(mask_in, labels, loads.at[1])
    get_layers.start()
    get_mask.start()
    whole = []
    for index, ref in ((1, potential_in), (2, source_in)):
        for plane in range(nz):
            pltpu.make_async_copy(
                ref.at[plane], fields.at[index, flip(plane, side), own], loads.at[1 + index]
            ).start()
        whole.append(pltpu.make_async_copy(ref, fields.at[index, 0:nz, own], loads.at[1 + index]))

    barrier = pltpu.get_barrier_semaphore()

    def greet(target):
        pl.semaphore_signal(
            barrier, inc=1, device_id=target, device_id_type=pl.DeviceIdType.MESH
        )

    expected = len(slab) + len(line) - 2
    for step in slab[1:] + line[1:]:
        greet(around(*step))
    for dx, dy in corners:
        pl.when(exists(dx, dy))(lambda: greet((gx + dx, gy + dy, side)))
        expected = expected + jnp.where(exists(dx, dy), 1, 0)

    def clear(when, ref, index):
        @pl.when(when)
        def _():
            ref[index] = jnp.zeros(ref.at[index].shape, jnp.float32)

    every = slice(None)
    clear(first_x, fields, (every, slice(0, nz), slice(0, 8)))
    clear(last_x, fields, (every, slice(0, nz), slice(8 + nx, held)))
    for index in range(2):
        clear(first_x, edge_recv, (0, index, 0))
        clear(last_x, edge_recv, (0, index, 1))
    for ref, edge in ((from_after, last_y), (from_before, first_y)):
        clear(edge, ref, (every,))
        clear(first_x, ref, (every, slice(0, 16)))
        clear(last_x, ref, (every, slice(16 + nx, deep)))
    def lanes_of(rows):
        lane = lax.broadcasted_iota(jnp.int32, (rows, ny), 1)
        return lane, lane // GROUP, lane % GROUP

    get_layers.wait()
    get_mask.wait()
    for plane in range(nz):
        fields[0, flip(plane, side), own] = labels[plane].astype(jnp.float32)
    for copy in whole:
        copy.wait()

    lane = lax.broadcasted_iota(jnp.int32, (1, ny), 1)

    def pick(vector, index):
        return jnp.sum(jnp.where(lane == index, vector, 0.0), axis=1, keepdims=True)

    _, group, inner = lanes_of(nx)

    def packed(values, shift):
        total = values[0]
        total = lane_roll(total, shift)
        for g in range(1, nz):
            total = jnp.where(group == g, lane_roll(values[g], GROUP * g + shift), total)
        return total

    for index in range(3):
        values = [fields[index, slot, own] for slot in range(nz)]
        packs[2 * index] = packed(values, 8)
        if index < 2:
            packs[2 * index + 1] = jnp.where(inner == 15, packed(values, 7), packed(values, 9))
            for slot in range(nz):
                edge_send[index, 0, slot : slot + 1] = values[slot][8:9]
                edge_send[index, 1, slot : slot + 1] = values[slot][nx - 9 : nx - 8]

    cells = jnp.zeros((8, ny), jnp.float32)
    injected = cells
    for slot in range(nz):
        for row in range(8, 8 + nx, 8):
            inside = jnp.where(fields[0, slot, row : row + 8] > 0.0, 1.0, 0.0)
            cells = cells + inside
            injected = injected + inside * fields[2, slot, row : row + 8]
    cells = jnp.sum(jnp.sum(cells, axis=0, keepdims=True), axis=1, keepdims=True)
    injected = jnp.sum(jnp.sum(injected, axis=0, keepdims=True), axis=1, keepdims=True)
    early_row[...] = jnp.where(lane == 0, cells, jnp.where(lane == 1, injected, 0.0))

    pl.semaphore_wait(barrier, expected)

    def spread(number, row, gathered, targets):
        for index, step in enumerate(targets):
            if index:
                pltpu.make_async_remote_copy(
                    src_ref=row, dst_ref=gathered.at[index], send_sem=sum_send.at[number],
                    recv_sem=sum_recv.at[number], device_id=around(*step),
                    device_id_type=pl.DeviceIdType.MESH,
                ).start()

    def collect(number, row, gathered, targets):
        arrived = gathered.at[pl.ds(1, len(targets) - 1)]
        pltpu.make_async_copy(arrived, arrived, sum_recv.at[number]).wait()
        pltpu.make_async_copy(arrived, arrived, sum_send.at[number]).wait()
        gathered[0] = row[...]
        return jnp.sum(gathered[...], axis=0)

    spread(0, early_row, early_all, slab)

    def link(number, src, dst, target):
        return pltpu.make_async_remote_copy(
            src_ref=src, dst_ref=dst, send_sem=halo_send.at[number],
            recv_sem=halo_recv.at[number], device_id=target,
            device_id_type=pl.DeviceIdType.MESH,
        )

    other = (gx, gy, 1 - side)
    numbers = iter(range(64))

    def swap(src, dst):
        copy = link(next(numbers), src, dst, other)
        copy.start()
        return copy

    def exchange(picked, rows, edge):
        found = []

        def move(dx, dy, src, dst):
            copy = link(next(numbers), src, dst, (gx + dx, gy + dy, side))
            pl.when(exists(dx, dy))(copy.start)
            found.append((exists(-dx, -dy), exists(dx, dy), copy))

        for dx, dy in corners:
            into = from_before if dy == 1 else from_after
            if dx == 1:
                move(dx, dy, packs.at[picked, nx - 16 : nx], into.at[picked, 0:16])
            else:
                move(dx, dy, packs.at[picked, 0:16], into.at[picked, 16 + nx : deep])
        move(0, 1, packs.at[picked], from_before.at[picked, 16 : 16 + nx])
        move(0, -1, packs.at[picked], from_after.at[picked, 16 : 16 + nx])
        move(1, 0, edge_send.at[edge, 1], edge_recv.at[0, edge, 0])
        move(-1, 0, edge_send.at[edge, 0], edge_recv.at[0, edge, 1])
        move(1, 0, fields.at[rows, 0:nz, nx : nx + 8], fields.at[rows, 0:nz, 0:8])
        move(-1, 0, fields.at[rows, 0:nz, 8:16], fields.at[rows, 0:nz, 8 + nx : held])
        return found

    groups = [(slice(0, 2), slice(0, 1), 0), (slice(2, 5), slice(1, 3), 1)]
    layer_swap = swap(layers_own, layers_far)
    moves, relays = [], []
    for picked, rows, edge in groups:
        moves.append(exchange(picked, rows, edge))
        relays.append([swap(fields.at[rows, 0:nz, own], fields.at[rows, nz:planes, own])])

    def relay(picked, rows, edge):
        for receives, _, copy in moves[edge]:
            pl.when(receives)(copy.wait_recv)
        for index in range(picked.start, picked.stop):
            strips[index, 0] = jnp.where(inner_deep < 8, from_before[index], from_after[index])
        relays[edge] += [
            swap(strips.at[picked, 0], strips.at[picked, 1]),
            swap(edge_recv.at[0, edge], edge_recv.at[1, edge]),
            swap(fields.at[rows, 0:nz, 0:8], fields.at[rows, nz:planes, 0:8]),
            swap(fields.at[rows, 0:nz, 8 + nx : held], fields.at[rows, nz:planes, 8 + nx : held]),
        ]

    for layer in range(LAYERS):
        for column in range(18):
            table[layer, column] = jnp.float32(HALF_TABLE[layer, column])

    layer_swap.wait()
    for slot in range(nz):
        layers[slot] = layers_own[flip(slot, side)]
        layers[nz + slot] = layers_far[flip(slot, 1 - side)]

    def slot_of(j):
        return jnp.where(j < nz, j, 3 * nz - 1 - j)

    def coefficients(slot, carry):
        j = slot_of(slot)
        layer = layers[slot]
        for n, k in enumerate(LEVEL):
            coefs[slot, 2 * n] = table[layer, k]
            coefs[slot, 2 * n + 1] = 2.0 * table[layer, 9 + k]
        for half, dz in enumerate((1, -1)):
            near = (j + dz >= 0) & (j + dz < planes)
            there = layers[slot_of(jnp.where(near, j + dz, j))]
            open_ = jnp.where(near, 1.0, 0.0).astype(jnp.float32)
            start = 2 * len(LEVEL) + half * (1 + 3 * len(STEEP))
            coefs[slot, start] = 0.5 * bath_sigma * open_
            for n, (dx, dy) in enumerate(STEEP):
                k = column_of(dz, dx, dy, side)
                coefs[slot, start + 1 + 3 * n] = table[layer, k] * open_
                coefs[slot, start + 2 + 3 * n] = table[there, k] * open_
                coefs[slot, start + 3 + 3 * n] = (table[layer, 9 + k] + table[there, 9 + k]) * open_
        return carry

    lax.fori_loop(0, planes, coefficients, 0)
    _, group8, _ = lanes_of(8)

    def widen(n, carry):
        for q in range(2):
            value = jnp.full((8, ny), coefs[q * nz, n], jnp.float32)
            for g in range(1, nz):
                value = jnp.where(group8 == g, coefs[q * nz + g, n], value)
            coef_lanes[q, n] = value
        return carry

    lax.fori_loop(0, COEFS, widen, 0)

    lane_of, group_of, inner_deep = lanes_of(deep)
    relay(*groups[0])
    line_row[...] = collect(0, early_row, early_all, slab)
    spread(1, line_row, line_all, line)

    def sides(value, strip, g):
        ring = lane_roll(strip, -(GROUP * g + 8))
        after = lane_roll(jnp.where(lane_of == 0, ring, value), -1)
        before = lane_roll(jnp.where(lane_of == ny - 1, ring, value), 1)
        return after, before

    def stored(index, number, slot, value):
        if index:
            derived[3 * number + 2, slot] = value
        else:
            derived[3 * number, slot] = jnp.where(value == 2.0, 1.0, 0.0)
            derived[3 * number + 1, slot] = jnp.where(value > 0.0, 1.0, 0.0)

    def framed_plane(index, q, g):
        before = jnp.broadcast_to(edge_recv[q, index, 0, g : g + 1], (8, ny))
        after = jnp.broadcast_to(edge_recv[q, index, 1, g : g + 1], (8, ny))
        return jnp.concatenate([before, fields[index, q * nz + g], after], axis=0)

    def derive(index):
        def one(q, carry):
            @pl.when(q == 1)
            def _():
                for copy in relays[index]:
                    copy.wait_recv()

            strip, edge = strips[2 * index, q], strips[2 * index + 1, q]
            mixed = strip
            for g in range(nz):
                value = framed_plane(index, q, g)
                mixed = jnp.where(group_of == g, lane_roll(value, GROUP * g + 8), mixed)
                for number, part in enumerate((value,) + sides(value, strip, g)):
                    stored(index, number, q * nz + g, part)
            after = lane_roll(jnp.where(inner_deep == 8, mixed, strip), -1)
            before = lane_roll(jnp.where(inner_deep == 7, mixed, strip), 1)
            stored(index, 0, planes + q, strip)
            stored(index, 1, planes + q, jnp.where(inner_deep == 15, edge, after))
            stored(index, 2, planes + q, jnp.where(inner_deep == 0, edge, before))
            return carry

        lax.fori_loop(0, 2, one, 0)
        for number in ((2, 5, 8) if index else (0, 1, 3, 4, 6, 7)):
            found = across(derived[number, planes], derived[number, planes + 1])
            for shift, value in enumerate(found):
                derived[number, planes + 2 + shift] = value

    def across(lower, upper):
        up0 = jnp.where(group_of == nz - 1, upper, lane_roll(lower, -GROUP))
        up1 = lane_roll(upper, GROUP)
        down0 = lane_roll(lower, GROUP)
        down1 = jnp.where(group_of == nz - 1, lower, lane_roll(upper, -GROUP))
        return up0, up1, down0, down1

    derive(0)

    def level_of(coef):
        return {k: (coef(2 * n), coef(2 * n + 1)) for n, k in enumerate(LEVEL)}

    def steep_of(coef, dz):
        start = 2 * len(LEVEL) + (0 if dz == 1 else 1 + 3 * len(STEEP))
        entries = {}
        for n, key in enumerate(STEEP):
            entries[key] = tuple(coef(start + 1 + 3 * n + m) for m in range(3))
        return coef(start), entries

    middle = slice(8, 8 + held)

    def by(value, factor):
        if isinstance(factor, float) or factor.ndim == 0:
            return value * factor
        return value * tiled(factor, value.shape[0])

    def gathered_terms(edges, full):
        sums = edges(tuple(value[middle] for value in full), middle, 0, TERMS_SAME, 0)
        high = tuple(row_roll(value, 1)[8:deep] for value in full)
        part = edges(high, slice(8, deep), 1, TERMS_SIDE, 8)
        sums = sums + row_roll(part, -1)[0:held]
        low = tuple(row_roll(value, -1)[0 : 8 + held] for value in full)
        part = edges(low, slice(0, 8 + held), -1, TERMS_SIDE, 13)
        return sums + row_roll(part, 1)[middle]

    def weigh(slot, above, below, coef):
        level, slopes = level_of(coef), {1: steep_of(coef, 1), -1: steep_of(coef, -1)}
        base_bath = 0.5 * bath_sigma
        neighbour = {0: slot, 1: above, -1: below}

        def fetch(dz, dy, rows):
            number = {0: 0, 1: 1, -1: 2}[dy]
            return tuple(derived[3 * number + m, neighbour[dz], rows] for m in range(2))

        def edges(centre, rows, dx, terms, first):
            t, i = centre
            total = None
            keep = {0: slice(0, held), 1: slice(0, held), -1: slice(8, 8 + held)}[dx]
            for number, (dz, dy) in enumerate(terms):
                tn, i_n = fetch(dz, dy, rows)
                if dz == 0:
                    g_here = g_there = level[SLOT[(0, dx, dy)][0]][0]
                    bath = base_bath
                else:
                    bath, entries = slopes[dz]
                    g_here, g_there, _ = entries[(dx, dy)]
                if (dz != 0) + (dx != 0) + (dy != 0) == 1:
                    ours = by(t, g_here - bath) + by(i, bath)
                    theirs = by(tn, g_there - bath) + by(i_n, bath)
                else:
                    ours, theirs = by(t, g_here), by(tn, g_there)
                weight = i_n * ours + i * theirs
                weights[first + number, slot] = weight[keep]
                total = weight if total is None else total + weight
            return total

        full = fetch(0, 0, slice(0, deep))
        total = gathered_terms(edges, full)
        inside = full[1][middle]
        bounded = jnp.maximum(total, 1.0)
        jacobi = inside / bounded
        jac[slot] = jacobi + jacobi
        spare[slot] = 2.0 * (inside - inside * (jacobi * total))
        return (inside * bounded)[own]

    def begin(slot, above, below, coef, source):
        level, slopes = level_of(coef), {1: steep_of(coef, 1), -1: steep_of(coef, -1)}
        neighbour = {0: slot, 1: above, -1: below}

        def edges(centre, rows, dx, terms, first):
            v = centre[0]
            image = None
            for dz, dy in terms:
                number = {0: 0, 1: 1, -1: 2}[dy]
                tn = derived[3 * number, neighbour[dz], rows]
                vn = derived[3 * number + 2, neighbour[dz], rows]
                if dz == 0:
                    intra = level[SLOT[(0, dx, dy)][0]][1]
                else:
                    intra = slopes[dz][1][(dx, dy)][2]
                term = by(tn * (v - vn), intra)
                image = term if image is None else image + term
            return image

        image = gathered_terms(edges, (derived[2, slot],))
        tissue, inside = derived[0, slot, middle], derived[1, slot, middle]
        value = 0.5 * jac[slot] * (inside * (source - mean_rhs) - tissue * image)
        basis[0, slot] = value
        return value[own]

    def beyond(slot):
        j = slot_of(slot)
        return slot_of(jnp.minimum(j + 1, planes - 1)), slot_of(jnp.maximum(j - 1, 0))

    def from_table(slot):
        return lambda n: coefs[slot, n]

    def from_lanes(q):
        return lambda n: coef_lanes[q, n]

    def own_weigh(slot, carry):
        scale[slot] = weigh(slot, *beyond(slot), from_table(slot))
        return carry

    def far_weigh(slot, carry):
        weigh(slot, *beyond(slot), from_table(slot))
        return carry

    def strip_weigh(q, carry):
        slot = planes + q
        weigh(slot, slot + 2, slot + 4, from_lanes(q))
        return carry

    lax.fori_loop(0, nz, own_weigh, 0)
    relay(*groups[1])
    lax.fori_loop(nz, planes, far_weigh, 0)
    lax.fori_loop(0, 2, strip_weigh, 0)
    derive(1)

    totals = collect(1, line_row, line_all, line)
    count = pick(totals, 0)
    mean_rhs = pick(totals, 1) / count

    def plane_begin(slot, carry):
        begin(slot, *beyond(slot), from_table(slot), fields[2, slot])
        return carry

    def strip_begin(q, carry):
        slot = planes + q
        begin(slot, slot + 2, slot + 4, from_lanes(q), strips[4, q, middle])
        return carry

    lax.fori_loop(0, planes, plane_begin, 0)
    lax.fori_loop(0, 2, strip_begin, 0)

    def folded(value):
        total = value[0:8]
        for row in range(8, value.shape[0], 8):
            total = total + value[row : row + 8]
        return total

    zero8 = jnp.zeros((8, ny), jnp.float32)

    def record(step, sums):
        for kind, value in enumerate(sums):
            dots[kind * (ITERS + 1) + step] = value

    sums = [zero8, zero8, zero8]
    for slot in range(nz):
        value = basis[0, slot, own]
        sums[0] = sums[0] + folded(value * value * scale[slot])
        sums[2] = sums[2] + folded(value)
    record(0, sums)

    lane_of, group_of, inner_held = lanes_of(held)

    def at(j):
        return j if j < nz else 3 * nz - 1 - j

    def advance(step, slot, near, rows, first):
        same = None
        for number, (dz, dy) in enumerate(TERMS_SAME):
            value = near(dz, dy)
            if value is None:
                continue
            term = weights[number, slot, rows] * value[rows]
            same = term if same is None else same + term
        for dx, begin in ((1, 8), (-1, 13)):
            part = None
            for number, (dz, dy) in enumerate(TERMS_SIDE):
                value = near(dz, dy)
                if value is None:
                    continue
                term = weights[begin + number, slot] * value[...]
                part = term if part is None else part + term
            same = same + row_roll(part, -dx)[rows]
        value = basis[step - 1, slot, rows]
        fresh = jac[slot, rows] * same + spare[slot, rows] * value
        if first:
            factor = jnp.where(step == 1, 0.5, 1.0).astype(jnp.float32)
            back = jnp.where(step == 1, 0.0, 1.0).astype(jnp.float32)
            fresh = factor * fresh - back * basis[jnp.maximum(step - 2, 0), slot, rows]
        else:
            fresh = fresh - basis[step - 2, slot, rows]
        basis[step, slot, rows] = fresh
        return fresh, value

    def one_step(step, last, first=False, final=False):
        now = basis.at[step - 1]
        for j in range(min(last + 1, planes)):
            slot = at(j)
            found = sides(now[slot], now[planes + slot // nz], slot % nz)
            moved[0, slot], moved[1, slot] = found
        if not final:
            triples = []
            for q in range(2):
                strip = now[planes + q]
                mixed = strip
                for g in range(nz):
                    slot = q * nz + g
                    j = slot if q == 0 else 3 * nz - 1 - slot
                    if j <= last:
                        mixed = jnp.where(
                            group_of == g, lane_roll(now[slot], GROUP * g + 8), mixed
                        )
                after = lane_roll(jnp.where(inner_held == 8, mixed, strip), -1)
                before = lane_roll(jnp.where(inner_held == 7, mixed, strip), 1)
                moved[0, planes + q], moved[1, planes + q] = after, before
                triples.append((strip, after, before))
            for number in range(3):
                found = across(triples[0][number], triples[1][number])
                for which, value in enumerate(found):
                    beside[which, number] = value
            for q in range(2):
                slot = planes + q

                def near(dz, dy):
                    number = {0: 0, 1: 1, -1: 2}[dy]
                    if dz:
                        return beside.at[q if dz == 1 else 2 + q, number]
                    return now.at[slot] if dy == 0 else moved.at[number - 1, slot]

                advance(step, slot, near, slice(0, held), first)
        sums = [zero8, zero8, zero8]
        for j in range(last):
            slot = at(j)

            def near(dz, dy):
                if j + dz < 0:
                    return None
                spot = at(j + dz)
                return now.at[spot] if dy == 0 else moved.at[0 if dy == 1 else 1, spot]

            rows = own if final else slice(0, held)
            fresh, value = advance(step, slot, near, rows, first)
            if j < nz:
                if not final:
                    fresh, value = fresh[own], value[own]
                weighted = fresh * scale[slot]
                sums[0] = sums[0] + folded(weighted * fresh)
                sums[1] = sums[1] + folded(weighted * value)
                sums[2] = sums[2] + folded(fresh)
        record(step, sums)

    def early_steps(step, carry):
        one_step(step, planes - 1, first=True)
        return carry

    def later_steps(step, carry):
        one_step(step, planes - 4)
        return carry

    lax.fori_loop(1, 4, early_steps, 0)
    lax.fori_loop(4, ITERS, later_steps, 0)
    one_step(ITERS, nz, final=True)
    partial = jnp.sum(jnp.sum(dots[...], axis=1), axis=1, keepdims=True)
    entry = lax.broadcasted_iota(jnp.int32, (3 * (ITERS + 1), ny), 0)
    kind, index = entry // (ITERS + 1), entry % (ITERS + 1)
    place_of = jnp.where(kind == 0, 2 * index, jnp.where(kind == 1, 2 * index - 1, 2 * ITERS + 1 + index))
    wanted = place_of == lax.broadcasted_iota(jnp.int32, entry.shape, 1)
    final_row[...] = jnp.sum(jnp.where(wanted, partial, 0.0), axis=0, keepdims=True)
    spread(2, final_row, final_all, everyone)
    for group in moves:
        for _, sends, copy in group:
            pl.when(sends)(copy.wait_send)
    for group in relays:
        for copy in group:
            copy.wait_send()
    sums = collect(2, final_row, final_all, everyone)

    mu = [pick(sums, n) for n in range(2 * ITERS)]
    ones = [pick(sums, 2 * ITERS + 1 + n) for n in range(ITERS)]
    for n in range(2, 2 * ITERS):
        mu[n] = 2.0 * mu[n] - mu[n % 2]
    one = jnp.ones((1, 1), jnp.float32)
    y, p = [one], [one]
    m_y, m_p = list(mu), list(mu)
    x = []
    rz = mu[0]

    def plus(first, second):
        if first is None or second is None:
            return second if first is None else first
        return first + second

    def get(values, n):
        return values[n] if 0 <= n < len(values) else None

    for step in range(ITERS):
        h_p = []
        for n in range(step + 2):
            right = get(p, n - 1)
            if n == 1:
                right = right + right
            around_n = plus(get(p, n + 1), right)
            here = get(p, n)
            drop = None if around_n is None else -0.5 * around_n
            h_p.append(plus(here, drop))
        m_h = [m_p[0] - m_p[1]]
        for n in range(1, 2 * ITERS - 1 - step):
            m_h.append(m_p[n] - 0.5 * (m_p[n + 1] + m_p[n - 1]))
        bottom = p[0] * m_h[0]
        for n in range(1, step + 1):
            bottom = bottom + p[n] * m_h[n]
        alpha = rz / bottom
        x = [plus(get(x, n), alpha * p[n]) for n in range(step + 1)]
        y = [plus(get(y, n), -(alpha * h_p[n])) for n in range(step + 2)]
        if step + 1 < ITERS:
            m_y = [m_y[n] - alpha * m_h[n] for n in range(len(m_h))]
            rz_next = y[0] * m_y[0]
            for n in range(1, step + 2):
                rz_next = rz_next + y[n] * m_y[n]
            beta = rz_next / rz
            p = [plus(y[n], None if n > step else beta * p[n]) for n in range(step + 2)]
            m_p = [m_y[n] + beta * m_p[n] for n in range(len(m_y))]
            rz = rz_next
    mean = x[0] * ones[0]
    for n in range(1, ITERS):
        mean = mean + x[n] * ones[n]
    mean = mean / count
    xs = [jnp.broadcast_to(value, (8, ny)) for value in x]
    ys = [jnp.broadcast_to(value, (8, ny)) for value in y]
    mean = jnp.broadcast_to(mean, (8, ny))
    for slot in range(nz):
        target = flip(slot, side)
        for row in range(0, nx, 8):
            spot = slice(8 + row, 16 + row)
            weight = scale[slot, row : row + 8]
            total = jnp.where(weight > 0.0, -mean, 0.0)
            rest = ys[ITERS] * basis[ITERS, slot, spot]
            for n in range(ITERS):
                value = basis[n, slot, spot]
                total = total + xs[n] * value
                rest = rest + ys[n] * value
            phi[target, row : row + 8] = total
            residual[target, row : row + 8] = weight * rest


def fast_body(potential, tissue_mask, layer_index, source):
    extent = tissue_mask.shape
    nz, nx, ny = extent
    sizes = tuple(lax.axis_size(axis) for axis in AXES)
    planes, held, deep = 2 * nz, nx + 16, nx + 32
    peers = math.prod(sizes)
    vmem = pl.BlockSpec(memory_space=pltpu.VMEM)
    hbm = pl.BlockSpec(memory_space=pltpu.HBM)

    def real(*shape):
        return pltpu.VMEM(shape + (ny,), jnp.float32)

    moves = 40
    inputs = (potential, tissue_mask, layer_index, source)
    scratch = [
        real(3, planes, held), pltpu.VMEM(extent, jnp.int32), real(5, nx), real(2, 2, nz),
        real(2, 2, 2, nz), real(5, deep), real(5, deep), real(5, 2, deep),
        real(9, planes + 6, deep), real(18, planes + 2, held), real(ITERS + 1, planes + 2, held),
        real(2, planes + 2, held), real(4, 3, held), real(planes + 2, held),
        real(planes + 2, held), real(nz, nx), real(2, COEFS, 8), real(3 * (ITERS + 1), 8),
        real(1), real(sizes[1] * sizes[2], 1), real(1), real(sizes[0], 1), real(1), real(peers, 1),
        pltpu.SMEM((LAYERS, 18), jnp.float32), pltpu.SMEM((planes, COEFS), jnp.float32),
        pltpu.SMEM((nz,), jnp.int32), pltpu.SMEM((nz,), jnp.int32), pltpu.SMEM((planes,), jnp.int32),
        pltpu.SemaphoreType.DMA((4,)), pltpu.SemaphoreType.DMA((moves,)),
        pltpu.SemaphoreType.DMA((moves,)), pltpu.SemaphoreType.DMA((3,)),
        pltpu.SemaphoreType.DMA((3,)),
    ]
    return tuple(
        pl.pallas_call(
            functools.partial(fast_kernel, extent, sizes),
            out_shape=(jax.ShapeDtypeStruct(extent, jnp.float32),) * 2,
            in_specs=[hbm] * 4,
            out_specs=(vmem, vmem),
            scratch_shapes=scratch,
            compiler_params=pltpu.CompilerParams(
                vmem_limit_bytes=32 * 1024 * 1024, collective_id=0, has_side_effects=True
            ),
        )(*(pltpu.with_memory_space_constraint(ref, pltpu.HBM) for ref in inputs))
    )


def body(potential, tissue_mask, layer_index, source):
    nz, nx, ny = tissue_mask.shape
    fits = (
        lax.axis_size("gz") == 2 and nz == 8 and ITERS == 8 and nx % 8 == 0 and nx >= 16
        and ny == nz * GROUP and lax.axis_size("gx") > 1 and lax.axis_size("gy") > 1
    )
    return (fast_body if fits else general_body)(potential, tissue_mask, layer_index, source)


def solution(mesh):
    placed = (P("gz", "gx", "gy"), P("gz", "gx", "gy"), P("gz"), P("gz", "gx", "gy"))
    return jax.shard_map(
        body,
        mesh=mesh,
        in_specs=placed,
        out_specs=(P("gz", "gx", "gy"), P("gz", "gx", "gy")),
        check_vma=False,
    )
```

```python
import functools
import math

import jax
import jax.numpy as jnp
from jax import lax
from jax.experimental import pallas as pl
from jax.experimental.pallas import tpu as pltpu
from jax.sharding import PartitionSpec as P
import numpy as np

ITERS = 8
DEPTH = ITERS + 1
LAYERS = 16
AXES = ("gx", "gy", "gz")

OFFSETS = [
    (0, 1, 0),
    (0, 0, 1),
    (1, 0, 0),
    (0, 1, 1),
    (0, 1, -1),
    (1, 1, 0),
    (-1, 1, 0),
    (1, 0, 1),
    (-1, 0, 1),
]
bulk_long = 7.99
bulk_trans = 2.55
intra_long = 1.74
intra_trans = 0.19
bath_sigma = 5.0


def tensor_table(layers, longitudinal, transverse):
    depth = jnp.arange(layers, dtype=jnp.float32) / (layers - 1)
    helix = math.pi / 3.0 * (1.0 - 2.0 * depth)
    tilted = 0.35 * jnp.cos(math.pi * depth)
    fiber_x = jnp.cos(tilted) * jnp.cos(helix)
    fiber_y = jnp.cos(tilted) * jnp.sin(helix)
    fiber_z = jnp.sin(tilted)
    spread = longitudinal - transverse
    s_xx = transverse + spread * fiber_x * fiber_x
    s_yy = transverse + spread * fiber_y * fiber_y
    s_zz = transverse + spread * fiber_z * fiber_z
    s_xy = spread * fiber_x * fiber_y
    s_xz = spread * fiber_x * fiber_z
    s_yz = spread * fiber_y * fiber_z
    columns = [
        s_xx - jnp.abs(s_xy) - jnp.abs(s_xz),
        s_yy - jnp.abs(s_xy) - jnp.abs(s_yz),
        s_zz - jnp.abs(s_xz) - jnp.abs(s_yz),
        jnp.maximum(s_xy, 0.0),
        jnp.maximum(-s_xy, 0.0),
        jnp.maximum(s_xz, 0.0),
        jnp.maximum(-s_xz, 0.0),
        jnp.maximum(s_yz, 0.0),
        jnp.maximum(-s_yz, 0.0),
    ]
    return jnp.stack(columns, axis=1)


def shifted(value, axis, hop):
    count = lax.axis_size(axis)
    pairs = [(i + hop, i) for i in range(count) if 0 <= i + hop < count]
    return lax.ppermute(value, axis, pairs)


def framed(value, axis, dim, multiple):
    count, length = lax.axis_size(axis), value.shape[dim]
    if count == 1:
        return value
    if count == 2 and 2 * length <= length + 2 * DEPTH and multiple == 1:
        other = lax.ppermute(value, axis, [(0, 1), (1, 0)])
        return jnp.concatenate([value, other], axis=dim)
    after, before = [], []
    left, hop = DEPTH, 1
    while left > 0:
        width = min(left, length)
        if hop < count:
            after.append(
                shifted(lax.slice_in_dim(value, 0, width, axis=dim), axis, hop)
            )
            before.insert(
                0, shifted(lax.slice_in_dim(value, length - width, length, axis=dim), axis, -hop)
            )
        else:
            shape = list(value.shape)
            shape[dim] = width
            after.append(jnp.zeros(shape, value.dtype))
            before.insert(0, jnp.zeros(shape, value.dtype))
        left, hop = left - width, hop + 1
    gap = -(length + 2 * DEPTH) % multiple
    shape = list(value.shape)
    shape[dim] = gap
    middle = [jnp.zeros(shape, value.dtype)] if gap else []
    return jnp.concatenate([value] + after + middle + before, axis=dim)


def fields_around(ref, here, above, below, rows, lanes):
    def along_x(value, step):
        return pltpu.roll(value, (-step) % rows, 0)

    def along_y(value, step):
        return pltpu.roll(value, (-step) % lanes, 1)

    for dz, plane in ((0, here), (1, above), (-1, below)):
        value = ref[plane]
        if dz:
            yield (dz, 0, 0), value
        for step in (1, -1):
            yield (dz, step, 0), along_x(value, step)
        for step in (1, -1):
            moved = along_y(value, step)
            yield (dz, 0, step), moved
            if dz == 0:
                for other in (1, -1):
                    yield (0, other, step), along_x(moved, other)


SLOT = {}
for _column, _offset in enumerate(OFFSETS):
    SLOT[_offset] = (_column, 2 * _column)
    SLOT[tuple(-o for o in _offset)] = (_column, 2 * _column + 1)


def grid_kernel(extent, sizes, table, mask_in, potential_in, source_in, phi, residual,
                basis, scale, dots, weights, spare, first, second, jac,
                own_row, early, final_row, late, sends, early_recv, late_recv):
    mask, potential, source = mask_in, potential_in, source_in
    planes, rows, lanes = mask.shape
    nz, nx, ny = extent
    held = jac.shape[1]
    keep = nx + ITERS
    peers = math.prod(sizes)
    me = 0
    for axis, size in zip(AXES, sizes):
        me = me * size + lax.axis_index(axis)

    def device(index):
        return (index // (sizes[1] * sizes[2]), index // sizes[2] % sizes[1], index % sizes[2])

    def peer(k):
        return lax.rem(me + k, peers)

    barrier = pltpu.get_barrier_semaphore()

    def greet(k, carry):
        pl.semaphore_signal(
            barrier, inc=1, device_id=device(peer(k)), device_id_type=pl.DeviceIdType.MESH
        )
        return carry

    lax.fori_loop(1, peers, greet, 0)

    def spread(row, gathered, recv):
        def one(k, carry):
            pltpu.make_async_remote_copy(
                src_ref=row, dst_ref=gathered.at[me], send_sem=sends.at[k],
                recv_sem=recv.at[me], device_id=device(peer(k)),
                device_id_type=pl.DeviceIdType.MESH,
            ).start()
            return carry

        lax.fori_loop(1, peers, one, 0)

    def collect(row, gathered, recv):
        def one(k, carry):
            other = peer(k)
            copy = pltpu.make_async_remote_copy(
                src_ref=row, dst_ref=gathered.at[other], send_sem=sends.at[k],
                recv_sem=recv.at[other], device_id=device(other),
                device_id_type=pl.DeviceIdType.MESH,
            )
            copy.wait_recv()
            copy.wait_send()
            return carry

        lax.fori_loop(1, peers, one, 0)
        gathered[me] = row[...]
        return jnp.sum(gathered[...], axis=0)

    lane = lax.broadcasted_iota(jnp.int32, (1, 128), 1)

    def pick(vector, index):
        return jnp.sum(jnp.where(lane == index, vector, 0.0), axis=1, keepdims=True)

    cells = jnp.zeros((1, ny), jnp.float32)
    injected = jnp.zeros((1, ny), jnp.float32)
    for plane in range(nz):
        own_inside = jnp.where(mask_in[plane, 0:nx, 0:ny] > 0.0, 1.0, 0.0)
        cells = cells + jnp.sum(own_inside, axis=0, keepdims=True)
        injected = injected + jnp.sum(
            own_inside * source_in[plane, 0:nx, 0:ny], axis=0, keepdims=True
        )
    cells = jnp.sum(cells, axis=1, keepdims=True)
    injected = jnp.sum(injected, axis=1, keepdims=True)
    own_row[...] = jnp.where(lane == 0, cells, jnp.where(lane == 1, injected, 0.0))

    def neighbours(plane):
        above = jnp.where(plane + 1 == planes, 0, plane + 1)
        below = jnp.where(plane == 0, planes - 1, plane - 1)
        return above, below

    def store(ref, index, value):
        if held == rows:
            ref[index] = value
        else:
            ref[(*index, slice(0, keep))] = value[:keep]
            ref[(*index, slice(keep, held))] = value[rows - held + keep :]

    def setup(plane, carry):
        above, below = neighbours(plane)
        labels = mask[plane]
        tissue = jnp.where(labels == 2.0, 1.0, 0.0)
        bath = jnp.where(labels == 1.0, 1.0, 0.0)
        inside = tissue + bath
        volts = potential[plane]
        total = jnp.zeros((rows, lanes), jnp.float32)
        image = jnp.zeros((rows, lanes), jnp.float32)
        pairs = zip(
            fields_around(mask, plane, above, below, rows, lanes),
            fields_around(potential, plane, above, below, rows, lanes),
        )
        for (offset, label), (_, volt) in pairs:
            column, slot = SLOT[offset]
            beyond = {0: plane, 1: above, -1: below}[offset[0]]
            link = 0.5
            if offset[0] == 1:
                link = 0.5 * table[plane, 18]
            if offset[0] == -1:
                link = 0.5 * table[below, 18]
            their_tissue = jnp.where(label == 2.0, 1.0, 0.0)
            g_here, g_there = table[plane, column] * link, table[beyond, column] * link
            weight = tissue * g_here
            if column < 3:
                their_bath = jnp.where(label == 1.0, 1.0, 0.0)
                sigma = bath_sigma * link
                weight = inside * (
                    jnp.where(label > 0.0, weight + bath * sigma, 0.0)
                    + (their_tissue * g_there + their_bath * sigma)
                )
            else:
                weight = inside * (jnp.where(label > 0.0, weight, 0.0) + their_tissue * g_there)
            store(weights, (slot, plane), weight)
            total = total + weight
            intra = (table[plane, 9 + column] + table[beyond, 9 + column]) * link
            image = image + (tissue * their_tissue * intra) * (volts - volt)
        bounded = jnp.maximum(total, 1.0)
        jacobi = inside / bounded
        store(jac, (plane,), jacobi + jacobi)
        store(spare, (plane,), inside * (1.0 - jacobi * total))
        store(first, (plane,), jacobi * (inside * source[plane] - image))

        @pl.when(plane < nz)
        def _():
            scale[plane] = (inside * bounded)[:nx, :ny]

        return carry

    lax.fori_loop(0, planes // 2, setup, 0)
    pl.semaphore_wait(barrier, peers - 1)
    spread(own_row, early, early_recv)
    lax.fori_loop(planes // 2, planes, setup, 0)
    totals = collect(own_row, early, early_recv)
    count = pick(totals, 0)
    mean_rhs = pick(totals, 1) / count

    def centre(plane, carry):
        first[plane] = first[plane] - 0.5 * jac[plane] * mean_rhs
        return carry

    lax.fori_loop(0, planes, centre, 0)

    def record(step, now, before):
        rowsum = jnp.zeros((1, ny), jnp.float32)
        square, cross, plain = rowsum, rowsum, rowsum
        for plane in range(nz):
            value = now[plane, 0:nx, 0:ny]
            basis[step, plane] = value
            weighted = value * scale[plane]
            square = square + jnp.sum(weighted * value, axis=0, keepdims=True)
            if step:
                past = basis[step - 1, plane]
                cross = cross + jnp.sum(weighted * past, axis=0, keepdims=True)
            plain = plain + jnp.sum(value, axis=0, keepdims=True)
        if step < ITERS:
            dots[pl.ds(2 * step, 1)] = square
            dots[pl.ds(2 * ITERS + step, 1)] = plain
        if step:
            dots[pl.ds(2 * step - 1, 1)] = cross

    record(0, first, None)

    def apply(now, old, step):
        reach = ITERS - step
        if planes == nz:
            begin, span = 0, nz
        elif planes == sizes[2] * nz:
            begin = planes - lax.axis_index("gz") * reach
            span = min(planes, nz + reach)
        else:
            begin, span = planes - reach, nz + 2 * reach

        def one(index, carry):
            plane = lax.rem(begin + index, planes)
            above, below = neighbours(plane)
            total = jnp.zeros((held, lanes), jnp.float32)
            for offset, value in fields_around(now, plane, above, below, held, lanes):
                total = total + weights[SLOT[offset][1], plane] * value
            if step == 1:
                old[plane] = 0.5 * jac[plane] * total + spare[plane] * now[plane]
            else:
                old[plane] = (
                    jac[plane] * total + 2.0 * spare[plane] * now[plane] - old[plane]
                )
            return carry

        lax.fori_loop(0, span, one, 0)

    now, old = first, second
    for step in range(1, ITERS + 1):
        apply(now, old, step)
        now, old = old, now
        record(step, now, old)

    partial = jnp.sum(dots[...], axis=1, keepdims=True)
    diagonal = lax.broadcasted_iota(jnp.int32, (3 * ITERS, 128), 0) == lax.broadcasted_iota(
        jnp.int32, (3 * ITERS, 128), 1
    )
    final_row[...] = jnp.sum(jnp.where(diagonal, partial, 0.0), axis=0, keepdims=True)
    spread(final_row, late, late_recv)
    sums = collect(final_row, late, late_recv)

    def left(vector):
        return pltpu.roll(vector, 127, 1)

    def right(vector):
        return pltpu.roll(vector, 1, 1)

    mu0, mu1 = pick(sums, 0), pick(sums, 1)
    mu = jnp.where(lane < 2, sums, 2.0 * sums - jnp.where(lane % 2 == 0, mu0, mu1))
    mu = jnp.where(lane < 2 * ITERS, mu, 0.0)
    ones = pltpu.roll(sums, 128 - 2 * ITERS, 1)
    y = jnp.where(lane == 0, 1.0, 0.0)
    p = y
    m_y, m_p = mu, mu
    x = jnp.zeros((1, 128), jnp.float32)
    rz = mu0
    for step in range(ITERS):
        h_p = p - 0.5 * (left(p) + jnp.where(lane == 1, 2.0, 1.0) * right(p))
        h_p = jnp.where(lane <= ITERS, h_p, 0.0)
        before = jnp.where(lane == 0, left(m_p), right(m_p))
        m_h = m_p - 0.5 * (left(m_p) + before)
        alpha = rz / jnp.sum(jnp.where(lane < ITERS, p * m_h, 0.0), axis=1, keepdims=True)
        x = x + alpha * p
        y = y - alpha * h_p
        m_y = m_y - alpha * m_h
        if step + 1 < ITERS:
            rz_next = jnp.sum(jnp.where(lane < ITERS, y * m_y, 0.0), axis=1, keepdims=True)
            beta = rz_next / rz
            p = y + beta * p
            m_p = m_y + beta * m_p
            rz = rz_next
    mean = jnp.sum(jnp.where(lane < ITERS, x * ones, 0.0), axis=1, keepdims=True) / count
    xs = [pick(x, j) for j in range(ITERS)]
    ys = [pick(y, j) for j in range(ITERS + 1)]

    def one(plane, carry):
        weight = scale[plane]
        total = jnp.where(weight > 0.0, -mean, 0.0)
        rest = ys[ITERS] * basis[ITERS, plane]
        for j in range(ITERS):
            value = basis[j, plane]
            total = total + xs[j] * value
            rest = rest + ys[j] * value
        phi[plane] = total
        residual[plane] = weight * rest
        return carry

    lax.fori_loop(0, nz, one, 0)


def general_body(potential, tissue_mask, layer_index, source):
    extent = tissue_mask.shape
    nz = extent[0]
    labels = tissue_mask.astype(jnp.float32)
    sizes = tuple(lax.axis_size(axis) for axis in AXES)
    packed = jnp.stack([labels, potential, source], axis=1)
    packed = framed(packed, "gz", 0, 1)
    packed = framed(packed, "gx", 2, 8)
    packed = framed(packed, "gy", 3, 128)
    operands = (packed[:, 0], packed[:, 1], packed[:, 2])
    frame = operands[0].shape
    layers = framed(layer_index, "gz", 0, 1)
    planes = layers.shape[0]
    selector = (layers[:, None] == jnp.arange(LAYERS, dtype=jnp.int32)[None, :]).astype(
        jnp.float32
    )
    tables = jnp.concatenate(
        [
            tensor_table(LAYERS, bulk_long, bulk_trans),
            tensor_table(LAYERS, intra_long, intra_trans),
        ],
        axis=1,
    )
    table = jnp.dot(selector, tables, precision=lax.Precision.HIGHEST)
    size = lax.axis_size("gz")
    link = jnp.ones((planes, 1), jnp.float32)
    if planes == size * nz:
        place = (lax.axis_index("gz") * nz + jnp.arange(planes)) % planes
        link = (place + 1 < planes).astype(jnp.float32)[:, None]
    table = jnp.concatenate([table, link], axis=1)
    smem = pl.BlockSpec(memory_space=pltpu.SMEM)
    vmem = pl.BlockSpec(memory_space=pltpu.VMEM)
    compact = frame
    if extent[1] % 8 == 0 and ITERS % 8 == 0 and frame[1] > extent[1] + 2 * ITERS:
        compact = (planes, extent[1] + 2 * ITERS, frame[2])
    peers = math.prod(sizes)
    row = pltpu.VMEM((1, 128), jnp.float32)
    gathered = pltpu.VMEM((peers, 1, 128), jnp.float32)
    return tuple(
        pl.pallas_call(
            functools.partial(grid_kernel, extent, sizes),
            out_shape=(jax.ShapeDtypeStruct(extent, jnp.float32),) * 2,
            in_specs=[smem, vmem, vmem, vmem],
            out_specs=(vmem, vmem),
            scratch_shapes=[
                pltpu.VMEM((ITERS + 1,) + extent, jnp.float32),
                pltpu.VMEM(extent, jnp.float32),
                pltpu.VMEM((3 * ITERS, extent[2]), jnp.float32),
                pltpu.VMEM((18,) + compact, jnp.float32),
            ]
            + [pltpu.VMEM(compact, jnp.float32)] * 4
            + [row, gathered, row, gathered]
            + [pltpu.SemaphoreType.DMA((peers,))] * 3,
            compiler_params=pltpu.CompilerParams(
                vmem_limit_bytes=60 * 1024 * 1024, collective_id=0, has_side_effects=True
            ),
        )(table, *operands)
    )


GROUP = 16
TERMS_SAME = [(0, 1), (0, -1), (1, 0), (-1, 0), (1, 1), (1, -1), (-1, 1), (-1, -1)]
TERMS_SIDE = [(0, 0), (0, 1), (0, -1), (1, 0), (-1, 0)]
LEVEL = [0, 1, 3, 4]
STEEP = [(0, 0), (1, 0), (-1, 0), (0, 1), (0, -1)]
UPWARD = 2 * len(LEVEL)
COEFS = UPWARD + 1 + 3 * len(STEEP)


def numpy_table(longitudinal, transverse):
    depth = np.arange(LAYERS, dtype=np.float64) / (LAYERS - 1)
    helix = math.pi / 3.0 * (1.0 - 2.0 * depth)
    tilted = 0.35 * np.cos(math.pi * depth)
    fiber = (np.cos(tilted) * np.cos(helix), np.cos(tilted) * np.sin(helix), np.sin(tilted))
    spread = longitudinal - transverse
    s_xx, s_yy, s_zz = (transverse + spread * f * f for f in fiber)
    s_xy = spread * fiber[0] * fiber[1]
    s_xz = spread * fiber[0] * fiber[2]
    s_yz = spread * fiber[1] * fiber[2]
    columns = [s_xx - abs(s_xy) - abs(s_xz), s_yy - abs(s_xy) - abs(s_yz), s_zz - abs(s_xz) - abs(s_yz)]
    for value in (s_xy, s_xz, s_yz):
        columns += [np.maximum(value, 0.0), np.maximum(-value, 0.0)]
    return np.stack(columns, axis=1)


HALF_TABLE = 0.5 * np.concatenate(
    [numpy_table(bulk_long, bulk_trans), numpy_table(intra_long, intra_trans)], axis=1
)


def lane_roll(value, step):
    return pltpu.roll(value, step % value.shape[1], 1)


def row_roll(value, step):
    return pltpu.roll(value, step % value.shape[0], 0)


def tiled(value, rows):
    return jnp.concatenate([value] * (rows // value.shape[0]), axis=0)


def column_of(dz, dx, dy, side):
    same, flipped = SLOT[(dz, dx, dy)][0], SLOT[(-dz, dx, dy)][0]
    return same if same == flipped else same + side * (flipped - same)


def fast_kernel(extent, sizes, potential_in, mask_in, layers_in, source_in, phi, residual,
                fields, labels, packs, edge_send, edge_recv, from_after, from_before, strips,
                derived, weights, basis, moved, beside, jac, spare, scale, coef_lanes, dots,
                early_row, early_all, line_row, line_all, final_row, final_all,
                table, coefs, layers_own, layers_far, layers,
                loads, halo_send, halo_recv, sum_send, sum_recv):
    nz, nx, ny = extent
    planes, held, deep = 2 * nz, nx + 16, nx + 32
    own = slice(8, 8 + nx)
    place = tuple(lax.axis_index(axis) for axis in AXES)
    gx, gy, side = place
    first_x, last_x = gx == 0, gx == sizes[0] - 1
    first_y, last_y = gy == 0, gy == sizes[1] - 1

    def exists(dx, dy):
        return (gx + dx >= 0) & (gx + dx < sizes[0]) & (gy + dy >= 0) & (gy + dy < sizes[1])

    def around(a, b, c):
        return tuple(
            lax.rem(here + step, size) if step else here
            for here, step, size in zip(place, (a, b, c), sizes)
        )

    slab = [(0, b, c) for b in range(sizes[1]) for c in range(sizes[2])]
    line = [(a, 0, 0) for a in range(sizes[0])]
    everyone = [(a, b, c) for a, _, _ in line for _, b, c in slab]
    corners = [(dx, dy) for dx in (1, -1) for dy in (1, -1)]

    def flip(slot, turned):
        return slot + turned * (nz - 1 - 2 * slot)

    get_layers = pltpu.make_async_copy(layers_in, layers_own, loads.at[0])
    get_mask = pltpu.make_async_copy(mask_in, labels, loads.at[1])
    get_layers.start()
    get_mask.start()
    whole = []
    for index, ref in ((1, potential_in), (2, source_in)):
        for plane in range(nz):
            pltpu.make_async_copy(
                ref.at[plane], fields.at[index, flip(plane, side), own], loads.at[1 + index]
            ).start()
        whole.append(pltpu.make_async_copy(ref, fields.at[index, 0:nz, own], loads.at[1 + index]))

    barrier = pltpu.get_barrier_semaphore()

    def greet(target):
        pl.semaphore_signal(
            barrier, inc=1, device_id=target, device_id_type=pl.DeviceIdType.MESH
        )

    expected = len(slab) + len(line) - 2
    for step in slab[1:] + line[1:]:
        greet(around(*step))
    for dx, dy in corners:
        pl.when(exists(dx, dy))(lambda: greet((gx + dx, gy + dy, side)))
        expected = expected + jnp.where(exists(dx, dy), 1, 0)

    def clear(when, ref, index):
        @pl.when(when)
        def _():
            ref[index] = jnp.zeros(ref.at[index].shape, jnp.float32)

    every = slice(None)
    clear(first_x, fields, (every, slice(0, nz), slice(0, 8)))
    clear(last_x, fields, (every, slice(0, nz), slice(8 + nx, held)))
    for index in range(2):
        clear(first_x, edge_recv, (0, index, 0))
        clear(last_x, edge_recv, (0, index, 1))
    for ref, edge in ((from_after, last_y), (from_before, first_y)):
        clear(edge, ref, (every,))
        clear(first_x, ref, (every, slice(0, 16)))
        clear(last_x, ref, (every, slice(16 + nx, deep)))
    def lanes_of(rows):
        lane = lax.broadcasted_iota(jnp.int32, (rows, ny), 1)
        return lane, lane // GROUP, lane % GROUP

    lane = lax.broadcasted_iota(jnp.int32, (1, ny), 1)

    def pick(vector, index):
        return jnp.sum(jnp.where(lane == index, vector, 0.0), axis=1, keepdims=True)

    own_lane, _, _ = lanes_of(nx)
    later = (own_lane + 1) % ny // GROUP
    sooner = (own_lane + ny - 1) % ny // GROUP

    def pack(index):
        values = [fields[index, slot, own] for slot in range(nz)]
        turned = [lane_roll(value, GROUP * slot + 8) for slot, value in enumerate(values)]
        for toward, owner in ((0, later), (1, sooner)):
            total = turned[0]
            for slot in range(1, nz):
                total = jnp.where(owner == slot, turned[slot], total)
            packs[index, toward] = total
        if index < 2:
            for slot in range(nz):
                edge_send[index, 0, slot : slot + 1] = values[slot][8:9]
                edge_send[index, 1, slot : slot + 1] = values[slot][nx - 9 : nx - 8]

    def spread(number, row, gathered, targets):
        for index, step in enumerate(targets):
            if index:
                pltpu.make_async_remote_copy(
                    src_ref=row, dst_ref=gathered.at[index], send_sem=sum_send.at[number],
                    recv_sem=sum_recv.at[number], device_id=around(*step),
                    device_id_type=pl.DeviceIdType.MESH,
                ).start()

    def collect(number, row, gathered, targets):
        arrived = gathered.at[pl.ds(1, len(targets) - 1)]
        pltpu.make_async_copy(arrived, arrived, sum_recv.at[number]).wait()
        pltpu.make_async_copy(arrived, arrived, sum_send.at[number]).wait()
        gathered[0] = row[...]
        return jnp.sum(gathered[...], axis=0)

    def link(number, src, dst, target):
        return pltpu.make_async_remote_copy(
            src_ref=src, dst_ref=dst, send_sem=halo_send.at[number],
            recv_sem=halo_recv.at[number], device_id=target,
            device_id_type=pl.DeviceIdType.MESH,
        )

    other = (gx, gy, 1 - side)
    numbers = iter(range(64))

    def swap(src, dst):
        copy = link(next(numbers), src, dst, other)
        copy.start()
        return copy

    def exchange(picked, rows, edge):
        found = []

        def move(dx, dy, src, dst):
            copy = link(next(numbers), src, dst, (gx + dx, gy + dy, side))
            pl.when(exists(dx, dy))(copy.start)
            found.append((exists(-dx, -dy), exists(dx, dy), copy))

        for dx, dy in corners:
            into, toward = (from_before, 0) if dy == 1 else (from_after, 1)
            if dx == 1:
                move(dx, dy, packs.at[rows, toward, nx - 16 : nx], into.at[rows, 0:16])
            else:
                move(dx, dy, packs.at[rows, toward, 0:16], into.at[rows, 16 + nx : deep])
        move(0, 1, packs.at[rows, 0], from_before.at[rows, 16 : 16 + nx])
        move(0, -1, packs.at[rows, 1], from_after.at[rows, 16 : 16 + nx])
        move(1, 0, edge_send.at[edge, 1], edge_recv.at[0, edge, 0])
        move(-1, 0, edge_send.at[edge, 0], edge_recv.at[0, edge, 1])
        move(1, 0, fields.at[rows, 0:nz, nx : nx + 8], fields.at[rows, 0:nz, 0:8])
        move(-1, 0, fields.at[rows, 0:nz, 8:16], fields.at[rows, 0:nz, 8 + nx : held])
        return found

    groups = [(slice(0, 2), slice(0, 1), 0), (slice(2, 5), slice(1, 3), 1)]
    moves, relays = [], []

    def launch(picked, rows, edge):
        moves.append(exchange(picked, rows, edge))
        relays.append([swap(fields.at[rows, 0:nz, own], fields.at[rows, nz:planes, own])])

    def relay(picked, rows, edge):
        for receives, _, copy in moves[edge]:
            pl.when(receives)(copy.wait_recv)
        for index in range(rows.start, rows.stop):
            below, above = from_before[index], from_after[index]
            strips[2 * index, 0] = jnp.where(inner_deep < 8, below, above)
            if index < 2:
                strips[2 * index + 1, 0] = jnp.where(
                    inner_deep == 15, lane_roll(above, -1), lane_roll(below, 1)
                )
        relays[edge] += [
            swap(strips.at[picked, 0], strips.at[picked, 1]),
            swap(edge_recv.at[0, edge], edge_recv.at[1, edge]),
            swap(fields.at[rows, 0:nz, 0:8], fields.at[rows, nz:planes, 0:8]),
            swap(fields.at[rows, 0:nz, 8 + nx : held], fields.at[rows, nz:planes, 8 + nx : held]),
        ]

    get_mask.wait()
    get_layers.wait()
    for plane in range(nz):
        fields[0, flip(plane, side), own] = labels[plane].astype(jnp.float32)
    pack(0)
    pl.semaphore_wait(barrier, expected)
    layer_swap = swap(layers_own, layers_far)
    launch(*groups[0])
    for copy in whole:
        copy.wait()
    cells = jnp.zeros((8, ny), jnp.float32)
    injected = cells
    for slot in range(nz):
        for row in range(8, 8 + nx, 8):
            inside = jnp.where(fields[0, slot, row : row + 8] > 0.0, 1.0, 0.0)
            cells = cells + inside
            injected = injected + inside * fields[2, slot, row : row + 8]
    cells = jnp.sum(jnp.sum(cells, axis=0, keepdims=True), axis=1, keepdims=True)
    injected = jnp.sum(jnp.sum(injected, axis=0, keepdims=True), axis=1, keepdims=True)
    early_row[...] = jnp.where(lane == 0, cells, jnp.where(lane == 1, injected, 0.0))

    spread(0, early_row, early_all, slab)
    pack(1)
    pack(2)

    for layer in range(LAYERS):
        for column in range(18):
            table[layer, column] = jnp.float32(HALF_TABLE[layer, column])

    layer_swap.wait()
    for slot in range(nz):
        layers[slot] = layers_own[flip(slot, side)]
        layers[nz + slot] = layers_far[flip(slot, 1 - side)]

    def slot_of(j):
        return jnp.where(j < nz, j, 3 * nz - 1 - j)

    def coefficients(pair, carry):
        for slot in (2 * pair, 2 * pair + 1):
            j = slot_of(slot)
            layer = layers[slot]
            for n, k in enumerate(LEVEL):
                coefs[slot, 2 * n] = table[layer, k]
                coefs[slot, 2 * n + 1] = 2.0 * table[layer, 9 + k]
            near = j + 1 < planes
            there = layers[slot_of(jnp.where(near, j + 1, j))]
            open_ = jnp.where(near, 1.0, 0.0).astype(jnp.float32)
            coefs[slot, UPWARD] = 0.5 * bath_sigma * open_
            for n, (dx, dy) in enumerate(STEEP):
                k = column_of(1, dx, dy, side)
                coefs[slot, UPWARD + 1 + 3 * n] = table[layer, k] * open_
                coefs[slot, UPWARD + 2 + 3 * n] = table[there, k] * open_
                coefs[slot, UPWARD + 3 + 3 * n] = (table[layer, 9 + k] + table[there, 9 + k]) * open_
        return carry

    launch(*groups[1])
    lax.fori_loop(0, nz, coefficients, 0)
    for n in range(COEFS):
        coefs[planes, n] = jnp.float32(0.0)
    _, group8, _ = lanes_of(8)

    def at(j):
        return j if j < nz else 3 * nz - 1 - j

    def widen(block, carry):
        for n in [8 * block + m for m in range(8)]:
            for q in range(2):
                for which, shift in enumerate((0, -1)):
                    value = None
                    for g in range(nz):
                        j = at(q * nz + g) + shift
                        entry = coefs[planes if j < 0 else at(j), n]
                        if value is None:
                            value = jnp.full((8, ny), entry, jnp.float32)
                        else:
                            value = jnp.where(group8 == g, entry, value)
                    coef_lanes[which, q, n] = value
        return carry

    lax.fori_loop(0, COEFS // 8, widen, 0)

    lane_of, group_of, inner_deep = lanes_of(deep)
    relay(*groups[0])
    def sides(value, strip, g):
        ring = lane_roll(strip, -(GROUP * g + 8))
        after = lane_roll(jnp.where(lane_of == 0, ring, value), -1)
        before = lane_roll(jnp.where(lane_of == ny - 1, ring, value), 1)
        return after, before

    def stored(index, number, slot, value):
        if index:
            derived[3 * number + 2, slot] = value
        else:
            derived[3 * number, slot] = jnp.where(value == 2.0, 1.0, 0.0)
            derived[3 * number + 1, slot] = jnp.where(value > 0.0, 1.0, 0.0)

    def framed_plane(index, q, g):
        before = jnp.broadcast_to(edge_recv[q, index, 0, g : g + 1], (8, ny))
        after = jnp.broadcast_to(edge_recv[q, index, 1, g : g + 1], (8, ny))
        return jnp.concatenate([before, fields[index, q * nz + g], after], axis=0)

    def derive(index, q):
        strip, edge = strips[2 * index, q], strips[2 * index + 1, q]
        mixed = strip
        for g in range(nz):
            value = framed_plane(index, q, g)
            mixed = jnp.where(group_of == g, lane_roll(value, GROUP * g + 8), mixed)
            for number, part in enumerate((value,) + sides(value, strip, g)):
                stored(index, number, q * nz + g, part)
        after = lane_roll(jnp.where(inner_deep == 8, mixed, strip), -1)
        before = lane_roll(jnp.where(inner_deep == 7, mixed, strip), 1)
        stored(index, 0, planes + q, strip)
        stored(index, 1, planes + q, jnp.where(inner_deep == 15, edge, after))
        stored(index, 2, planes + q, jnp.where(inner_deep == 0, edge, before))

    def derive_beside(index):
        for number in ((2, 5, 8) if index else (0, 1, 3, 4, 6, 7)):
            found = across(derived[number, planes], derived[number, planes + 1])
            for shift, value in enumerate(found):
                derived[number, planes + 2 + shift] = value

    def across(lower, upper):
        up0 = jnp.where(group_of == nz - 1, upper, lane_roll(lower, -GROUP))
        up1 = lane_roll(upper, GROUP)
        down0 = lane_roll(lower, GROUP)
        down1 = jnp.where(group_of == nz - 1, lower, lane_roll(upper, -GROUP))
        return up0, up1, down0, down1

    def level_of(coef):
        return {k: (coef(1, 2 * n), coef(1, 2 * n + 1)) for n, k in enumerate(LEVEL)}

    def steep_of(coef, dz):
        entries = {}
        for n, (dx, dy) in enumerate(STEEP):
            here, there, intra = (coef(dz, UPWARD + 1 + 3 * n + m) for m in range(3))
            if dz == 1:
                entries[(dx, dy)] = here, there, intra
            else:
                entries[(-dx, -dy)] = there, here, intra
        return coef(dz, UPWARD), entries

    middle = slice(8, 8 + held)

    def by(value, factor):
        if isinstance(factor, float) or factor.ndim == 0:
            return value * factor
        return value * tiled(factor, value.shape[0])

    def gathered_terms(edges, full):
        sums = edges(tuple(value[middle] for value in full), middle, 0, TERMS_SAME, 0)
        high = tuple(row_roll(value, 1)[8:deep] for value in full)
        part = edges(high, slice(8, deep), 1, TERMS_SIDE, 8)
        sums = sums + row_roll(part, -1)[0:held]
        low = tuple(row_roll(value, -1)[0 : 8 + held] for value in full)
        part = edges(low, slice(0, 8 + held), -1, TERMS_SIDE, 13)
        return sums + row_roll(part, 1)[middle]

    def weigh(slot, above, below, coef):
        level, slopes = level_of(coef), {1: steep_of(coef, 1), -1: steep_of(coef, -1)}
        base_bath = 0.5 * bath_sigma
        neighbour = {0: slot, 1: above, -1: below}

        def fetch(dz, dy, rows):
            number = {0: 0, 1: 1, -1: 2}[dy]
            return tuple(derived[3 * number + m, neighbour[dz], rows] for m in range(2))

        def edges(centre, rows, dx, terms, first):
            t, i = centre
            total = None
            keep = {0: slice(0, held), 1: slice(0, held), -1: slice(8, 8 + held)}[dx]
            for number, (dz, dy) in enumerate(terms):
                tn, i_n = fetch(dz, dy, rows)
                if dz == 0:
                    g_here = g_there = level[SLOT[(0, dx, dy)][0]][0]
                    bath = base_bath
                else:
                    bath, entries = slopes[dz]
                    g_here, g_there, _ = entries[(dx, dy)]
                if (dz != 0) + (dx != 0) + (dy != 0) == 1:
                    ours = by(t, g_here - bath) + by(i, bath)
                    theirs = by(tn, g_there - bath) + by(i_n, bath)
                else:
                    ours, theirs = by(t, g_here), by(tn, g_there)
                weight = i_n * ours + i * theirs
                weights[first + number, slot] = weight[keep]
                total = weight if total is None else total + weight
            return total

        full = fetch(0, 0, slice(0, deep))
        total = gathered_terms(edges, full)
        inside = full[1][middle]
        bounded = jnp.maximum(total, 1.0)
        jacobi = inside / bounded
        jac[slot] = jacobi + jacobi
        spare[slot] = 2.0 * (inside - inside * (jacobi * total))
        return (inside * bounded)[own]

    def begin(slot, above, below, coef, source):
        level, slopes = level_of(coef), {1: steep_of(coef, 1), -1: steep_of(coef, -1)}
        neighbour = {0: slot, 1: above, -1: below}

        def edges(centre, rows, dx, terms, first):
            v = centre[0]
            image = None
            for dz, dy in terms:
                number = {0: 0, 1: 1, -1: 2}[dy]
                tn = derived[3 * number, neighbour[dz], rows]
                vn = derived[3 * number + 2, neighbour[dz], rows]
                if dz == 0:
                    intra = level[SLOT[(0, dx, dy)][0]][1]
                else:
                    intra = slopes[dz][1][(dx, dy)][2]
                term = by(tn * (v - vn), intra)
                image = term if image is None else image + term
            return image

        image = gathered_terms(edges, (derived[2, slot],))
        tissue, inside = derived[0, slot, middle], derived[1, slot, middle]
        value = 0.5 * jac[slot] * (inside * (source - mean_rhs) - tissue * image)
        basis[0, slot] = value
        return value[own]

    def beyond(slot):
        j = slot_of(slot)
        return slot_of(jnp.minimum(j + 1, planes - 1)), slot_of(jnp.maximum(j - 1, 0))

    def from_table(slot):
        j = slot_of(slot)
        under = jnp.where(j == 0, planes, slot_of(j - 1))
        return lambda dz, n: coefs[slot if dz == 1 else under, n]

    def from_lanes(q):
        return lambda dz, n: coef_lanes[0 if dz == 1 else 1, q, n]

    def plane_weigh(slot, carry):
        scale[slot] = weigh(slot, *beyond(slot), from_table(slot))
        return carry

    def strip_weigh(q, carry):
        slot = planes + q
        weigh(slot, slot + 2, slot + 4, from_lanes(q))
        return carry

    def label_half(q, carry):
        @pl.when(q == 1)
        def _():
            for copy in relays[0]:
                copy.wait_recv()
            line_row[...] = collect(0, early_row, early_all, slab)
            spread(1, line_row, line_all, line)

        derive(0, q)
        lax.fori_loop(q * (nz - 1), nz - 1 + q, plane_weigh, 0)
        return carry

    lax.fori_loop(0, 2, label_half, 0)
    relay(*groups[1])
    lax.fori_loop(nz, planes, plane_weigh, 0)
    derive_beside(0)
    lax.fori_loop(0, 2, strip_weigh, 0)
    def volt_half(q, carry):
        @pl.when(q == 1)
        def _():
            for copy in relays[1]:
                copy.wait_recv()

        derive(1, q)
        return carry

    lax.fori_loop(0, 2, volt_half, 0)
    derive_beside(1)

    totals = collect(1, line_row, line_all, line)
    count = pick(totals, 0)
    mean_rhs = pick(totals, 1) / count

    def plane_begin(slot, carry):
        begin(slot, *beyond(slot), from_table(slot), fields[2, slot])
        return carry

    def strip_begin(q, carry):
        slot = planes + q
        begin(slot, slot + 2, slot + 4, from_lanes(q), strips[4, q, middle])
        return carry

    lax.fori_loop(0, planes, plane_begin, 0)
    lax.fori_loop(0, 2, strip_begin, 0)

    def folded(value):
        total = value[0:8]
        for row in range(8, value.shape[0], 8):
            total = total + value[row : row + 8]
        return total

    zero8 = jnp.zeros((8, ny), jnp.float32)

    def record(step, sums):
        for kind, value in enumerate(sums):
            dots[kind * (ITERS + 1) + step] = value

    sums = [zero8, zero8, zero8]
    for slot in range(nz):
        value = basis[0, slot, own]
        sums[0] = sums[0] + folded(value * value * scale[slot])
        sums[2] = sums[2] + folded(value)
    record(0, sums)

    lane_of, group_of, inner_held = lanes_of(held)

    def advance(step, slot, near, rows, first):
        same = None
        for number, (dz, dy) in enumerate(TERMS_SAME):
            value = near(dz, dy)
            if value is None:
                continue
            term = weights[number, slot, rows] * value[rows]
            same = term if same is None else same + term
        for dx, begin in ((1, 8), (-1, 13)):
            part = None
            for number, (dz, dy) in enumerate(TERMS_SIDE):
                value = near(dz, dy)
                if value is None:
                    continue
                term = weights[begin + number, slot] * value[...]
                part = term if part is None else part + term
            same = same + row_roll(part, -dx)[rows]
        value = basis[step - 1, slot, rows]
        fresh = jac[slot, rows] * same + spare[slot, rows] * value
        if first:
            factor = jnp.where(step == 1, 0.5, 1.0).astype(jnp.float32)
            back = jnp.where(step == 1, 0.0, 1.0).astype(jnp.float32)
            fresh = factor * fresh - back * basis[jnp.maximum(step - 2, 0), slot, rows]
        else:
            fresh = fresh - basis[step - 2, slot, rows]
        basis[step, slot, rows] = fresh
        return fresh, value

    def one_step(step, last, first=False, final=False):
        now = basis.at[step - 1]
        for j in range(min(last + 1, planes)):
            slot = at(j)
            found = sides(now[slot], now[planes + slot // nz], slot % nz)
            moved[0, slot], moved[1, slot] = found
        if not final:
            triples = []
            for q in range(2):
                strip = now[planes + q]
                mixed = strip
                for g in range(nz):
                    slot = q * nz + g
                    j = slot if q == 0 else 3 * nz - 1 - slot
                    if j <= last:
                        mixed = jnp.where(
                            group_of == g, lane_roll(now[slot], GROUP * g + 8), mixed
                        )
                after = lane_roll(jnp.where(inner_held == 8, mixed, strip), -1)
                before = lane_roll(jnp.where(inner_held == 7, mixed, strip), 1)
                moved[0, planes + q], moved[1, planes + q] = after, before
                triples.append((strip, after, before))
            for number in range(3):
                found = across(triples[0][number], triples[1][number])
                for which, value in enumerate(found):
                    beside[which, number] = value
            for q in range(2):
                slot = planes + q

                def near(dz, dy):
                    number = {0: 0, 1: 1, -1: 2}[dy]
                    if dz:
                        return beside.at[q if dz == 1 else 2 + q, number]
                    return now.at[slot] if dy == 0 else moved.at[number - 1, slot]

                advance(step, slot, near, slice(0, held), first)
        sums = [zero8, zero8, zero8]
        for j in range(last):
            slot = at(j)

            def near(dz, dy):
                if j + dz < 0:
                    return None
                spot = at(j + dz)
                return now.at[spot] if dy == 0 else moved.at[0 if dy == 1 else 1, spot]

            rows = own if final else slice(0, held)
            fresh, value = advance(step, slot, near, rows, first)
            if j < nz:
                if not final:
                    fresh, value = fresh[own], value[own]
                weighted = fresh * scale[slot]
                sums[0] = sums[0] + folded(weighted * fresh)
                sums[1] = sums[1] + folded(weighted * value)
                sums[2] = sums[2] + folded(fresh)
        record(step, sums)

    def early_steps(step, carry):
        one_step(step, planes - 1, first=True)
        return carry

    def later_steps(step, carry):
        one_step(step, planes - 4)
        return carry

    lax.fori_loop(1, 4, early_steps, 0)
    lax.fori_loop(4, ITERS, later_steps, 0)
    one_step(ITERS, nz, final=True)
    partial = jnp.sum(jnp.sum(dots[...], axis=1), axis=1, keepdims=True)
    entry = lax.broadcasted_iota(jnp.int32, (3 * (ITERS + 1), ny), 0)
    kind, index = entry // (ITERS + 1), entry % (ITERS + 1)
    place_of = jnp.where(kind == 0, 2 * index, jnp.where(kind == 1, 2 * index - 1, 2 * ITERS + 1 + index))
    wanted = place_of == lax.broadcasted_iota(jnp.int32, entry.shape, 1)
    final_row[...] = jnp.sum(jnp.where(wanted, partial, 0.0), axis=0, keepdims=True)
    spread(2, final_row, final_all, everyone)
    for group in moves:
        for _, sends, copy in group:
            pl.when(sends)(copy.wait_send)
    for group in relays:
        for copy in group:
            copy.wait_send()
    sums = collect(2, final_row, final_all, everyone)

    mu = [pick(sums, n) for n in range(2 * ITERS)]
    ones = [pick(sums, 2 * ITERS + 1 + n) for n in range(ITERS)]
    for n in range(2, 2 * ITERS):
        mu[n] = 2.0 * mu[n] - mu[n % 2]
    one = jnp.ones((1, 1), jnp.float32)
    y, p = [one], [one]
    m_y, m_p = list(mu), list(mu)
    x = []
    rz = mu[0]

    def plus(first, second):
        if first is None or second is None:
            return second if first is None else first
        return first + second

    def get(values, n):
        return values[n] if 0 <= n < len(values) else None

    for step in range(ITERS):
        h_p = []
        for n in range(step + 2):
            right = get(p, n - 1)
            if n == 1:
                right = right + right
            around_n = plus(get(p, n + 1), right)
            here = get(p, n)
            drop = None if around_n is None else -0.5 * around_n
            h_p.append(plus(here, drop))
        m_h = [m_p[0] - m_p[1]]
        for n in range(1, 2 * ITERS - 1 - step):
            m_h.append(m_p[n] - 0.5 * (m_p[n + 1] + m_p[n - 1]))
        bottom = p[0] * m_h[0]
        for n in range(1, step + 1):
            bottom = bottom + p[n] * m_h[n]
        alpha = rz / bottom
        x = [plus(get(x, n), alpha * p[n]) for n in range(step + 1)]
        y = [plus(get(y, n), -(alpha * h_p[n])) for n in range(step + 2)]
        if step + 1 < ITERS:
            m_y = [m_y[n] - alpha * m_h[n] for n in range(len(m_h))]
            rz_next = y[0] * m_y[0]
            for n in range(1, step + 2):
                rz_next = rz_next + y[n] * m_y[n]
            beta = rz_next / rz
            p = [plus(y[n], None if n > step else beta * p[n]) for n in range(step + 2)]
            m_p = [m_y[n] + beta * m_p[n] for n in range(len(m_y))]
            rz = rz_next
    mean = x[0] * ones[0]
    for n in range(1, ITERS):
        mean = mean + x[n] * ones[n]
    mean = mean / count
    xs = [jnp.broadcast_to(value, (8, ny)) for value in x]
    ys = [jnp.broadcast_to(value, (8, ny)) for value in y]
    mean = jnp.broadcast_to(mean, (8, ny))
    for slot in range(nz):
        target = flip(slot, side)
        for row in range(0, nx, 8):
            spot = slice(8 + row, 16 + row)
            weight = scale[slot, row : row + 8]
            total = jnp.where(weight > 0.0, -mean, 0.0)
            rest = ys[ITERS] * basis[ITERS, slot, spot]
            for n in range(ITERS):
                value = basis[n, slot, spot]
                total = total + xs[n] * value
                rest = rest + ys[n] * value
            phi[target, row : row + 8] = total
            residual[target, row : row + 8] = weight * rest


def fast_body(potential, tissue_mask, layer_index, source):
    extent = tissue_mask.shape
    nz, nx, ny = extent
    sizes = tuple(lax.axis_size(axis) for axis in AXES)
    planes, held, deep = 2 * nz, nx + 16, nx + 32
    peers = math.prod(sizes)
    vmem = pl.BlockSpec(memory_space=pltpu.VMEM)
    hbm = pl.BlockSpec(memory_space=pltpu.HBM)

    def real(*shape):
        return pltpu.VMEM(shape + (ny,), jnp.float32)

    moves = 40
    inputs = (potential, tissue_mask, layer_index, source)
    scratch = [
        real(3, planes, held), pltpu.VMEM(extent, jnp.int32), real(3, 2, nx), real(2, 2, nz),
        real(2, 2, 2, nz), real(3, deep), real(3, deep), real(5, 2, deep),
        real(9, planes + 6, deep), real(18, planes + 2, held), real(ITERS + 1, planes + 2, held),
        real(2, planes + 2, held), real(4, 3, held), real(planes + 2, held),
        real(planes + 2, held), real(planes, nx), real(2, 2, COEFS, 8), real(3 * (ITERS + 1), 8),
        real(1), real(sizes[1] * sizes[2], 1), real(1), real(sizes[0], 1), real(1), real(peers, 1),
        pltpu.SMEM((LAYERS, 18), jnp.float32), pltpu.SMEM((planes + 1, COEFS), jnp.float32),
        pltpu.SMEM((nz,), jnp.int32), pltpu.SMEM((nz,), jnp.int32), pltpu.SMEM((planes,), jnp.int32),
        pltpu.SemaphoreType.DMA((4,)), pltpu.SemaphoreType.DMA((moves,)),
        pltpu.SemaphoreType.DMA((moves,)), pltpu.SemaphoreType.DMA((3,)),
        pltpu.SemaphoreType.DMA((3,)),
    ]
    return tuple(
        pl.pallas_call(
            functools.partial(fast_kernel, extent, sizes),
            out_shape=(jax.ShapeDtypeStruct(extent, jnp.float32),) * 2,
            in_specs=[hbm] * 4,
            out_specs=(vmem, vmem),
            scratch_shapes=scratch,
            compiler_params=pltpu.CompilerParams(
                vmem_limit_bytes=32 * 1024 * 1024, collective_id=0, has_side_effects=True
            ),
        )(*(pltpu.with_memory_space_constraint(ref, pltpu.HBM) for ref in inputs))
    )


def body(potential, tissue_mask, layer_index, source):
    nz, nx, ny = tissue_mask.shape
    fits = (
        lax.axis_size("gz") == 2 and nz == 8 and ITERS == 8 and nx % 8 == 0 and nx >= 16
        and ny == nz * GROUP and lax.axis_size("gx") > 1 and lax.axis_size("gy") > 1
    )
    return (fast_body if fits else general_body)(potential, tissue_mask, layer_index, source)


def solution(mesh):
    placed = (P("gz", "gx", "gy"), P("gz", "gx", "gy"), P("gz"), P("gz", "gx", "gy"))
    return jax.shard_map(
        body,
        mesh=mesh,
        in_specs=placed,
        out_specs=(P("gz", "gx", "gy"), P("gz", "gx", "gy")),
        check_vma=False,
    )
```

```python
import functools
import math

import jax
import jax.numpy as jnp
from jax import lax
from jax.experimental import pallas as pl
from jax.experimental.pallas import tpu as pltpu
from jax.sharding import PartitionSpec as P
import numpy as np

ITERS = 8
DEPTH = ITERS + 1
LAYERS = 16
AXES = ("gx", "gy", "gz")

OFFSETS = [
    (0, 1, 0),
    (0, 0, 1),
    (1, 0, 0),
    (0, 1, 1),
    (0, 1, -1),
    (1, 1, 0),
    (-1, 1, 0),
    (1, 0, 1),
    (-1, 0, 1),
]
bulk_long = 7.99
bulk_trans = 2.55
intra_long = 1.74
intra_trans = 0.19
bath_sigma = 5.0


def tensor_table(layers, longitudinal, transverse):
    depth = jnp.arange(layers, dtype=jnp.float32) / (layers - 1)
    helix = math.pi / 3.0 * (1.0 - 2.0 * depth)
    tilted = 0.35 * jnp.cos(math.pi * depth)
    fiber_x = jnp.cos(tilted) * jnp.cos(helix)
    fiber_y = jnp.cos(tilted) * jnp.sin(helix)
    fiber_z = jnp.sin(tilted)
    spread = longitudinal - transverse
    s_xx = transverse + spread * fiber_x * fiber_x
    s_yy = transverse + spread * fiber_y * fiber_y
    s_zz = transverse + spread * fiber_z * fiber_z
    s_xy = spread * fiber_x * fiber_y
    s_xz = spread * fiber_x * fiber_z
    s_yz = spread * fiber_y * fiber_z
    columns = [
        s_xx - jnp.abs(s_xy) - jnp.abs(s_xz),
        s_yy - jnp.abs(s_xy) - jnp.abs(s_yz),
        s_zz - jnp.abs(s_xz) - jnp.abs(s_yz),
        jnp.maximum(s_xy, 0.0),
        jnp.maximum(-s_xy, 0.0),
        jnp.maximum(s_xz, 0.0),
        jnp.maximum(-s_xz, 0.0),
        jnp.maximum(s_yz, 0.0),
        jnp.maximum(-s_yz, 0.0),
    ]
    return jnp.stack(columns, axis=1)


def shifted(value, axis, hop):
    count = lax.axis_size(axis)
    pairs = [(i + hop, i) for i in range(count) if 0 <= i + hop < count]
    return lax.ppermute(value, axis, pairs)


def framed(value, axis, dim, multiple):
    count, length = lax.axis_size(axis), value.shape[dim]
    if count == 1:
        return value
    if count == 2 and 2 * length <= length + 2 * DEPTH and multiple == 1:
        other = lax.ppermute(value, axis, [(0, 1), (1, 0)])
        return jnp.concatenate([value, other], axis=dim)
    after, before = [], []
    left, hop = DEPTH, 1
    while left > 0:
        width = min(left, length)
        if hop < count:
            after.append(
                shifted(lax.slice_in_dim(value, 0, width, axis=dim), axis, hop)
            )
            before.insert(
                0, shifted(lax.slice_in_dim(value, length - width, length, axis=dim), axis, -hop)
            )
        else:
            shape = list(value.shape)
            shape[dim] = width
            after.append(jnp.zeros(shape, value.dtype))
            before.insert(0, jnp.zeros(shape, value.dtype))
        left, hop = left - width, hop + 1
    gap = -(length + 2 * DEPTH) % multiple
    shape = list(value.shape)
    shape[dim] = gap
    middle = [jnp.zeros(shape, value.dtype)] if gap else []
    return jnp.concatenate([value] + after + middle + before, axis=dim)


def fields_around(ref, here, above, below, rows, lanes):
    def along_x(value, step):
        return pltpu.roll(value, (-step) % rows, 0)

    def along_y(value, step):
        return pltpu.roll(value, (-step) % lanes, 1)

    for dz, plane in ((0, here), (1, above), (-1, below)):
        value = ref[plane]
        if dz:
            yield (dz, 0, 0), value
        for step in (1, -1):
            yield (dz, step, 0), along_x(value, step)
        for step in (1, -1):
            moved = along_y(value, step)
            yield (dz, 0, step), moved
            if dz == 0:
                for other in (1, -1):
                    yield (0, other, step), along_x(moved, other)


SLOT = {}
for _column, _offset in enumerate(OFFSETS):
    SLOT[_offset] = (_column, 2 * _column)
    SLOT[tuple(-o for o in _offset)] = (_column, 2 * _column + 1)


def grid_kernel(extent, sizes, table, mask_in, potential_in, source_in, phi, residual,
                basis, scale, dots, weights, spare, first, second, jac,
                own_row, early, final_row, late, sends, early_recv, late_recv):
    mask, potential, source = mask_in, potential_in, source_in
    planes, rows, lanes = mask.shape
    nz, nx, ny = extent
    held = jac.shape[1]
    keep = nx + ITERS
    peers = math.prod(sizes)
    me = 0
    for axis, size in zip(AXES, sizes):
        me = me * size + lax.axis_index(axis)

    def device(index):
        return (index // (sizes[1] * sizes[2]), index // sizes[2] % sizes[1], index % sizes[2])

    def peer(k):
        return lax.rem(me + k, peers)

    barrier = pltpu.get_barrier_semaphore()

    def greet(k, carry):
        pl.semaphore_signal(
            barrier, inc=1, device_id=device(peer(k)), device_id_type=pl.DeviceIdType.MESH
        )
        return carry

    lax.fori_loop(1, peers, greet, 0)

    def spread(row, gathered, recv):
        def one(k, carry):
            pltpu.make_async_remote_copy(
                src_ref=row, dst_ref=gathered.at[me], send_sem=sends.at[k],
                recv_sem=recv.at[me], device_id=device(peer(k)),
                device_id_type=pl.DeviceIdType.MESH,
            ).start()
            return carry

        lax.fori_loop(1, peers, one, 0)

    def collect(row, gathered, recv):
        def one(k, carry):
            other = peer(k)
            copy = pltpu.make_async_remote_copy(
                src_ref=row, dst_ref=gathered.at[other], send_sem=sends.at[k],
                recv_sem=recv.at[other], device_id=device(other),
                device_id_type=pl.DeviceIdType.MESH,
            )
            copy.wait_recv()
            copy.wait_send()
            return carry

        lax.fori_loop(1, peers, one, 0)
        gathered[me] = row[...]
        return jnp.sum(gathered[...], axis=0)

    lane = lax.broadcasted_iota(jnp.int32, (1, 128), 1)

    def pick(vector, index):
        return jnp.sum(jnp.where(lane == index, vector, 0.0), axis=1, keepdims=True)

    cells = jnp.zeros((1, ny), jnp.float32)
    injected = jnp.zeros((1, ny), jnp.float32)
    for plane in range(nz):
        own_inside = jnp.where(mask_in[plane, 0:nx, 0:ny] > 0.0, 1.0, 0.0)
        cells = cells + jnp.sum(own_inside, axis=0, keepdims=True)
        injected = injected + jnp.sum(
            own_inside * source_in[plane, 0:nx, 0:ny], axis=0, keepdims=True
        )
    cells = jnp.sum(cells, axis=1, keepdims=True)
    injected = jnp.sum(injected, axis=1, keepdims=True)
    own_row[...] = jnp.where(lane == 0, cells, jnp.where(lane == 1, injected, 0.0))

    def neighbours(plane):
        above = jnp.where(plane + 1 == planes, 0, plane + 1)
        below = jnp.where(plane == 0, planes - 1, plane - 1)
        return above, below

    def store(ref, index, value):
        if held == rows:
            ref[index] = value
        else:
            ref[(*index, slice(0, keep))] = value[:keep]
            ref[(*index, slice(keep, held))] = value[rows - held + keep :]

    def setup(plane, carry):
        above, below = neighbours(plane)
        labels = mask[plane]
        tissue = jnp.where(labels == 2.0, 1.0, 0.0)
        bath = jnp.where(labels == 1.0, 1.0, 0.0)
        inside = tissue + bath
        volts = potential[plane]
        total = jnp.zeros((rows, lanes), jnp.float32)
        image = jnp.zeros((rows, lanes), jnp.float32)
        pairs = zip(
            fields_around(mask, plane, above, below, rows, lanes),
            fields_around(potential, plane, above, below, rows, lanes),
        )
        for (offset, label), (_, volt) in pairs:
            column, slot = SLOT[offset]
            beyond = {0: plane, 1: above, -1: below}[offset[0]]
            link = 0.5
            if offset[0] == 1:
                link = 0.5 * table[plane, 18]
            if offset[0] == -1:
                link = 0.5 * table[below, 18]
            their_tissue = jnp.where(label == 2.0, 1.0, 0.0)
            g_here, g_there = table[plane, column] * link, table[beyond, column] * link
            weight = tissue * g_here
            if column < 3:
                their_bath = jnp.where(label == 1.0, 1.0, 0.0)
                sigma = bath_sigma * link
                weight = inside * (
                    jnp.where(label > 0.0, weight + bath * sigma, 0.0)
                    + (their_tissue * g_there + their_bath * sigma)
                )
            else:
                weight = inside * (jnp.where(label > 0.0, weight, 0.0) + their_tissue * g_there)
            store(weights, (slot, plane), weight)
            total = total + weight
            intra = (table[plane, 9 + column] + table[beyond, 9 + column]) * link
            image = image + (tissue * their_tissue * intra) * (volts - volt)
        bounded = jnp.maximum(total, 1.0)
        jacobi = inside / bounded
        store(jac, (plane,), jacobi + jacobi)
        store(spare, (plane,), inside * (1.0 - jacobi * total))
        store(first, (plane,), jacobi * (inside * source[plane] - image))

        @pl.when(plane < nz)
        def _():
            scale[plane] = (inside * bounded)[:nx, :ny]

        return carry

    lax.fori_loop(0, planes // 2, setup, 0)
    pl.semaphore_wait(barrier, peers - 1)
    spread(own_row, early, early_recv)
    lax.fori_loop(planes // 2, planes, setup, 0)
    totals = collect(own_row, early, early_recv)
    count = pick(totals, 0)
    mean_rhs = pick(totals, 1) / count

    def centre(plane, carry):
        first[plane] = first[plane] - 0.5 * jac[plane] * mean_rhs
        return carry

    lax.fori_loop(0, planes, centre, 0)

    def record(step, now, before):
        rowsum = jnp.zeros((1, ny), jnp.float32)
        square, cross, plain = rowsum, rowsum, rowsum
        for plane in range(nz):
            value = now[plane, 0:nx, 0:ny]
            basis[step, plane] = value
            weighted = value * scale[plane]
            square = square + jnp.sum(weighted * value, axis=0, keepdims=True)
            if step:
                past = basis[step - 1, plane]
                cross = cross + jnp.sum(weighted * past, axis=0, keepdims=True)
            plain = plain + jnp.sum(value, axis=0, keepdims=True)
        if step < ITERS:
            dots[pl.ds(2 * step, 1)] = square
            dots[pl.ds(2 * ITERS + step, 1)] = plain
        if step:
            dots[pl.ds(2 * step - 1, 1)] = cross

    record(0, first, None)

    def apply(now, old, step):
        reach = ITERS - step
        if planes == nz:
            begin, span = 0, nz
        elif planes == sizes[2] * nz:
            begin = planes - lax.axis_index("gz") * reach
            span = min(planes, nz + reach)
        else:
            begin, span = planes - reach, nz + 2 * reach

        def one(index, carry):
            plane = lax.rem(begin + index, planes)
            above, below = neighbours(plane)
            total = jnp.zeros((held, lanes), jnp.float32)
            for offset, value in fields_around(now, plane, above, below, held, lanes):
                total = total + weights[SLOT[offset][1], plane] * value
            if step == 1:
                old[plane] = 0.5 * jac[plane] * total + spare[plane] * now[plane]
            else:
                old[plane] = (
                    jac[plane] * total + 2.0 * spare[plane] * now[plane] - old[plane]
                )
            return carry

        lax.fori_loop(0, span, one, 0)

    now, old = first, second
    for step in range(1, ITERS + 1):
        apply(now, old, step)
        now, old = old, now
        record(step, now, old)

    partial = jnp.sum(dots[...], axis=1, keepdims=True)
    diagonal = lax.broadcasted_iota(jnp.int32, (3 * ITERS, 128), 0) == lax.broadcasted_iota(
        jnp.int32, (3 * ITERS, 128), 1
    )
    final_row[...] = jnp.sum(jnp.where(diagonal, partial, 0.0), axis=0, keepdims=True)
    spread(final_row, late, late_recv)
    sums = collect(final_row, late, late_recv)

    def left(vector):
        return pltpu.roll(vector, 127, 1)

    def right(vector):
        return pltpu.roll(vector, 1, 1)

    mu0, mu1 = pick(sums, 0), pick(sums, 1)
    mu = jnp.where(lane < 2, sums, 2.0 * sums - jnp.where(lane % 2 == 0, mu0, mu1))
    mu = jnp.where(lane < 2 * ITERS, mu, 0.0)
    ones = pltpu.roll(sums, 128 - 2 * ITERS, 1)
    y = jnp.where(lane == 0, 1.0, 0.0)
    p = y
    m_y, m_p = mu, mu
    x = jnp.zeros((1, 128), jnp.float32)
    rz = mu0
    for step in range(ITERS):
        h_p = p - 0.5 * (left(p) + jnp.where(lane == 1, 2.0, 1.0) * right(p))
        h_p = jnp.where(lane <= ITERS, h_p, 0.0)
        before = jnp.where(lane == 0, left(m_p), right(m_p))
        m_h = m_p - 0.5 * (left(m_p) + before)
        alpha = rz / jnp.sum(jnp.where(lane < ITERS, p * m_h, 0.0), axis=1, keepdims=True)
        x = x + alpha * p
        y = y - alpha * h_p
        m_y = m_y - alpha * m_h
        if step + 1 < ITERS:
            rz_next = jnp.sum(jnp.where(lane < ITERS, y * m_y, 0.0), axis=1, keepdims=True)
            beta = rz_next / rz
            p = y + beta * p
            m_p = m_y + beta * m_p
            rz = rz_next
    mean = jnp.sum(jnp.where(lane < ITERS, x * ones, 0.0), axis=1, keepdims=True) / count
    xs = [pick(x, j) for j in range(ITERS)]
    ys = [pick(y, j) for j in range(ITERS + 1)]

    def one(plane, carry):
        weight = scale[plane]
        total = jnp.where(weight > 0.0, -mean, 0.0)
        rest = ys[ITERS] * basis[ITERS, plane]
        for j in range(ITERS):
            value = basis[j, plane]
            total = total + xs[j] * value
            rest = rest + ys[j] * value
        phi[plane] = total
        residual[plane] = weight * rest
        return carry

    lax.fori_loop(0, nz, one, 0)


def general_body(potential, tissue_mask, layer_index, source):
    extent = tissue_mask.shape
    nz = extent[0]
    labels = tissue_mask.astype(jnp.float32)
    sizes = tuple(lax.axis_size(axis) for axis in AXES)
    packed = jnp.stack([labels, potential, source], axis=1)
    packed = framed(packed, "gz", 0, 1)
    packed = framed(packed, "gx", 2, 8)
    packed = framed(packed, "gy", 3, 128)
    operands = (packed[:, 0], packed[:, 1], packed[:, 2])
    frame = operands[0].shape
    layers = framed(layer_index, "gz", 0, 1)
    planes = layers.shape[0]
    selector = (layers[:, None] == jnp.arange(LAYERS, dtype=jnp.int32)[None, :]).astype(
        jnp.float32
    )
    tables = jnp.concatenate(
        [
            tensor_table(LAYERS, bulk_long, bulk_trans),
            tensor_table(LAYERS, intra_long, intra_trans),
        ],
        axis=1,
    )
    table = jnp.dot(selector, tables, precision=lax.Precision.HIGHEST)
    size = lax.axis_size("gz")
    link = jnp.ones((planes, 1), jnp.float32)
    if planes == size * nz:
        place = (lax.axis_index("gz") * nz + jnp.arange(planes)) % planes
        link = (place + 1 < planes).astype(jnp.float32)[:, None]
    table = jnp.concatenate([table, link], axis=1)
    smem = pl.BlockSpec(memory_space=pltpu.SMEM)
    vmem = pl.BlockSpec(memory_space=pltpu.VMEM)
    compact = frame
    if extent[1] % 8 == 0 and ITERS % 8 == 0 and frame[1] > extent[1] + 2 * ITERS:
        compact = (planes, extent[1] + 2 * ITERS, frame[2])
    peers = math.prod(sizes)
    row = pltpu.VMEM((1, 128), jnp.float32)
    gathered = pltpu.VMEM((peers, 1, 128), jnp.float32)
    return tuple(
        pl.pallas_call(
            functools.partial(grid_kernel, extent, sizes),
            out_shape=(jax.ShapeDtypeStruct(extent, jnp.float32),) * 2,
            in_specs=[smem, vmem, vmem, vmem],
            out_specs=(vmem, vmem),
            scratch_shapes=[
                pltpu.VMEM((ITERS + 1,) + extent, jnp.float32),
                pltpu.VMEM(extent, jnp.float32),
                pltpu.VMEM((3 * ITERS, extent[2]), jnp.float32),
                pltpu.VMEM((18,) + compact, jnp.float32),
            ]
            + [pltpu.VMEM(compact, jnp.float32)] * 4
            + [row, gathered, row, gathered]
            + [pltpu.SemaphoreType.DMA((peers,))] * 3,
            compiler_params=pltpu.CompilerParams(
                vmem_limit_bytes=60 * 1024 * 1024, collective_id=0, has_side_effects=True
            ),
        )(table, *operands)
    )


GROUP = 16
TERMS_SAME = [(0, 1), (0, -1), (1, 0), (-1, 0), (1, 1), (1, -1), (-1, 1), (-1, -1)]
TERMS_SIDE = [(0, 0), (0, 1), (0, -1), (1, 0), (-1, 0)]
LEVEL = [0, 1, 3, 4]
STEEP = [(0, 0), (1, 0), (-1, 0), (0, 1), (0, -1)]
UPWARD = 2 * len(LEVEL)
COEFS = UPWARD + 1 + 3 * len(STEEP)


def numpy_table(longitudinal, transverse):
    depth = np.arange(LAYERS, dtype=np.float64) / (LAYERS - 1)
    helix = math.pi / 3.0 * (1.0 - 2.0 * depth)
    tilted = 0.35 * np.cos(math.pi * depth)
    fiber = (np.cos(tilted) * np.cos(helix), np.cos(tilted) * np.sin(helix), np.sin(tilted))
    spread = longitudinal - transverse
    s_xx, s_yy, s_zz = (transverse + spread * f * f for f in fiber)
    s_xy = spread * fiber[0] * fiber[1]
    s_xz = spread * fiber[0] * fiber[2]
    s_yz = spread * fiber[1] * fiber[2]
    columns = [s_xx - abs(s_xy) - abs(s_xz), s_yy - abs(s_xy) - abs(s_yz), s_zz - abs(s_xz) - abs(s_yz)]
    for value in (s_xy, s_xz, s_yz):
        columns += [np.maximum(value, 0.0), np.maximum(-value, 0.0)]
    return np.stack(columns, axis=1)


HALF_TABLE = 0.5 * np.concatenate(
    [numpy_table(bulk_long, bulk_trans), numpy_table(intra_long, intra_trans)], axis=1
)


def lane_roll(value, step):
    size = value.shape[1]
    return pltpu.roll(value, step % size if isinstance(step, int) else lax.rem(step + size, size), 1)


def row_roll(value, step):
    return pltpu.roll(value, step % value.shape[0], 0)


def tiled(value, rows):
    return jnp.concatenate([value] * (rows // value.shape[0]), axis=0)


def column_of(dz, dx, dy, side):
    same, flipped = SLOT[(dz, dx, dy)][0], SLOT[(-dz, dx, dy)][0]
    return same if same == flipped else same + side * (flipped - same)


def fast_kernel(extent, sizes, potential_in, mask_in, layers_in, source_in, phi, residual,
                fields, labels, packs, edge_send, edge_recv, from_after, from_before, strips,
                derived, weights, basis, moved, beside, jac, spare, scale, coef_lanes, dots,
                early_row, early_all, line_row, line_all, final_row, final_all,
                table, coefs, layers_own, layers_far, layers,
                loads, halo_send, halo_recv, sum_send, sum_recv):
    nz, nx, ny = extent
    planes, held, deep = 2 * nz, nx + 16, nx + 32
    own = slice(8, 8 + nx)
    place = tuple(lax.axis_index(axis) for axis in AXES)
    gx, gy, side = place
    first_x, last_x = gx == 0, gx == sizes[0] - 1
    first_y, last_y = gy == 0, gy == sizes[1] - 1

    def exists(dx, dy):
        return (gx + dx >= 0) & (gx + dx < sizes[0]) & (gy + dy >= 0) & (gy + dy < sizes[1])

    def around(a, b, c):
        return tuple(
            lax.rem(here + step, size) if step else here
            for here, step, size in zip(place, (a, b, c), sizes)
        )

    slab = [(0, b, c) for b in range(sizes[1]) for c in range(sizes[2])]
    line = [(a, 0, 0) for a in range(sizes[0])]
    everyone = [(a, b, c) for a, _, _ in line for _, b, c in slab]
    corners = [(dx, dy) for dx in (1, -1) for dy in (1, -1)]

    def flip(slot, turned):
        return slot + turned * (nz - 1 - 2 * slot)

    get_layers = pltpu.make_async_copy(layers_in, layers_own, loads.at[0])
    get_mask = pltpu.make_async_copy(mask_in, labels, loads.at[1])
    get_layers.start()
    get_mask.start()
    whole = []
    for index, ref in ((1, potential_in), (2, source_in)):
        for plane in range(nz):
            pltpu.make_async_copy(
                ref.at[plane], fields.at[index, flip(plane, side), own], loads.at[1 + index]
            ).start()
        whole.append(pltpu.make_async_copy(ref, fields.at[index, 0:nz, own], loads.at[1 + index]))

    barrier = pltpu.get_barrier_semaphore()

    def greet(target):
        pl.semaphore_signal(
            barrier, inc=1, device_id=target, device_id_type=pl.DeviceIdType.MESH
        )

    expected = len(slab) + len(line) - 2
    for step in slab[1:] + line[1:]:
        greet(around(*step))
    for dx, dy in corners:
        pl.when(exists(dx, dy))(lambda: greet((gx + dx, gy + dy, side)))
        expected = expected + jnp.where(exists(dx, dy), 1, 0)

    def clear(when, ref, index):
        @pl.when(when)
        def _():
            ref[index] = jnp.zeros(ref.at[index].shape, jnp.float32)

    every = slice(None)
    clear(first_x, fields, (every, slice(0, nz), slice(0, 8)))
    clear(last_x, fields, (every, slice(0, nz), slice(8 + nx, held)))
    for index in range(2):
        clear(first_x, edge_recv, (0, index, 0))
        clear(last_x, edge_recv, (0, index, 1))
    for ref, edge in ((from_after, last_y), (from_before, first_y)):
        clear(edge, ref, (every,))
        clear(first_x, ref, (every, slice(0, 16)))
        clear(last_x, ref, (every, slice(16 + nx, deep)))
    def lanes_of(rows):
        lane = lax.broadcasted_iota(jnp.int32, (rows, ny), 1)
        return lane, lane // GROUP, lane % GROUP

    lane = lax.broadcasted_iota(jnp.int32, (1, ny), 1)

    def pick(vector, index):
        return jnp.sum(jnp.where(lane == index, vector, 0.0), axis=1, keepdims=True)

    own_lane, _, _ = lanes_of(nx)
    later = (own_lane + 1) % ny // GROUP
    sooner = (own_lane + ny - 1) % ny // GROUP

    def pack(index):
        values = [fields[index, slot, own] for slot in range(nz)]
        turned = [lane_roll(value, GROUP * slot + 8) for slot, value in enumerate(values)]
        for toward, owner in ((0, later), (1, sooner)):
            total = turned[0]
            for slot in range(1, nz):
                total = jnp.where(owner == slot, turned[slot], total)
            packs[index, toward] = total
        if index < 2:
            for slot in range(nz):
                edge_send[index, 0, slot : slot + 1] = values[slot][8:9]
                edge_send[index, 1, slot : slot + 1] = values[slot][nx - 9 : nx - 8]

    def spread(number, row, gathered, targets):
        for index, step in enumerate(targets):
            if index:
                pltpu.make_async_remote_copy(
                    src_ref=row, dst_ref=gathered.at[index], send_sem=sum_send.at[number],
                    recv_sem=sum_recv.at[number], device_id=around(*step),
                    device_id_type=pl.DeviceIdType.MESH,
                ).start()

    def collect(number, row, gathered, targets):
        arrived = gathered.at[pl.ds(1, len(targets) - 1)]
        pltpu.make_async_copy(arrived, arrived, sum_recv.at[number]).wait()
        pltpu.make_async_copy(arrived, arrived, sum_send.at[number]).wait()
        gathered[0] = row[...]
        return jnp.sum(gathered[...], axis=0)

    def link(number, src, dst, target):
        return pltpu.make_async_remote_copy(
            src_ref=src, dst_ref=dst, send_sem=halo_send.at[number],
            recv_sem=halo_recv.at[number], device_id=target,
            device_id_type=pl.DeviceIdType.MESH,
        )

    other = (gx, gy, 1 - side)
    numbers = iter(range(64))

    def swap(src, dst):
        copy = link(next(numbers), src, dst, other)
        copy.start()
        return copy

    def exchange(picked, rows, edge):
        found = []

        def move(dx, dy, src, dst):
            copy = link(next(numbers), src, dst, (gx + dx, gy + dy, side))
            pl.when(exists(dx, dy))(copy.start)
            found.append((exists(-dx, -dy), exists(dx, dy), copy))

        for dx, dy in corners:
            into, toward = (from_before, 0) if dy == 1 else (from_after, 1)
            if dx == 1:
                move(dx, dy, packs.at[rows, toward, nx - 16 : nx], into.at[rows, 0:16])
            else:
                move(dx, dy, packs.at[rows, toward, 0:16], into.at[rows, 16 + nx : deep])
        move(0, 1, packs.at[rows, 0], from_before.at[rows, 16 : 16 + nx])
        move(0, -1, packs.at[rows, 1], from_after.at[rows, 16 : 16 + nx])
        move(1, 0, edge_send.at[edge, 1], edge_recv.at[0, edge, 0])
        move(-1, 0, edge_send.at[edge, 0], edge_recv.at[0, edge, 1])
        move(1, 0, fields.at[rows, 0:nz, nx : nx + 8], fields.at[rows, 0:nz, 0:8])
        move(-1, 0, fields.at[rows, 0:nz, 8:16], fields.at[rows, 0:nz, 8 + nx : held])
        return found

    groups = [(slice(0, 2), slice(0, 1), 0), (slice(2, 5), slice(1, 3), 1)]
    moves, relays = [], []

    def launch(picked, rows, edge):
        moves.append(exchange(picked, rows, edge))
        relays.append([swap(fields.at[rows, 0:nz, own], fields.at[rows, nz:planes, own])])

    def relay(picked, rows, edge):
        for receives, _, copy in moves[edge]:
            pl.when(receives)(copy.wait_recv)
        for index in range(rows.start, rows.stop):
            below, above = from_before[index], from_after[index]
            strips[2 * index, 0] = jnp.where(inner_deep < 8, below, above)
            if index < 2:
                strips[2 * index + 1, 0] = jnp.where(
                    inner_deep == 15, lane_roll(above, -1), lane_roll(below, 1)
                )
        relays[edge] += [
            swap(strips.at[picked, 0], strips.at[picked, 1]),
            swap(edge_recv.at[0, edge], edge_recv.at[1, edge]),
            swap(fields.at[rows, 0:nz, 0:8], fields.at[rows, nz:planes, 0:8]),
            swap(fields.at[rows, 0:nz, 8 + nx : held], fields.at[rows, nz:planes, 8 + nx : held]),
        ]

    get_mask.wait()
    get_layers.wait()
    for plane in range(nz):
        fields[0, flip(plane, side), own] = labels[plane].astype(jnp.float32)
    pack(0)
    pl.semaphore_wait(barrier, expected)
    layer_swap = swap(layers_own, layers_far)
    launch(*groups[0])
    for copy in whole:
        copy.wait()
    cells = jnp.zeros((8, ny), jnp.float32)
    injected = cells
    for slot in range(nz):
        for row in range(8, 8 + nx, 8):
            inside = jnp.where(fields[0, slot, row : row + 8] > 0.0, 1.0, 0.0)
            cells = cells + inside
            injected = injected + inside * fields[2, slot, row : row + 8]
    cells = jnp.sum(jnp.sum(cells, axis=0, keepdims=True), axis=1, keepdims=True)
    injected = jnp.sum(jnp.sum(injected, axis=0, keepdims=True), axis=1, keepdims=True)
    early_row[...] = jnp.where(lane == 0, cells, jnp.where(lane == 1, injected, 0.0))

    spread(0, early_row, early_all, slab)
    pack(1)
    pack(2)

    for layer in range(LAYERS):
        for column in range(18):
            table[layer, column] = jnp.float32(HALF_TABLE[layer, column])

    layer_swap.wait()
    for slot in range(nz):
        layers[slot] = layers_own[flip(slot, side)]
        layers[nz + slot] = layers_far[flip(slot, 1 - side)]

    def slot_of(j):
        return jnp.where(j < nz, j, 3 * nz - 1 - j)

    def coefficients(pair, carry):
        for slot in (2 * pair, 2 * pair + 1):
            j = slot_of(slot)
            layer = layers[slot]
            for n, k in enumerate(LEVEL):
                coefs[slot, 2 * n] = table[layer, k]
                coefs[slot, 2 * n + 1] = 2.0 * table[layer, 9 + k]
            near = j + 1 < planes
            there = layers[slot_of(jnp.where(near, j + 1, j))]
            open_ = jnp.where(near, 1.0, 0.0).astype(jnp.float32)
            coefs[slot, UPWARD] = 0.5 * bath_sigma * open_
            for n, (dx, dy) in enumerate(STEEP):
                k = column_of(1, dx, dy, side)
                coefs[slot, UPWARD + 1 + 3 * n] = table[layer, k] * open_
                coefs[slot, UPWARD + 2 + 3 * n] = table[there, k] * open_
                coefs[slot, UPWARD + 3 + 3 * n] = (table[layer, 9 + k] + table[there, 9 + k]) * open_
        return carry

    launch(*groups[1])
    lax.fori_loop(0, nz, coefficients, 0)
    for n in range(COEFS):
        coefs[planes, n] = jnp.float32(0.0)
    _, group8, _ = lanes_of(8)

    def at(j):
        return j if j < nz else 3 * nz - 1 - j

    def widen(block, carry):
        for n in [8 * block + m for m in range(8)]:
            for q in range(2):
                for which, shift in enumerate((0, -1)):
                    value = None
                    for g in range(nz):
                        j = at(q * nz + g) + shift
                        entry = coefs[planes if j < 0 else at(j), n]
                        if value is None:
                            value = jnp.full((8, ny), entry, jnp.float32)
                        else:
                            value = jnp.where(group8 == g, entry, value)
                    coef_lanes[which, q, n] = value
        return carry

    lax.fori_loop(0, COEFS // 8, widen, 0)

    lane_of, group_of, inner_deep = lanes_of(deep)
    relay(*groups[0])
    def ring_of(strip, g):
        return lane_roll(strip, -(GROUP * g + 8))

    def sides(value, ring):
        after = lane_roll(jnp.where(lane_of == 0, ring, value), -1)
        before = lane_roll(jnp.where(lane_of == ny - 1, ring, value), 1)
        return after, before

    def stored(index, number, slot, value):
        if index:
            derived[3 * number + 2, slot] = value
        else:
            derived[3 * number, slot] = jnp.where(value == 2.0, 1.0, 0.0)
            derived[3 * number + 1, slot] = jnp.where(value > 0.0, 1.0, 0.0)

    def framed_plane(index, q, g):
        before = jnp.broadcast_to(edge_recv[q, index, 0, pl.ds(g, 1)], (8, ny))
        after = jnp.broadcast_to(edge_recv[q, index, 1, pl.ds(g, 1)], (8, ny))
        return jnp.concatenate([before, fields[index, q * nz + g], after], axis=0)

    def derive_plane(index, q, g, mixed, ring):
        value = framed_plane(index, q, g)
        for number, part in enumerate((value,) + sides(value, ring)):
            stored(index, number, q * nz + g, part)
        return jnp.where(group_of == g, lane_roll(value, GROUP * g + 8), mixed)

    def derive_strip(index, q, mixed):
        strip, edge = strips[2 * index, q], strips[2 * index + 1, q]
        after = lane_roll(jnp.where(inner_deep == 8, mixed, strip), -1)
        before = lane_roll(jnp.where(inner_deep == 7, mixed, strip), 1)
        stored(index, 0, planes + q, strip)
        stored(index, 1, planes + q, jnp.where(inner_deep == 15, edge, after))
        stored(index, 2, planes + q, jnp.where(inner_deep == 0, edge, before))

    def derive_beside(index):
        for number in ((2, 5, 8) if index else (0, 1, 3, 4, 6, 7)):
            found = across(derived[number, planes], derived[number, planes + 1])
            for shift, value in enumerate(found):
                derived[number, planes + 2 + shift] = value

    def across(lower, upper):
        up0 = jnp.where(group_of == nz - 1, upper, lane_roll(lower, -GROUP))
        up1 = lane_roll(upper, GROUP)
        down0 = lane_roll(lower, GROUP)
        down1 = jnp.where(group_of == nz - 1, lower, lane_roll(upper, -GROUP))
        return up0, up1, down0, down1

    def level_of(coef):
        return {k: (coef(1, 2 * n), coef(1, 2 * n + 1)) for n, k in enumerate(LEVEL)}

    def steep_of(coef, dz):
        entries = {}
        for n, (dx, dy) in enumerate(STEEP):
            here, there, intra = (coef(dz, UPWARD + 1 + 3 * n + m) for m in range(3))
            if dz == 1:
                entries[(dx, dy)] = here, there, intra
            else:
                entries[(-dx, -dy)] = there, here, intra
        return coef(dz, UPWARD), entries

    middle = slice(8, 8 + held)

    def by(value, factor):
        if isinstance(factor, float) or factor.ndim == 0:
            return value * factor
        return value * tiled(factor, value.shape[0])

    def gathered_terms(edges, full):
        sums = edges(tuple(value[middle] for value in full), middle, 0, TERMS_SAME, 0)
        high = tuple(row_roll(value, 1)[8:deep] for value in full)
        part = edges(high, slice(8, deep), 1, TERMS_SIDE, 8)
        sums = sums + row_roll(part, -1)[0:held]
        low = tuple(row_roll(value, -1)[0 : 8 + held] for value in full)
        part = edges(low, slice(0, 8 + held), -1, TERMS_SIDE, 13)
        return sums + row_roll(part, 1)[middle]

    def weigh(slot, above, below, coef):
        level, slopes = level_of(coef), {1: steep_of(coef, 1), -1: steep_of(coef, -1)}
        base_bath = 0.5 * bath_sigma
        neighbour = {0: slot, 1: above, -1: below}

        def fetch(dz, dy, rows):
            number = {0: 0, 1: 1, -1: 2}[dy]
            return tuple(derived[3 * number + m, neighbour[dz], rows] for m in range(2))

        def edges(centre, rows, dx, terms, first):
            t, i = centre
            total = None
            keep = {0: slice(0, held), 1: slice(0, held), -1: slice(8, 8 + held)}[dx]
            for number, (dz, dy) in enumerate(terms):
                tn, i_n = fetch(dz, dy, rows)
                if dz == 0:
                    g_here = g_there = level[SLOT[(0, dx, dy)][0]][0]
                    bath = base_bath
                else:
                    bath, entries = slopes[dz]
                    g_here, g_there, _ = entries[(dx, dy)]
                if (dz != 0) + (dx != 0) + (dy != 0) == 1:
                    ours = by(t, g_here - bath) + by(i, bath)
                    theirs = by(tn, g_there - bath) + by(i_n, bath)
                else:
                    ours, theirs = by(t, g_here), by(tn, g_there)
                weight = i_n * ours + i * theirs
                weights[first + number, slot] = weight[keep]
                total = weight if total is None else total + weight
            return total

        full = fetch(0, 0, slice(0, deep))
        total = gathered_terms(edges, full)
        inside = full[1][middle]
        bounded = jnp.maximum(total, 1.0)
        jacobi = inside / bounded
        jac[slot] = jacobi + jacobi
        spare[slot] = 2.0 * (inside - inside * (jacobi * total))
        return (inside * bounded)[own]

    def begin(slot, above, below, coef, source):
        level, slopes = level_of(coef), {1: steep_of(coef, 1), -1: steep_of(coef, -1)}
        neighbour = {0: slot, 1: above, -1: below}

        def edges(centre, rows, dx, terms, first):
            v = centre[0]
            image = None
            for dz, dy in terms:
                number = {0: 0, 1: 1, -1: 2}[dy]
                tn = derived[3 * number, neighbour[dz], rows]
                vn = derived[3 * number + 2, neighbour[dz], rows]
                if dz == 0:
                    intra = level[SLOT[(0, dx, dy)][0]][1]
                else:
                    intra = slopes[dz][1][(dx, dy)][2]
                term = by(tn * (v - vn), intra)
                image = term if image is None else image + term
            return image

        image = gathered_terms(edges, (derived[2, slot],))
        tissue, inside = derived[0, slot, middle], derived[1, slot, middle]
        value = 0.5 * jac[slot] * (inside * (source - mean_rhs) - tissue * image)
        basis[0, slot] = value
        return value[own]

    def beyond(slot):
        j = slot_of(slot)
        return slot_of(jnp.minimum(j + 1, planes - 1)), slot_of(jnp.maximum(j - 1, 0))

    def from_table(slot):
        j = slot_of(slot)
        under = jnp.where(j == 0, planes, slot_of(j - 1))
        return lambda dz, n: coefs[slot if dz == 1 else under, n]

    def from_lanes(q):
        return lambda dz, n: coef_lanes[0 if dz == 1 else 1, q, n]

    def plane_weigh(slot, carry):
        scale[slot] = weigh(slot, *beyond(slot), from_table(slot))
        return carry

    def strip_weigh(q, carry):
        slot = planes + q
        weigh(slot, slot + 2, slot + 4, from_lanes(q))
        return carry

    def label_half(q, carry):
        @pl.when(q == 1)
        def _():
            for copy in relays[0]:
                copy.wait_recv()
            line_row[...] = collect(0, early_row, early_all, slab)
            spread(1, line_row, line_all, line)

        mixed = strips[0, q]
        for g in range(nz):
            mixed = derive_plane(0, q, g, mixed, ring_of(strips[0, q], g))
        derive_strip(0, q, mixed)
        lax.fori_loop(q * (nz - 1), nz - 1 + q, plane_weigh, 0)
        return carry

    lax.fori_loop(0, 2, label_half, 0)
    relay(*groups[1])
    def derive_pair(q, pair, mixed):
        for g in (2 * pair, 2 * pair + 1):
            mixed = derive_plane(1, q, g, mixed, ring_of(strips[2, q], g))
        return mixed

    def far_weigh(pair, mixed):
        for m in range(2):
            plane_weigh(nz + 2 * pair + m, 0)
        return derive_pair(0, pair, mixed)

    mixed = lax.fori_loop(0, nz // 2, far_weigh, strips[2, 0])
    derive_strip(1, 0, mixed)
    derive_beside(0)
    lax.fori_loop(0, 2, strip_weigh, 0)
    for copy in relays[1]:
        copy.wait_recv()

    totals = collect(1, line_row, line_all, line)
    count = pick(totals, 0)
    mean_rhs = pick(totals, 1) / count

    def plane_begin(slot, carry):
        begin(slot, *beyond(slot), from_table(slot), fields[2, slot])
        return carry

    def own_begin(pair, mixed):
        plane_begin(2 * pair, 0)
        plane_begin(jnp.minimum(2 * pair + 1, nz - 2), 0)
        return derive_pair(1, pair, mixed)

    def strip_begin(q, carry):
        slot = planes + q
        begin(slot, slot + 2, slot + 4, from_lanes(q), strips[4, q, middle])
        return carry

    mixed = lax.fori_loop(0, nz // 2, own_begin, strips[2, 1])
    derive_strip(1, 1, mixed)
    derive_beside(1)
    lax.fori_loop(nz - 1, planes, plane_begin, 0)
    lax.fori_loop(0, 2, strip_begin, 0)

    def folded(value):
        total = value[0:8]
        for row in range(8, value.shape[0], 8):
            total = total + value[row : row + 8]
        return total

    zero8 = jnp.zeros((8, ny), jnp.float32)

    def record(step, sums):
        for kind, value in enumerate(sums):
            dots[kind * (ITERS + 1) + step] = value

    sums = [zero8, zero8, zero8]
    for slot in range(nz):
        value = basis[0, slot, own]
        sums[0] = sums[0] + folded(value * value * scale[slot])
        sums[2] = sums[2] + folded(value)
    record(0, sums)

    lane_of, group_of, inner_held = lanes_of(held)

    def advance(step, slot, near, rows, first):
        same = None
        for number, (dz, dy) in enumerate(TERMS_SAME):
            value = near(dz, dy)
            if value is None:
                continue
            term = weights[number, slot, rows] * value[rows]
            same = term if same is None else same + term
        for dx, begin in ((1, 8), (-1, 13)):
            part = None
            for number, (dz, dy) in enumerate(TERMS_SIDE):
                value = near(dz, dy)
                if value is None:
                    continue
                term = weights[begin + number, slot] * value[...]
                part = term if part is None else part + term
            same = same + row_roll(part, -dx)[rows]
        value = basis[step - 1, slot, rows]
        fresh = jac[slot, rows] * same + spare[slot, rows] * value
        if first:
            factor = jnp.where(step == 1, 0.5, 1.0).astype(jnp.float32)
            back = jnp.where(step == 1, 0.0, 1.0).astype(jnp.float32)
            fresh = factor * fresh - back * basis[jnp.maximum(step - 2, 0), slot, rows]
        else:
            fresh = fresh - basis[step - 2, slot, rows]
        basis[step, slot, rows] = fresh
        return fresh, value

    def one_step(step, last, first=False, final=False):
        now = basis.at[step - 1]
        for j in range(min(last + 1, planes)):
            slot = at(j)
            found = sides(now[slot], ring_of(now[planes + slot // nz], slot % nz))
            moved[0, slot], moved[1, slot] = found
        if not final:
            triples = []
            for q in range(2):
                strip = now[planes + q]
                mixed = strip
                for g in range(nz):
                    slot = q * nz + g
                    j = slot if q == 0 else 3 * nz - 1 - slot
                    if j <= last:
                        mixed = jnp.where(
                            group_of == g, lane_roll(now[slot], GROUP * g + 8), mixed
                        )
                after = lane_roll(jnp.where(inner_held == 8, mixed, strip), -1)
                before = lane_roll(jnp.where(inner_held == 7, mixed, strip), 1)
                moved[0, planes + q], moved[1, planes + q] = after, before
                triples.append((strip, after, before))
            for number in range(3):
                found = across(triples[0][number], triples[1][number])
                for which, value in enumerate(found):
                    beside[which, number] = value
            for q in range(2):
                slot = planes + q

                def near(dz, dy):
                    number = {0: 0, 1: 1, -1: 2}[dy]
                    if dz:
                        return beside.at[q if dz == 1 else 2 + q, number]
                    return now.at[slot] if dy == 0 else moved.at[number - 1, slot]

                advance(step, slot, near, slice(0, held), first)
        sums = [zero8, zero8, zero8]
        for j in range(last):
            slot = at(j)

            def near(dz, dy):
                if j + dz < 0:
                    return None
                spot = at(j + dz)
                return now.at[spot] if dy == 0 else moved.at[0 if dy == 1 else 1, spot]

            rows = own if final else slice(0, held)
            fresh, value = advance(step, slot, near, rows, first)
            if j < nz:
                if not final:
                    fresh, value = fresh[own], value[own]
                weighted = fresh * scale[slot]
                sums[0] = sums[0] + folded(weighted * fresh)
                sums[1] = sums[1] + folded(weighted * value)
                sums[2] = sums[2] + folded(fresh)
        record(step, sums)

    def early_steps(step, carry):
        one_step(step, planes - 1, first=True)
        return carry

    def later_steps(step, carry):
        one_step(step, planes - 4)
        return carry

    lax.fori_loop(1, 4, early_steps, 0)
    lax.fori_loop(4, ITERS, later_steps, 0)
    one_step(ITERS, nz, final=True)
    partial = jnp.sum(jnp.sum(dots[...], axis=1), axis=1, keepdims=True)
    entry = lax.broadcasted_iota(jnp.int32, (3 * (ITERS + 1), ny), 0)
    kind, index = entry // (ITERS + 1), entry % (ITERS + 1)
    place_of = jnp.where(kind == 0, 2 * index, jnp.where(kind == 1, 2 * index - 1, 2 * ITERS + 1 + index))
    wanted = place_of == lax.broadcasted_iota(jnp.int32, entry.shape, 1)
    final_row[...] = jnp.sum(jnp.where(wanted, partial, 0.0), axis=0, keepdims=True)
    spread(2, final_row, final_all, everyone)
    for group in moves:
        for _, sends, copy in group:
            pl.when(sends)(copy.wait_send)
    for group in relays:
        for copy in group:
            copy.wait_send()
    sums = collect(2, final_row, final_all, everyone)

    mu = [pick(sums, n) for n in range(2 * ITERS)]
    ones = [pick(sums, 2 * ITERS + 1 + n) for n in range(ITERS)]
    for n in range(2, 2 * ITERS):
        mu[n] = 2.0 * mu[n] - mu[n % 2]
    one = jnp.ones((1, 1), jnp.float32)
    y, p = [one], [one]
    m_y, m_p = list(mu), list(mu)
    x = []
    rz = mu[0]

    def plus(first, second):
        if first is None or second is None:
            return second if first is None else first
        return first + second

    def get(values, n):
        return values[n] if 0 <= n < len(values) else None

    for step in range(ITERS):
        h_p = []
        for n in range(step + 2):
            right = get(p, n - 1)
            if n == 1:
                right = right + right
            around_n = plus(get(p, n + 1), right)
            here = get(p, n)
            drop = None if around_n is None else -0.5 * around_n
            h_p.append(plus(here, drop))
        m_h = [m_p[0] - m_p[1]]
        for n in range(1, 2 * ITERS - 1 - step):
            m_h.append(m_p[n] - 0.5 * (m_p[n + 1] + m_p[n - 1]))
        bottom = p[0] * m_h[0]
        for n in range(1, step + 1):
            bottom = bottom + p[n] * m_h[n]
        alpha = rz / bottom
        x = [plus(get(x, n), alpha * p[n]) for n in range(step + 1)]
        y = [plus(get(y, n), -(alpha * h_p[n])) for n in range(step + 2)]
        if step + 1 < ITERS:
            m_y = [m_y[n] - alpha * m_h[n] for n in range(len(m_h))]
            rz_next = y[0] * m_y[0]
            for n in range(1, step + 2):
                rz_next = rz_next + y[n] * m_y[n]
            beta = rz_next / rz
            p = [plus(y[n], None if n > step else beta * p[n]) for n in range(step + 2)]
            m_p = [m_y[n] + beta * m_p[n] for n in range(len(m_y))]
            rz = rz_next
    mean = x[0] * ones[0]
    for n in range(1, ITERS):
        mean = mean + x[n] * ones[n]
    mean = mean / count
    xs = [jnp.broadcast_to(value, (8, ny)) for value in x]
    ys = [jnp.broadcast_to(value, (8, ny)) for value in y]
    mean = jnp.broadcast_to(mean, (8, ny))
    for slot in range(nz):
        target = flip(slot, side)
        for row in range(0, nx, 8):
            spot = slice(8 + row, 16 + row)
            weight = scale[slot, row : row + 8]
            total = jnp.where(weight > 0.0, -mean, 0.0)
            rest = ys[ITERS] * basis[ITERS, slot, spot]
            for n in range(ITERS):
                value = basis[n, slot, spot]
                total = total + xs[n] * value
                rest = rest + ys[n] * value
            phi[target, row : row + 8] = total
            residual[target, row : row + 8] = weight * rest


def hand_out(phi, residual, phi_out, residual_out, sems):
    copies = [
        pltpu.make_async_copy(phi, phi_out, sems.at[0]),
        pltpu.make_async_copy(residual, residual_out, sems.at[1]),
    ]
    for copy in copies:
        copy.start()
    for copy in copies:
        copy.wait()


def fast_body(potential, tissue_mask, layer_index, source):
    extent = tissue_mask.shape
    nz, nx, ny = extent
    sizes = tuple(lax.axis_size(axis) for axis in AXES)
    planes, held, deep = 2 * nz, nx + 16, nx + 32
    peers = math.prod(sizes)
    vmem = pl.BlockSpec(memory_space=pltpu.VMEM)
    hbm = pl.BlockSpec(memory_space=pltpu.HBM)

    def real(*shape):
        return pltpu.VMEM(shape + (ny,), jnp.float32)

    moves = 40
    inputs = (potential, tissue_mask, layer_index, source)
    scratch = [
        real(3, planes, held), pltpu.VMEM(extent, jnp.int32), real(3, 2, nx), real(2, 2, nz),
        real(2, 2, 2, nz), real(3, deep), real(3, deep), real(5, 2, deep),
        real(9, planes + 6, deep), real(18, planes + 2, held), real(ITERS + 1, planes + 2, held),
        real(2, planes + 2, held), real(4, 3, held), real(planes + 2, held),
        real(planes + 2, held), real(planes, nx), real(2, 2, COEFS, 8), real(3 * (ITERS + 1), 8),
        real(1), real(sizes[1] * sizes[2], 1), real(1), real(sizes[0], 1), real(1), real(peers, 1),
        pltpu.SMEM((LAYERS, 18), jnp.float32), pltpu.SMEM((planes + 1, COEFS), jnp.float32),
        pltpu.SMEM((nz,), jnp.int32), pltpu.SMEM((nz,), jnp.int32), pltpu.SMEM((planes,), jnp.int32),
        pltpu.SemaphoreType.DMA((4,)), pltpu.SemaphoreType.DMA((moves,)),
        pltpu.SemaphoreType.DMA((moves,)), pltpu.SemaphoreType.DMA((3,)),
        pltpu.SemaphoreType.DMA((3,)),
    ]
    shapes = (jax.ShapeDtypeStruct(extent, jnp.float32),) * 2
    found = pl.pallas_call(
        functools.partial(fast_kernel, extent, sizes),
        out_shape=shapes,
        in_specs=[hbm] * 4,
        out_specs=(vmem, vmem),
        scratch_shapes=scratch,
        compiler_params=pltpu.CompilerParams(
            vmem_limit_bytes=32 * 1024 * 1024, collective_id=0, has_side_effects=True
        ),
    )(*(pltpu.with_memory_space_constraint(ref, pltpu.HBM) for ref in inputs))
    return tuple(
        pl.pallas_call(
            hand_out,
            out_shape=shapes,
            in_specs=[vmem] * 2,
            out_specs=(hbm, hbm),
            scratch_shapes=[pltpu.SemaphoreType.DMA((2,))],
            compiler_params=pltpu.CompilerParams(vmem_limit_bytes=4 * 1024 * 1024),
        )(*found)
    )


def body(potential, tissue_mask, layer_index, source):
    nz, nx, ny = tissue_mask.shape
    fits = (
        lax.axis_size("gz") == 2 and nz == 8 and ITERS == 8 and nx % 8 == 0 and nx >= 16
        and ny == nz * GROUP and lax.axis_size("gx") > 1 and lax.axis_size("gy") > 1
    )
    return (fast_body if fits else general_body)(potential, tissue_mask, layer_index, source)


def solution(mesh):
    placed = (P("gz", "gx", "gy"), P("gz", "gx", "gy"), P("gz"), P("gz", "gx", "gy"))
    return jax.shard_map(
        body,
        mesh=mesh,
        in_specs=placed,
        out_specs=(P("gz", "gx", "gy"), P("gz", "gx", "gy")),
        check_vma=False,
    )
```

```python
import functools
import math

import jax
import jax.numpy as jnp
from jax import lax
from jax.experimental import pallas as pl
from jax.experimental.pallas import tpu as pltpu
from jax.sharding import PartitionSpec as P
import numpy as np

ITERS = 8
DEPTH = ITERS + 1
LAYERS = 16
AXES = ("gx", "gy", "gz")

OFFSETS = [
    (0, 1, 0),
    (0, 0, 1),
    (1, 0, 0),
    (0, 1, 1),
    (0, 1, -1),
    (1, 1, 0),
    (-1, 1, 0),
    (1, 0, 1),
    (-1, 0, 1),
]
bulk_long = 7.99
bulk_trans = 2.55
intra_long = 1.74
intra_trans = 0.19
bath_sigma = 5.0


def tensor_table(layers, longitudinal, transverse):
    depth = jnp.arange(layers, dtype=jnp.float32) / (layers - 1)
    helix = math.pi / 3.0 * (1.0 - 2.0 * depth)
    tilted = 0.35 * jnp.cos(math.pi * depth)
    fiber_x = jnp.cos(tilted) * jnp.cos(helix)
    fiber_y = jnp.cos(tilted) * jnp.sin(helix)
    fiber_z = jnp.sin(tilted)
    spread = longitudinal - transverse
    s_xx = transverse + spread * fiber_x * fiber_x
    s_yy = transverse + spread * fiber_y * fiber_y
    s_zz = transverse + spread * fiber_z * fiber_z
    s_xy = spread * fiber_x * fiber_y
    s_xz = spread * fiber_x * fiber_z
    s_yz = spread * fiber_y * fiber_z
    columns = [
        s_xx - jnp.abs(s_xy) - jnp.abs(s_xz),
        s_yy - jnp.abs(s_xy) - jnp.abs(s_yz),
        s_zz - jnp.abs(s_xz) - jnp.abs(s_yz),
        jnp.maximum(s_xy, 0.0),
        jnp.maximum(-s_xy, 0.0),
        jnp.maximum(s_xz, 0.0),
        jnp.maximum(-s_xz, 0.0),
        jnp.maximum(s_yz, 0.0),
        jnp.maximum(-s_yz, 0.0),
    ]
    return jnp.stack(columns, axis=1)


def shifted(value, axis, hop):
    count = lax.axis_size(axis)
    pairs = [(i + hop, i) for i in range(count) if 0 <= i + hop < count]
    return lax.ppermute(value, axis, pairs)


def framed(value, axis, dim, multiple):
    count, length = lax.axis_size(axis), value.shape[dim]
    if count == 1:
        return value
    if count == 2 and 2 * length <= length + 2 * DEPTH and multiple == 1:
        other = lax.ppermute(value, axis, [(0, 1), (1, 0)])
        return jnp.concatenate([value, other], axis=dim)
    after, before = [], []
    left, hop = DEPTH, 1
    while left > 0:
        width = min(left, length)
        if hop < count:
            after.append(
                shifted(lax.slice_in_dim(value, 0, width, axis=dim), axis, hop)
            )
            before.insert(
                0, shifted(lax.slice_in_dim(value, length - width, length, axis=dim), axis, -hop)
            )
        else:
            shape = list(value.shape)
            shape[dim] = width
            after.append(jnp.zeros(shape, value.dtype))
            before.insert(0, jnp.zeros(shape, value.dtype))
        left, hop = left - width, hop + 1
    gap = -(length + 2 * DEPTH) % multiple
    shape = list(value.shape)
    shape[dim] = gap
    middle = [jnp.zeros(shape, value.dtype)] if gap else []
    return jnp.concatenate([value] + after + middle + before, axis=dim)


def fields_around(ref, here, above, below, rows, lanes):
    def along_x(value, step):
        return pltpu.roll(value, (-step) % rows, 0)

    def along_y(value, step):
        return pltpu.roll(value, (-step) % lanes, 1)

    for dz, plane in ((0, here), (1, above), (-1, below)):
        value = ref[plane]
        if dz:
            yield (dz, 0, 0), value
        for step in (1, -1):
            yield (dz, step, 0), along_x(value, step)
        for step in (1, -1):
            moved = along_y(value, step)
            yield (dz, 0, step), moved
            if dz == 0:
                for other in (1, -1):
                    yield (0, other, step), along_x(moved, other)


SLOT = {}
for _column, _offset in enumerate(OFFSETS):
    SLOT[_offset] = (_column, 2 * _column)
    SLOT[tuple(-o for o in _offset)] = (_column, 2 * _column + 1)


def grid_kernel(extent, sizes, table, mask_in, potential_in, source_in, phi, residual,
                basis, scale, dots, weights, spare, first, second, jac,
                own_row, early, final_row, late, sends, early_recv, late_recv):
    mask, potential, source = mask_in, potential_in, source_in
    planes, rows, lanes = mask.shape
    nz, nx, ny = extent
    held = jac.shape[1]
    keep = nx + ITERS
    peers = math.prod(sizes)
    me = 0
    for axis, size in zip(AXES, sizes):
        me = me * size + lax.axis_index(axis)

    def device(index):
        return (index // (sizes[1] * sizes[2]), index // sizes[2] % sizes[1], index % sizes[2])

    def peer(k):
        return lax.rem(me + k, peers)

    barrier = pltpu.get_barrier_semaphore()

    def greet(k, carry):
        pl.semaphore_signal(
            barrier, inc=1, device_id=device(peer(k)), device_id_type=pl.DeviceIdType.MESH
        )
        return carry

    lax.fori_loop(1, peers, greet, 0)

    def spread(row, gathered, recv):
        def one(k, carry):
            pltpu.make_async_remote_copy(
                src_ref=row, dst_ref=gathered.at[me], send_sem=sends.at[k],
                recv_sem=recv.at[me], device_id=device(peer(k)),
                device_id_type=pl.DeviceIdType.MESH,
            ).start()
            return carry

        lax.fori_loop(1, peers, one, 0)

    def collect(row, gathered, recv):
        def one(k, carry):
            other = peer(k)
            copy = pltpu.make_async_remote_copy(
                src_ref=row, dst_ref=gathered.at[other], send_sem=sends.at[k],
                recv_sem=recv.at[other], device_id=device(other),
                device_id_type=pl.DeviceIdType.MESH,
            )
            copy.wait_recv()
            copy.wait_send()
            return carry

        lax.fori_loop(1, peers, one, 0)
        gathered[me] = row[...]
        return jnp.sum(gathered[...], axis=0)

    lane = lax.broadcasted_iota(jnp.int32, (1, 128), 1)

    def pick(vector, index):
        return jnp.sum(jnp.where(lane == index, vector, 0.0), axis=1, keepdims=True)

    cells = jnp.zeros((1, ny), jnp.float32)
    injected = jnp.zeros((1, ny), jnp.float32)
    for plane in range(nz):
        own_inside = jnp.where(mask_in[plane, 0:nx, 0:ny] > 0.0, 1.0, 0.0)
        cells = cells + jnp.sum(own_inside, axis=0, keepdims=True)
        injected = injected + jnp.sum(
            own_inside * source_in[plane, 0:nx, 0:ny], axis=0, keepdims=True
        )
    cells = jnp.sum(cells, axis=1, keepdims=True)
    injected = jnp.sum(injected, axis=1, keepdims=True)
    own_row[...] = jnp.where(lane == 0, cells, jnp.where(lane == 1, injected, 0.0))

    def neighbours(plane):
        above = jnp.where(plane + 1 == planes, 0, plane + 1)
        below = jnp.where(plane == 0, planes - 1, plane - 1)
        return above, below

    def store(ref, index, value):
        if held == rows:
            ref[index] = value
        else:
            ref[(*index, slice(0, keep))] = value[:keep]
            ref[(*index, slice(keep, held))] = value[rows - held + keep :]

    def setup(plane, carry):
        above, below = neighbours(plane)
        labels = mask[plane]
        tissue = jnp.where(labels == 2.0, 1.0, 0.0)
        bath = jnp.where(labels == 1.0, 1.0, 0.0)
        inside = tissue + bath
        volts = potential[plane]
        total = jnp.zeros((rows, lanes), jnp.float32)
        image = jnp.zeros((rows, lanes), jnp.float32)
        pairs = zip(
            fields_around(mask, plane, above, below, rows, lanes),
            fields_around(potential, plane, above, below, rows, lanes),
        )
        for (offset, label), (_, volt) in pairs:
            column, slot = SLOT[offset]
            beyond = {0: plane, 1: above, -1: below}[offset[0]]
            link = 0.5
            if offset[0] == 1:
                link = 0.5 * table[plane, 18]
            if offset[0] == -1:
                link = 0.5 * table[below, 18]
            their_tissue = jnp.where(label == 2.0, 1.0, 0.0)
            g_here, g_there = table[plane, column] * link, table[beyond, column] * link
            weight = tissue * g_here
            if column < 3:
                their_bath = jnp.where(label == 1.0, 1.0, 0.0)
                sigma = bath_sigma * link
                weight = inside * (
                    jnp.where(label > 0.0, weight + bath * sigma, 0.0)
                    + (their_tissue * g_there + their_bath * sigma)
                )
            else:
                weight = inside * (jnp.where(label > 0.0, weight, 0.0) + their_tissue * g_there)
            store(weights, (slot, plane), weight)
            total = total + weight
            intra = (table[plane, 9 + column] + table[beyond, 9 + column]) * link
            image = image + (tissue * their_tissue * intra) * (volts - volt)
        bounded = jnp.maximum(total, 1.0)
        jacobi = inside / bounded
        store(jac, (plane,), jacobi + jacobi)
        store(spare, (plane,), inside * (1.0 - jacobi * total))
        store(first, (plane,), jacobi * (inside * source[plane] - image))

        @pl.when(plane < nz)
        def _():
            scale[plane] = (inside * bounded)[:nx, :ny]

        return carry

    lax.fori_loop(0, planes // 2, setup, 0)
    pl.semaphore_wait(barrier, peers - 1)
    spread(own_row, early, early_recv)
    lax.fori_loop(planes // 2, planes, setup, 0)
    totals = collect(own_row, early, early_recv)
    count = pick(totals, 0)
    mean_rhs = pick(totals, 1) / count

    def centre(plane, carry):
        first[plane] = first[plane] - 0.5 * jac[plane] * mean_rhs
        return carry

    lax.fori_loop(0, planes, centre, 0)

    def record(step, now, before):
        rowsum = jnp.zeros((1, ny), jnp.float32)
        square, cross, plain = rowsum, rowsum, rowsum
        for plane in range(nz):
            value = now[plane, 0:nx, 0:ny]
            basis[step, plane] = value
            weighted = value * scale[plane]
            square = square + jnp.sum(weighted * value, axis=0, keepdims=True)
            if step:
                past = basis[step - 1, plane]
                cross = cross + jnp.sum(weighted * past, axis=0, keepdims=True)
            plain = plain + jnp.sum(value, axis=0, keepdims=True)
        if step < ITERS:
            dots[pl.ds(2 * step, 1)] = square
            dots[pl.ds(2 * ITERS + step, 1)] = plain
        if step:
            dots[pl.ds(2 * step - 1, 1)] = cross

    record(0, first, None)

    def apply(now, old, step):
        reach = ITERS - step
        if planes == nz:
            begin, span = 0, nz
        elif planes == sizes[2] * nz:
            begin = planes - lax.axis_index("gz") * reach
            span = min(planes, nz + reach)
        else:
            begin, span = planes - reach, nz + 2 * reach

        def one(index, carry):
            plane = lax.rem(begin + index, planes)
            above, below = neighbours(plane)
            total = jnp.zeros((held, lanes), jnp.float32)
            for offset, value in fields_around(now, plane, above, below, held, lanes):
                total = total + weights[SLOT[offset][1], plane] * value
            if step == 1:
                old[plane] = 0.5 * jac[plane] * total + spare[plane] * now[plane]
            else:
                old[plane] = (
                    jac[plane] * total + 2.0 * spare[plane] * now[plane] - old[plane]
                )
            return carry

        lax.fori_loop(0, span, one, 0)

    now, old = first, second
    for step in range(1, ITERS + 1):
        apply(now, old, step)
        now, old = old, now
        record(step, now, old)

    partial = jnp.sum(dots[...], axis=1, keepdims=True)
    diagonal = lax.broadcasted_iota(jnp.int32, (3 * ITERS, 128), 0) == lax.broadcasted_iota(
        jnp.int32, (3 * ITERS, 128), 1
    )
    final_row[...] = jnp.sum(jnp.where(diagonal, partial, 0.0), axis=0, keepdims=True)
    spread(final_row, late, late_recv)
    sums = collect(final_row, late, late_recv)

    def left(vector):
        return pltpu.roll(vector, 127, 1)

    def right(vector):
        return pltpu.roll(vector, 1, 1)

    mu0, mu1 = pick(sums, 0), pick(sums, 1)
    mu = jnp.where(lane < 2, sums, 2.0 * sums - jnp.where(lane % 2 == 0, mu0, mu1))
    mu = jnp.where(lane < 2 * ITERS, mu, 0.0)
    ones = pltpu.roll(sums, 128 - 2 * ITERS, 1)
    y = jnp.where(lane == 0, 1.0, 0.0)
    p = y
    m_y, m_p = mu, mu
    x = jnp.zeros((1, 128), jnp.float32)
    rz = mu0
    for step in range(ITERS):
        h_p = p - 0.5 * (left(p) + jnp.where(lane == 1, 2.0, 1.0) * right(p))
        h_p = jnp.where(lane <= ITERS, h_p, 0.0)
        before = jnp.where(lane == 0, left(m_p), right(m_p))
        m_h = m_p - 0.5 * (left(m_p) + before)
        alpha = rz / jnp.sum(jnp.where(lane < ITERS, p * m_h, 0.0), axis=1, keepdims=True)
        x = x + alpha * p
        y = y - alpha * h_p
        m_y = m_y - alpha * m_h
        if step + 1 < ITERS:
            rz_next = jnp.sum(jnp.where(lane < ITERS, y * m_y, 0.0), axis=1, keepdims=True)
            beta = rz_next / rz
            p = y + beta * p
            m_p = m_y + beta * m_p
            rz = rz_next
    mean = jnp.sum(jnp.where(lane < ITERS, x * ones, 0.0), axis=1, keepdims=True) / count
    xs = [pick(x, j) for j in range(ITERS)]
    ys = [pick(y, j) for j in range(ITERS + 1)]

    def one(plane, carry):
        weight = scale[plane]
        total = jnp.where(weight > 0.0, -mean, 0.0)
        rest = ys[ITERS] * basis[ITERS, plane]
        for j in range(ITERS):
            value = basis[j, plane]
            total = total + xs[j] * value
            rest = rest + ys[j] * value
        phi[plane] = total
        residual[plane] = weight * rest
        return carry

    lax.fori_loop(0, nz, one, 0)


def general_body(potential, tissue_mask, layer_index, source):
    extent = tissue_mask.shape
    nz = extent[0]
    labels = tissue_mask.astype(jnp.float32)
    sizes = tuple(lax.axis_size(axis) for axis in AXES)
    packed = jnp.stack([labels, potential, source], axis=1)
    packed = framed(packed, "gz", 0, 1)
    packed = framed(packed, "gx", 2, 8)
    packed = framed(packed, "gy", 3, 128)
    operands = (packed[:, 0], packed[:, 1], packed[:, 2])
    frame = operands[0].shape
    layers = framed(layer_index, "gz", 0, 1)
    planes = layers.shape[0]
    selector = (layers[:, None] == jnp.arange(LAYERS, dtype=jnp.int32)[None, :]).astype(
        jnp.float32
    )
    tables = jnp.concatenate(
        [
            tensor_table(LAYERS, bulk_long, bulk_trans),
            tensor_table(LAYERS, intra_long, intra_trans),
        ],
        axis=1,
    )
    table = jnp.dot(selector, tables, precision=lax.Precision.HIGHEST)
    size = lax.axis_size("gz")
    link = jnp.ones((planes, 1), jnp.float32)
    if planes == size * nz:
        place = (lax.axis_index("gz") * nz + jnp.arange(planes)) % planes
        link = (place + 1 < planes).astype(jnp.float32)[:, None]
    table = jnp.concatenate([table, link], axis=1)
    smem = pl.BlockSpec(memory_space=pltpu.SMEM)
    vmem = pl.BlockSpec(memory_space=pltpu.VMEM)
    compact = frame
    if extent[1] % 8 == 0 and ITERS % 8 == 0 and frame[1] > extent[1] + 2 * ITERS:
        compact = (planes, extent[1] + 2 * ITERS, frame[2])
    peers = math.prod(sizes)
    row = pltpu.VMEM((1, 128), jnp.float32)
    gathered = pltpu.VMEM((peers, 1, 128), jnp.float32)
    return tuple(
        pl.pallas_call(
            functools.partial(grid_kernel, extent, sizes),
            out_shape=(jax.ShapeDtypeStruct(extent, jnp.float32),) * 2,
            in_specs=[smem, vmem, vmem, vmem],
            out_specs=(vmem, vmem),
            scratch_shapes=[
                pltpu.VMEM((ITERS + 1,) + extent, jnp.float32),
                pltpu.VMEM(extent, jnp.float32),
                pltpu.VMEM((3 * ITERS, extent[2]), jnp.float32),
                pltpu.VMEM((18,) + compact, jnp.float32),
            ]
            + [pltpu.VMEM(compact, jnp.float32)] * 4
            + [row, gathered, row, gathered]
            + [pltpu.SemaphoreType.DMA((peers,))] * 3,
            compiler_params=pltpu.CompilerParams(
                vmem_limit_bytes=60 * 1024 * 1024, collective_id=0, has_side_effects=True
            ),
        )(table, *operands)
    )


GROUP = 16
TERMS_SAME = [(0, 1), (0, -1), (1, 0), (-1, 0), (1, 1), (1, -1), (-1, 1), (-1, -1)]
TERMS_SIDE = [(0, 0), (0, 1), (0, -1), (1, 0), (-1, 0)]
LEVEL = [0, 1, 3, 4]
STEEP = [(0, 0), (1, 0), (-1, 0), (0, 1), (0, -1)]
UPWARD = 2 * len(LEVEL)
COEFS = UPWARD + 1 + 3 * len(STEEP)


def numpy_table(longitudinal, transverse):
    depth = np.arange(LAYERS, dtype=np.float64) / (LAYERS - 1)
    helix = math.pi / 3.0 * (1.0 - 2.0 * depth)
    tilted = 0.35 * np.cos(math.pi * depth)
    fiber = (np.cos(tilted) * np.cos(helix), np.cos(tilted) * np.sin(helix), np.sin(tilted))
    spread = longitudinal - transverse
    s_xx, s_yy, s_zz = (transverse + spread * f * f for f in fiber)
    s_xy = spread * fiber[0] * fiber[1]
    s_xz = spread * fiber[0] * fiber[2]
    s_yz = spread * fiber[1] * fiber[2]
    columns = [s_xx - abs(s_xy) - abs(s_xz), s_yy - abs(s_xy) - abs(s_yz), s_zz - abs(s_xz) - abs(s_yz)]
    for value in (s_xy, s_xz, s_yz):
        columns += [np.maximum(value, 0.0), np.maximum(-value, 0.0)]
    return np.stack(columns, axis=1)


HALF_TABLE = 0.5 * np.concatenate(
    [numpy_table(bulk_long, bulk_trans), numpy_table(intra_long, intra_trans)], axis=1
)


def lane_roll(value, step):
    size = value.shape[1]
    return pltpu.roll(value, step % size if isinstance(step, int) else lax.rem(step + size, size), 1)


def row_roll(value, step):
    return pltpu.roll(value, step % value.shape[0], 0)


def tiled(value, rows):
    return jnp.concatenate([value] * (rows // value.shape[0]), axis=0)


def column_of(dz, dx, dy, side):
    same, flipped = SLOT[(dz, dx, dy)][0], SLOT[(-dz, dx, dy)][0]
    return same if same == flipped else same + side * (flipped - same)


def fast_kernel(extent, sizes, potential_in, mask_in, layers_in, source_in, phi, residual,
                fields, labels, packs, edge_send, edge_recv, from_after, from_before, strips,
                derived, weights, basis, moved, beside, jac, spare, scale, coef_lanes, dots,
                early_row, early_all, line_row, line_all, final_row, final_all,
                table, coefs, layers_own, layers_far, layers,
                loads, halo_send, halo_recv, sum_send, sum_recv, reached):
    nz, nx, ny = extent
    planes, held, deep = 2 * nz, nx + 16, nx + 32
    own = slice(8, 8 + nx)
    place = tuple(lax.axis_index(axis) for axis in AXES)
    gx, gy, side = place
    first_x, last_x = gx == 0, gx == sizes[0] - 1
    first_y, last_y = gy == 0, gy == sizes[1] - 1

    def exists(dx, dy):
        return (gx + dx >= 0) & (gx + dx < sizes[0]) & (gy + dy >= 0) & (gy + dy < sizes[1])

    def around(a, b, c):
        return tuple(
            lax.rem(here + step, size) if step else here
            for here, step, size in zip(place, (a, b, c), sizes)
        )

    slab = [(0, b, c) for b in range(sizes[1]) for c in range(sizes[2])]
    line = [(a, 0, 0) for a in range(sizes[0])]
    everyone = [(a, b, c) for a, _, _ in line for _, b, c in slab]
    corners = [(dx, dy) for dx in (1, -1) for dy in (1, -1)]

    def flip(slot, turned):
        return slot + turned * (nz - 1 - 2 * slot)

    get_layers = pltpu.make_async_copy(layers_in, layers_own, loads.at[0])
    get_mask = pltpu.make_async_copy(mask_in, labels, loads.at[1])
    get_layers.start()
    get_mask.start()
    whole = []
    for index, ref in ((1, potential_in), (2, source_in)):
        for plane in range(nz):
            pltpu.make_async_copy(
                ref.at[plane], fields.at[index, flip(plane, side), own], loads.at[1 + index]
            ).start()
        whole.append(pltpu.make_async_copy(ref, fields.at[index, 0:nz, own], loads.at[1 + index]))

    barrier = pltpu.get_barrier_semaphore()

    def greet(target):
        pl.semaphore_signal(
            barrier, inc=1, device_id=target, device_id_type=pl.DeviceIdType.MESH
        )

    expected = len(slab) - 1
    for dx, dy in corners + [(1, 0), (-1, 0)]:
        pl.when(exists(dx, dy))(lambda: greet((gx + dx, gy + dy, side)))
        expected = expected + jnp.where(exists(dx, dy), 1, 0)
    for step in slab[1:]:
        greet(around(*step))

    def clear(when, ref, index):
        @pl.when(when)
        def _():
            ref[index] = jnp.zeros(ref.at[index].shape, jnp.float32)

    every = slice(None)
    clear(first_x, fields, (every, slice(0, nz), slice(0, 8)))
    clear(last_x, fields, (every, slice(0, nz), slice(8 + nx, held)))
    for index in range(2):
        clear(first_x, edge_recv, (0, index, 0))
        clear(last_x, edge_recv, (0, index, 1))
    for ref, edge in ((from_after, last_y), (from_before, first_y)):
        clear(edge, ref, (every,))
        clear(first_x, ref, (every, slice(0, 16)))
        clear(last_x, ref, (every, slice(16 + nx, deep)))
    def lanes_of(rows):
        lane = lax.broadcasted_iota(jnp.int32, (rows, ny), 1)
        return lane, lane // GROUP, lane % GROUP

    lane = lax.broadcasted_iota(jnp.int32, (1, ny), 1)

    def pick(vector, index):
        return jnp.sum(jnp.where(lane == index, vector, 0.0), axis=1, keepdims=True)

    own_lane, _, _ = lanes_of(nx)
    later = (own_lane + 1) % ny // GROUP
    sooner = (own_lane + ny - 1) % ny // GROUP

    def pack(index):
        values = [fields[index, slot, own] for slot in range(nz)]
        turned = [lane_roll(value, GROUP * slot + 8) for slot, value in enumerate(values)]
        for toward, owner in ((0, later), (1, sooner)):
            total = turned[0]
            for slot in range(1, nz):
                total = jnp.where(owner == slot, turned[slot], total)
            packs[index, toward] = total
        if index < 2:
            for slot in range(nz):
                edge_send[index, 0, slot : slot + 1] = values[slot][8:9]
                edge_send[index, 1, slot : slot + 1] = values[slot][nx - 9 : nx - 8]

    def spread(number, row, gathered, targets):
        for index, step in enumerate(targets):
            if index:
                pltpu.make_async_remote_copy(
                    src_ref=row, dst_ref=gathered.at[index], send_sem=sum_send.at[number],
                    recv_sem=sum_recv.at[number], device_id=around(*step),
                    device_id_type=pl.DeviceIdType.MESH,
                ).start()

    def collect(number, row, gathered, targets):
        arrived = gathered.at[pl.ds(1, len(targets) - 1)]
        pltpu.make_async_copy(arrived, arrived, sum_recv.at[number]).wait()
        pltpu.make_async_copy(arrived, arrived, sum_send.at[number]).wait()
        gathered[0] = row[...]
        return jnp.sum(gathered[...], axis=0)

    def link(number, src, dst, target):
        return pltpu.make_async_remote_copy(
            src_ref=src, dst_ref=dst, send_sem=halo_send.at[number],
            recv_sem=halo_recv.at[number], device_id=target,
            device_id_type=pl.DeviceIdType.MESH,
        )

    other = (gx, gy, 1 - side)
    numbers = iter(range(64))

    def swap(src, dst):
        copy = link(next(numbers), src, dst, other)
        copy.start()
        return copy

    def exchange(picked, rows, edge):
        found = []

        def move(dx, dy, src, dst):
            copy = link(next(numbers), src, dst, (gx + dx, gy + dy, side))
            pl.when(exists(dx, dy))(copy.start)
            found.append((exists(-dx, -dy), exists(dx, dy), copy))

        for dx, dy in corners:
            into, toward = (from_before, 0) if dy == 1 else (from_after, 1)
            if dx == 1:
                move(dx, dy, packs.at[rows, toward, nx - 16 : nx], into.at[rows, 0:16])
            else:
                move(dx, dy, packs.at[rows, toward, 0:16], into.at[rows, 16 + nx : deep])
        move(0, 1, packs.at[rows, 0], from_before.at[rows, 16 : 16 + nx])
        move(0, -1, packs.at[rows, 1], from_after.at[rows, 16 : 16 + nx])
        move(1, 0, edge_send.at[edge, 1], edge_recv.at[0, edge, 0])
        move(-1, 0, edge_send.at[edge, 0], edge_recv.at[0, edge, 1])
        move(1, 0, fields.at[rows, 0:nz, nx : nx + 8], fields.at[rows, 0:nz, 0:8])
        move(-1, 0, fields.at[rows, 0:nz, 8:16], fields.at[rows, 0:nz, 8 + nx : held])
        return found

    groups = [(slice(0, 2), slice(0, 1), 0), (slice(2, 5), slice(1, 3), 1)]
    moves, relays = [], []

    def launch(picked, rows, edge):
        moves.append(exchange(picked, rows, edge))
        relays.append([swap(fields.at[rows, 0:nz, own], fields.at[rows, nz:planes, own])])

    def relay(picked, rows, edge):
        for receives, _, copy in moves[edge]:
            pl.when(receives)(copy.wait_recv)
        for index in range(rows.start, rows.stop):
            below, above = from_before[index], from_after[index]
            strips[2 * index, 0] = jnp.where(inner_deep < 8, below, above)
            if index < 2:
                strips[2 * index + 1, 0] = jnp.where(
                    inner_deep == 15, lane_roll(above, -1), lane_roll(below, 1)
                )
        relays[edge] += [
            swap(strips.at[picked, 0], strips.at[picked, 1]),
            swap(edge_recv.at[0, edge], edge_recv.at[1, edge]),
            swap(fields.at[rows, 0:nz, 0:8], fields.at[rows, nz:planes, 0:8]),
            swap(fields.at[rows, 0:nz, 8 + nx : held], fields.at[rows, nz:planes, 8 + nx : held]),
        ]

    get_mask.wait()
    get_layers.wait()
    for plane in range(nz):
        fields[0, flip(plane, side), own] = labels[plane].astype(jnp.float32)
    pack(0)
    pl.semaphore_wait(barrier, expected)
    layer_swap = swap(layers_own, layers_far)
    launch(*groups[0])
    for copy in whole:
        copy.wait()
    cells = jnp.zeros((8, ny), jnp.float32)
    injected = cells
    for slot in range(nz):
        for row in range(8, 8 + nx, 8):
            inside = jnp.where(fields[0, slot, row : row + 8] > 0.0, 1.0, 0.0)
            cells = cells + inside
            injected = injected + inside * fields[2, slot, row : row + 8]
    cells = jnp.sum(jnp.sum(cells, axis=0, keepdims=True), axis=1, keepdims=True)
    injected = jnp.sum(jnp.sum(injected, axis=0, keepdims=True), axis=1, keepdims=True)
    early_row[...] = jnp.where(lane == 0, cells, jnp.where(lane == 1, injected, 0.0))

    spread(0, early_row, early_all, slab)
    pack(1)
    pack(2)

    for layer in range(LAYERS):
        for column in range(18):
            table[layer, column] = jnp.float32(HALF_TABLE[layer, column])

    layer_swap.wait()
    for slot in range(nz):
        layers[slot] = layers_own[flip(slot, side)]
        layers[nz + slot] = layers_far[flip(slot, 1 - side)]

    def slot_of(j):
        return jnp.where(j < nz, j, 3 * nz - 1 - j)

    def coefficients(pair, carry):
        for slot in (2 * pair, 2 * pair + 1):
            j = slot_of(slot)
            layer = layers[slot]
            for n, k in enumerate(LEVEL):
                coefs[slot, 2 * n] = table[layer, k]
                coefs[slot, 2 * n + 1] = 2.0 * table[layer, 9 + k]
            near = j + 1 < planes
            there = layers[slot_of(jnp.where(near, j + 1, j))]
            open_ = jnp.where(near, 1.0, 0.0).astype(jnp.float32)
            coefs[slot, UPWARD] = 0.5 * bath_sigma * open_
            for n, (dx, dy) in enumerate(STEEP):
                k = column_of(1, dx, dy, side)
                coefs[slot, UPWARD + 1 + 3 * n] = table[layer, k] * open_
                coefs[slot, UPWARD + 2 + 3 * n] = table[there, k] * open_
                coefs[slot, UPWARD + 3 + 3 * n] = (table[layer, 9 + k] + table[there, 9 + k]) * open_
        return carry

    launch(*groups[1])
    lax.fori_loop(0, nz, coefficients, 0)
    for n in range(COEFS):
        coefs[planes, n] = jnp.float32(0.0)
    _, group8, _ = lanes_of(8)

    def at(j):
        return j if j < nz else 3 * nz - 1 - j

    def widen(block, carry):
        for n in [8 * block + m for m in range(8)]:
            for q in range(2):
                for which, shift in enumerate((0, -1)):
                    value = None
                    for g in range(nz):
                        j = at(q * nz + g) + shift
                        entry = coefs[planes if j < 0 else at(j), n]
                        if value is None:
                            value = jnp.full((8, ny), entry, jnp.float32)
                        else:
                            value = jnp.where(group8 == g, entry, value)
                    coef_lanes[which, q, n] = value
        return carry

    lax.fori_loop(0, COEFS // 8, widen, 0)

    lane_of, group_of, inner_deep = lanes_of(deep)
    relay(*groups[0])
    for dx in (1, -1):
        @pl.when(exists(dx, 0))
        def _():
            pl.semaphore_signal(
                reached, inc=1, device_id=(gx + dx, gy, side), device_id_type=pl.DeviceIdType.MESH
            )
    def ring_of(strip, g):
        return lane_roll(strip, -(GROUP * g + 8))

    def sides(value, ring):
        after = lane_roll(jnp.where(lane_of == 0, ring, value), -1)
        before = lane_roll(jnp.where(lane_of == ny - 1, ring, value), 1)
        return after, before

    def stored(index, number, slot, value):
        if index:
            derived[3 * number + 2, slot] = value
        else:
            derived[3 * number, slot] = jnp.where(value == 2.0, 1.0, 0.0)
            derived[3 * number + 1, slot] = jnp.where(value > 0.0, 1.0, 0.0)

    def framed_plane(index, q, g):
        before = jnp.broadcast_to(edge_recv[q, index, 0, pl.ds(g, 1)], (8, ny))
        after = jnp.broadcast_to(edge_recv[q, index, 1, pl.ds(g, 1)], (8, ny))
        return jnp.concatenate([before, fields[index, q * nz + g], after], axis=0)

    def derive_plane(index, q, g, mixed, ring):
        value = framed_plane(index, q, g)
        for number, part in enumerate((value,) + sides(value, ring)):
            stored(index, number, q * nz + g, part)
        return jnp.where(group_of == g, lane_roll(value, GROUP * g + 8), mixed)

    def derive_strip(index, q, mixed):
        strip, edge = strips[2 * index, q], strips[2 * index + 1, q]
        after = lane_roll(jnp.where(inner_deep == 8, mixed, strip), -1)
        before = lane_roll(jnp.where(inner_deep == 7, mixed, strip), 1)
        stored(index, 0, planes + q, strip)
        stored(index, 1, planes + q, jnp.where(inner_deep == 15, edge, after))
        stored(index, 2, planes + q, jnp.where(inner_deep == 0, edge, before))

    def derive_beside(index):
        for number in ((2, 5, 8) if index else (0, 1, 3, 4, 6, 7)):
            found = across(derived[number, planes], derived[number, planes + 1])
            for shift, value in enumerate(found):
                derived[number, planes + 2 + shift] = value

    def across(lower, upper):
        up0 = jnp.where(group_of == nz - 1, upper, lane_roll(lower, -GROUP))
        up1 = lane_roll(upper, GROUP)
        down0 = lane_roll(lower, GROUP)
        down1 = jnp.where(group_of == nz - 1, lower, lane_roll(upper, -GROUP))
        return up0, up1, down0, down1

    def level_of(coef):
        return {k: (coef(1, 2 * n), coef(1, 2 * n + 1)) for n, k in enumerate(LEVEL)}

    def steep_of(coef, dz):
        entries = {}
        for n, (dx, dy) in enumerate(STEEP):
            here, there, intra = (coef(dz, UPWARD + 1 + 3 * n + m) for m in range(3))
            if dz == 1:
                entries[(dx, dy)] = here, there, intra
            else:
                entries[(-dx, -dy)] = there, here, intra
        return coef(dz, UPWARD), entries

    middle = slice(8, 8 + held)

    def by(value, factor):
        if isinstance(factor, float) or factor.ndim == 0:
            return value * factor
        return value * tiled(factor, value.shape[0])

    def gathered_terms(edges, full):
        sums = edges(tuple(value[middle] for value in full), middle, 0, TERMS_SAME, 0)
        high = tuple(row_roll(value, 1)[8:deep] for value in full)
        part = edges(high, slice(8, deep), 1, TERMS_SIDE, 8)
        sums = sums + row_roll(part, -1)[0:held]
        low = tuple(row_roll(value, -1)[0 : 8 + held] for value in full)
        part = edges(low, slice(0, 8 + held), -1, TERMS_SIDE, 13)
        return sums + row_roll(part, 1)[middle]

    def weigh(slot, above, below, coef):
        level, slopes = level_of(coef), {1: steep_of(coef, 1), -1: steep_of(coef, -1)}
        base_bath = 0.5 * bath_sigma
        neighbour = {0: slot, 1: above, -1: below}

        def fetch(dz, dy, rows):
            number = {0: 0, 1: 1, -1: 2}[dy]
            return tuple(derived[3 * number + m, neighbour[dz], rows] for m in range(2))

        def edges(centre, rows, dx, terms, first):
            t, i = centre
            total = None
            keep = {0: slice(0, held), 1: slice(0, held), -1: slice(8, 8 + held)}[dx]
            for number, (dz, dy) in enumerate(terms):
                tn, i_n = fetch(dz, dy, rows)
                if dz == 0:
                    g_here = g_there = level[SLOT[(0, dx, dy)][0]][0]
                    bath = base_bath
                else:
                    bath, entries = slopes[dz]
                    g_here, g_there, _ = entries[(dx, dy)]
                if (dz != 0) + (dx != 0) + (dy != 0) == 1:
                    ours = by(t, g_here - bath) + by(i, bath)
                    theirs = by(tn, g_there - bath) + by(i_n, bath)
                else:
                    ours, theirs = by(t, g_here), by(tn, g_there)
                weight = i_n * ours + i * theirs
                weights[first + number, slot] = weight[keep]
                total = weight if total is None else total + weight
            return total

        full = fetch(0, 0, slice(0, deep))
        total = gathered_terms(edges, full)
        inside = full[1][middle]
        bounded = jnp.maximum(total, 1.0)
        jacobi = inside / bounded
        jac[slot] = jacobi + jacobi
        spare[slot] = 2.0 * (inside - inside * (jacobi * total))
        return (inside * bounded)[own]

    def begin(slot, above, below, coef, source):
        level, slopes = level_of(coef), {1: steep_of(coef, 1), -1: steep_of(coef, -1)}
        neighbour = {0: slot, 1: above, -1: below}

        def edges(centre, rows, dx, terms, first):
            v = centre[0]
            image = None
            for dz, dy in terms:
                number = {0: 0, 1: 1, -1: 2}[dy]
                tn = derived[3 * number, neighbour[dz], rows]
                vn = derived[3 * number + 2, neighbour[dz], rows]
                if dz == 0:
                    intra = level[SLOT[(0, dx, dy)][0]][1]
                else:
                    intra = slopes[dz][1][(dx, dy)][2]
                term = by(tn * (v - vn), intra)
                image = term if image is None else image + term
            return image

        image = gathered_terms(edges, (derived[2, slot],))
        tissue, inside = derived[0, slot, middle], derived[1, slot, middle]
        basis[0, slot] = 0.5 * jac[slot] * (inside * source - tissue * image)

    def beyond(slot):
        j = slot_of(slot)
        return slot_of(jnp.minimum(j + 1, planes - 1)), slot_of(jnp.maximum(j - 1, 0))

    def from_table(slot):
        j = slot_of(slot)
        under = jnp.where(j == 0, planes, slot_of(j - 1))
        return lambda dz, n: coefs[slot if dz == 1 else under, n]

    def from_lanes(q):
        return lambda dz, n: coef_lanes[0 if dz == 1 else 1, q, n]

    def plane_weigh(slot, carry):
        scale[slot] = weigh(slot, *beyond(slot), from_table(slot))
        return carry

    def strip_weigh(q, carry):
        slot = planes + q
        weigh(slot, slot + 2, slot + 4, from_lanes(q))
        return carry

    def label_half(q, carry):
        @pl.when(q == 1)
        def _():
            for copy in relays[0]:
                copy.wait_recv()
            line_row[...] = collect(0, early_row, early_all, slab)
            sides_x = jnp.where(exists(1, 0), 1, 0) + jnp.where(exists(-1, 0), 1, 0)
            pl.semaphore_wait(reached, sides_x)
            spread(1, line_row, line_all, line)

        mixed = strips[0, q]
        for g in range(nz):
            mixed = derive_plane(0, q, g, mixed, ring_of(strips[0, q], g))
        derive_strip(0, q, mixed)
        lax.fori_loop(q * (nz - 1), nz - 1 + q, plane_weigh, 0)
        return carry

    lax.fori_loop(0, 2, label_half, 0)
    relay(*groups[1])
    def derive_pair(q, pair, mixed):
        for g in (2 * pair, 2 * pair + 1):
            mixed = derive_plane(1, q, g, mixed, ring_of(strips[2, q], g))
        return mixed

    def far_weigh(pair, mixed):
        for m in range(2):
            plane_weigh(nz + 2 * pair + m, 0)
        return derive_pair(0, pair, mixed)

    mixed = lax.fori_loop(0, nz // 2, far_weigh, strips[2, 0])
    derive_strip(1, 0, mixed)
    derive_beside(0)
    lax.fori_loop(0, 2, strip_weigh, 0)
    for copy in relays[1]:
        copy.wait_recv()

    def plane_begin(slot, carry):
        begin(slot, *beyond(slot), from_table(slot), fields[2, slot])
        return carry

    def own_begin(pair, mixed):
        plane_begin(2 * pair, 0)
        plane_begin(jnp.minimum(2 * pair + 1, nz - 2), 0)
        return derive_pair(1, pair, mixed)

    def strip_begin(q, carry):
        slot = planes + q
        begin(slot, slot + 2, slot + 4, from_lanes(q), strips[4, q, middle])
        return carry

    mixed = lax.fori_loop(0, nz // 2, own_begin, strips[2, 1])
    derive_strip(1, 1, mixed)
    derive_beside(1)
    lax.fori_loop(nz - 1, planes, plane_begin, 0)
    lax.fori_loop(0, 2, strip_begin, 0)

    def folded(value):
        total = value[0:8]
        for row in range(8, value.shape[0], 8):
            total = total + value[row : row + 8]
        return total

    zero8 = jnp.zeros((8, ny), jnp.float32)

    def record(step, sums):
        for kind, value in enumerate(sums):
            dots[kind * (ITERS + 1) + step] = value

    totals = collect(1, line_row, line_all, line)
    count = pick(totals, 0)
    mean_rhs = pick(totals, 1) / count

    half_mean = 0.5 * mean_rhs
    sums = [zero8, zero8, zero8]
    for slot in range(planes + 2):
        value = basis[0, slot] - half_mean * jac[slot]
        basis[0, slot] = value
        if slot < nz:
            value = value[own]
            sums[0] = sums[0] + folded(value * value * scale[slot])
            sums[2] = sums[2] + folded(value)
    record(0, sums)

    lane_of, group_of, inner_held = lanes_of(held)

    def advance(step, slot, near, rows, first):
        same = None
        for number, (dz, dy) in enumerate(TERMS_SAME):
            value = near(dz, dy)
            if value is None:
                continue
            term = weights[number, slot, rows] * value[rows]
            same = term if same is None else same + term
        for dx, begin in ((1, 8), (-1, 13)):
            part = None
            for number, (dz, dy) in enumerate(TERMS_SIDE):
                value = near(dz, dy)
                if value is None:
                    continue
                term = weights[begin + number, slot] * value[...]
                part = term if part is None else part + term
            same = same + row_roll(part, -dx)[rows]
        value = basis[step - 1, slot, rows]
        fresh = jac[slot, rows] * same + spare[slot, rows] * value
        if first:
            factor = jnp.where(step == 1, 0.5, 1.0).astype(jnp.float32)
            back = jnp.where(step == 1, 0.0, 1.0).astype(jnp.float32)
            fresh = factor * fresh - back * basis[jnp.maximum(step - 2, 0), slot, rows]
        else:
            fresh = fresh - basis[step - 2, slot, rows]
        basis[step, slot, rows] = fresh
        return fresh, value

    LEAD = 4

    def roll_plane(field, j, ring):
        slot = at(j)
        moved[0, slot], moved[1, slot] = sides(field[slot], ring)

    def ring_plane(field, j):
        slot = at(j)
        return ring_of(field[planes + slot // nz], slot % nz)

    def one_step(step, last, first=False, final=False):
        now = basis.at[step - 1]
        entering = min(last + 1, planes)
        rings = {}

        def turn(j):
            if LEAD <= j < entering:
                rings[j] = ring_plane(now, j)

        def roll(j):
            if LEAD <= j < entering:
                roll_plane(now, j, rings.pop(j))

        mixed, triples = {}, {}

        def insert(q):
            total = now[planes + q]
            for g in range(nz):
                slot = q * nz + g
                j = slot if q == 0 else 3 * nz - 1 - slot
                if j <= last:
                    total = jnp.where(group_of == g, lane_roll(now[slot], GROUP * g + 8), total)
            mixed[q] = total

        def shift_strip(q):
            strip = now[planes + q]
            after = lane_roll(jnp.where(inner_held == 8, mixed[q], strip), -1)
            before = lane_roll(jnp.where(inner_held == 7, mixed[q], strip), 1)
            moved[0, planes + q], moved[1, planes + q] = after, before

        def cross(number):
            if number:
                found = across(moved[number - 1, planes], moved[number - 1, planes + 1])
            else:
                found = across(now[planes], now[planes + 1])
            for which, value in enumerate(found):
                beside[which, number] = value

        def advance_strip(q):
            slot = planes + q

            def near(dz, dy):
                number = {0: 0, 1: 1, -1: 2}[dy]
                if dz:
                    return beside.at[q if dz == 1 else 2 + q, number]
                return now.at[slot] if dy == 0 else moved.at[number - 1, slot]

            advance(step, slot, near, slice(0, held), first)

        coming = basis.at[step]
        plan = {
            0: [lambda: insert(0)],
            1: [lambda: insert(1)],
            2: [lambda: shift_strip(0), lambda: shift_strip(1)],
            3: [lambda: cross(0)],
            4: [lambda: cross(1)],
            5: [lambda: cross(2)],
            7: [lambda: advance_strip(0), lambda: advance_strip(1)],
            9: [lambda: rings.update({-1 - j: ring_plane(coming, j) for j in range(LEAD)})],
            10: [lambda: roll_plane(coming, 0, rings[-1]), lambda: roll_plane(coming, 1, rings[-2])],
            11: [lambda: roll_plane(coming, 2, rings[-3]), lambda: roll_plane(coming, 3, rings[-4])],
        }
        sums = [zero8, zero8, zero8]
        turn(LEAD)
        for j in range(last):
            turn(j + LEAD + 1)
            roll(j + LEAD)
            if not final:
                for work in plan.get(j, []):
                    work()
            slot = at(j)

            def near(dz, dy):
                if j + dz < 0:
                    return None
                spot = at(j + dz)
                return now.at[spot] if dy == 0 else moved.at[0 if dy == 1 else 1, spot]

            rows = own if final else slice(0, held)
            fresh, value = advance(step, slot, near, rows, first)
            if j < nz:
                if not final:
                    fresh, value = fresh[own], value[own]
                weighted = fresh * scale[slot]
                sums[0] = sums[0] + folded(weighted * fresh)
                sums[1] = sums[1] + folded(weighted * value)
                sums[2] = sums[2] + folded(fresh)
        record(step, sums)

    def early_steps(step, carry):
        one_step(step, planes - 1, first=True)
        return carry

    def later_steps(step, carry):
        one_step(step, planes - 4)
        return carry

    for j in range(LEAD):
        roll_plane(basis.at[0], j, ring_plane(basis.at[0], j))
    lax.fori_loop(1, 4, early_steps, 0)
    lax.fori_loop(4, ITERS, later_steps, 0)
    one_step(ITERS, nz, final=True)
    partial = jnp.sum(jnp.sum(dots[...], axis=1), axis=1, keepdims=True)
    entry = lax.broadcasted_iota(jnp.int32, (3 * (ITERS + 1), ny), 0)
    kind, index = entry // (ITERS + 1), entry % (ITERS + 1)
    place_of = jnp.where(kind == 0, 2 * index, jnp.where(kind == 1, 2 * index - 1, 2 * ITERS + 1 + index))
    wanted = place_of == lax.broadcasted_iota(jnp.int32, entry.shape, 1)
    final_row[...] = jnp.sum(jnp.where(wanted, partial, 0.0), axis=0, keepdims=True)
    spread(2, final_row, final_all, everyone)
    for group in moves:
        for _, sends, copy in group:
            pl.when(sends)(copy.wait_send)
    for group in relays:
        for copy in group:
            copy.wait_send()
    sums = collect(2, final_row, final_all, everyone)

    mu = [pick(sums, n) for n in range(2 * ITERS)]
    ones = [pick(sums, 2 * ITERS + 1 + n) for n in range(ITERS)]
    for n in range(2, 2 * ITERS):
        mu[n] = 2.0 * mu[n] - mu[n % 2]
    one = jnp.ones((1, 1), jnp.float32)
    y, p = [one], [one]
    m_y, m_p = list(mu), list(mu)
    x = []
    rz = mu[0]

    def plus(first, second):
        if first is None or second is None:
            return second if first is None else first
        return first + second

    def get(values, n):
        return values[n] if 0 <= n < len(values) else None

    for step in range(ITERS):
        h_p = []
        for n in range(step + 2):
            right = get(p, n - 1)
            if n == 1:
                right = right + right
            around_n = plus(get(p, n + 1), right)
            here = get(p, n)
            drop = None if around_n is None else -0.5 * around_n
            h_p.append(plus(here, drop))
        m_h = [m_p[0] - m_p[1]]
        for n in range(1, 2 * ITERS - 1 - step):
            m_h.append(m_p[n] - 0.5 * (m_p[n + 1] + m_p[n - 1]))
        bottom = p[0] * m_h[0]
        for n in range(1, step + 1):
            bottom = bottom + p[n] * m_h[n]
        alpha = rz / bottom
        x = [plus(get(x, n), alpha * p[n]) for n in range(step + 1)]
        y = [plus(get(y, n), -(alpha * h_p[n])) for n in range(step + 2)]
        if step + 1 < ITERS:
            m_y = [m_y[n] - alpha * m_h[n] for n in range(len(m_h))]
            rz_next = y[0] * m_y[0]
            for n in range(1, step + 2):
                rz_next = rz_next + y[n] * m_y[n]
            beta = rz_next / rz
            p = [plus(y[n], None if n > step else beta * p[n]) for n in range(step + 2)]
            m_p = [m_y[n] + beta * m_p[n] for n in range(len(m_y))]
            rz = rz_next
    mean = x[0] * ones[0]
    for n in range(1, ITERS):
        mean = mean + x[n] * ones[n]
    mean = mean / count
    xs = [jnp.broadcast_to(value, (8, ny)) for value in x]
    ys = [jnp.broadcast_to(value, (8, ny)) for value in y]
    mean = jnp.broadcast_to(mean, (8, ny))
    for slot in range(nz):
        target = flip(slot, side)
        for row in range(0, nx, 8):
            spot = slice(8 + row, 16 + row)
            weight = scale[slot, row : row + 8]
            total = jnp.where(weight > 0.0, -mean, 0.0)
            rest = ys[ITERS] * basis[ITERS, slot, spot]
            for n in range(ITERS):
                value = basis[n, slot, spot]
                total = total + xs[n] * value
                rest = rest + ys[n] * value
            phi[target, row : row + 8] = total
            residual[target, row : row + 8] = weight * rest


def hand_out(phi, residual, phi_out, residual_out, sems):
    copies = [
        pltpu.make_async_copy(phi, phi_out, sems.at[0]),
        pltpu.make_async_copy(residual, residual_out, sems.at[1]),
    ]
    for copy in copies:
        copy.start()
    for copy in copies:
        copy.wait()


def fast_body(potential, tissue_mask, layer_index, source):
    extent = tissue_mask.shape
    nz, nx, ny = extent
    sizes = tuple(lax.axis_size(axis) for axis in AXES)
    planes, held, deep = 2 * nz, nx + 16, nx + 32
    peers = math.prod(sizes)
    vmem = pl.BlockSpec(memory_space=pltpu.VMEM)
    hbm = pl.BlockSpec(memory_space=pltpu.HBM)

    def real(*shape):
        return pltpu.VMEM(shape + (ny,), jnp.float32)

    moves = 40
    inputs = (potential, tissue_mask, layer_index, source)
    scratch = [
        real(3, planes, held), pltpu.VMEM(extent, jnp.int32), real(3, 2, nx), real(2, 2, nz),
        real(2, 2, 2, nz), real(3, deep), real(3, deep), real(5, 2, deep),
        real(9, planes + 6, deep), real(18, planes + 2, held), real(ITERS + 1, planes + 2, held),
        real(2, planes + 2, held), real(4, 3, held), real(planes + 2, held),
        real(planes + 2, held), real(planes, nx), real(2, 2, COEFS, 8), real(3 * (ITERS + 1), 8),
        real(1), real(sizes[1] * sizes[2], 1), real(1), real(sizes[0], 1), real(1), real(peers, 1),
        pltpu.SMEM((LAYERS, 18), jnp.float32), pltpu.SMEM((planes + 1, COEFS), jnp.float32),
        pltpu.SMEM((nz,), jnp.int32), pltpu.SMEM((nz,), jnp.int32), pltpu.SMEM((planes,), jnp.int32),
        pltpu.SemaphoreType.DMA((4,)), pltpu.SemaphoreType.DMA((moves,)),
        pltpu.SemaphoreType.DMA((moves,)), pltpu.SemaphoreType.DMA((3,)),
        pltpu.SemaphoreType.DMA((3,)), pltpu.SemaphoreType.REGULAR,
    ]
    shapes = (jax.ShapeDtypeStruct(extent, jnp.float32),) * 2
    found = pl.pallas_call(
        functools.partial(fast_kernel, extent, sizes),
        out_shape=shapes,
        in_specs=[hbm] * 4,
        out_specs=(vmem, vmem),
        scratch_shapes=scratch,
        compiler_params=pltpu.CompilerParams(
            vmem_limit_bytes=32 * 1024 * 1024, collective_id=0, has_side_effects=True
        ),
    )(*(pltpu.with_memory_space_constraint(ref, pltpu.HBM) for ref in inputs))
    return tuple(
        pl.pallas_call(
            hand_out,
            out_shape=shapes,
            in_specs=[vmem] * 2,
            out_specs=(hbm, hbm),
            scratch_shapes=[pltpu.SemaphoreType.DMA((2,))],
            compiler_params=pltpu.CompilerParams(vmem_limit_bytes=4 * 1024 * 1024),
        )(*found)
    )


def body(potential, tissue_mask, layer_index, source):
    nz, nx, ny = tissue_mask.shape
    fits = (
        lax.axis_size("gz") == 2 and nz == 8 and ITERS == 8 and nx % 8 == 0 and nx >= 16
        and ny == nz * GROUP and 1 < lax.axis_size("gx") <= 4 and lax.axis_size("gy") > 1
    )
    return (fast_body if fits else general_body)(potential, tissue_mask, layer_index, source)


def solution(mesh):
    placed = (P("gz", "gx", "gy"), P("gz", "gx", "gy"), P("gz"), P("gz", "gx", "gy"))
    return jax.shard_map(
        body,
        mesh=mesh,
        in_specs=placed,
        out_specs=(P("gz", "gx", "gy"), P("gz", "gx", "gy")),
        check_vma=False,
    )
```

```python
import functools
import math

import jax
import jax.numpy as jnp
from jax import lax
from jax.experimental import pallas as pl
from jax.experimental.pallas import tpu as pltpu
from jax.sharding import PartitionSpec as P
import numpy as np

ITERS = 8
DEPTH = ITERS + 1
LAYERS = 16
AXES = ("gx", "gy", "gz")

OFFSETS = [
    (0, 1, 0),
    (0, 0, 1),
    (1, 0, 0),
    (0, 1, 1),
    (0, 1, -1),
    (1, 1, 0),
    (-1, 1, 0),
    (1, 0, 1),
    (-1, 0, 1),
]
bulk_long = 7.99
bulk_trans = 2.55
intra_long = 1.74
intra_trans = 0.19
bath_sigma = 5.0


def tensor_table(layers, longitudinal, transverse):
    depth = jnp.arange(layers, dtype=jnp.float32) / (layers - 1)
    helix = math.pi / 3.0 * (1.0 - 2.0 * depth)
    tilted = 0.35 * jnp.cos(math.pi * depth)
    fiber_x = jnp.cos(tilted) * jnp.cos(helix)
    fiber_y = jnp.cos(tilted) * jnp.sin(helix)
    fiber_z = jnp.sin(tilted)
    spread = longitudinal - transverse
    s_xx = transverse + spread * fiber_x * fiber_x
    s_yy = transverse + spread * fiber_y * fiber_y
    s_zz = transverse + spread * fiber_z * fiber_z
    s_xy = spread * fiber_x * fiber_y
    s_xz = spread * fiber_x * fiber_z
    s_yz = spread * fiber_y * fiber_z
    columns = [
        s_xx - jnp.abs(s_xy) - jnp.abs(s_xz),
        s_yy - jnp.abs(s_xy) - jnp.abs(s_yz),
        s_zz - jnp.abs(s_xz) - jnp.abs(s_yz),
        jnp.maximum(s_xy, 0.0),
        jnp.maximum(-s_xy, 0.0),
        jnp.maximum(s_xz, 0.0),
        jnp.maximum(-s_xz, 0.0),
        jnp.maximum(s_yz, 0.0),
        jnp.maximum(-s_yz, 0.0),
    ]
    return jnp.stack(columns, axis=1)


def shifted(value, axis, hop):
    count = lax.axis_size(axis)
    pairs = [(i + hop, i) for i in range(count) if 0 <= i + hop < count]
    return lax.ppermute(value, axis, pairs)


def framed(value, axis, dim, multiple):
    count, length = lax.axis_size(axis), value.shape[dim]
    if count == 1:
        return value
    if count == 2 and 2 * length <= length + 2 * DEPTH and multiple == 1:
        other = lax.ppermute(value, axis, [(0, 1), (1, 0)])
        return jnp.concatenate([value, other], axis=dim)
    after, before = [], []
    left, hop = DEPTH, 1
    while left > 0:
        width = min(left, length)
        if hop < count:
            after.append(
                shifted(lax.slice_in_dim(value, 0, width, axis=dim), axis, hop)
            )
            before.insert(
                0, shifted(lax.slice_in_dim(value, length - width, length, axis=dim), axis, -hop)
            )
        else:
            shape = list(value.shape)
            shape[dim] = width
            after.append(jnp.zeros(shape, value.dtype))
            before.insert(0, jnp.zeros(shape, value.dtype))
        left, hop = left - width, hop + 1
    gap = -(length + 2 * DEPTH) % multiple
    shape = list(value.shape)
    shape[dim] = gap
    middle = [jnp.zeros(shape, value.dtype)] if gap else []
    return jnp.concatenate([value] + after + middle + before, axis=dim)


def fields_around(ref, here, above, below, rows, lanes):
    def along_x(value, step):
        return pltpu.roll(value, (-step) % rows, 0)

    def along_y(value, step):
        return pltpu.roll(value, (-step) % lanes, 1)

    for dz, plane in ((0, here), (1, above), (-1, below)):
        value = ref[plane]
        if dz:
            yield (dz, 0, 0), value
        for step in (1, -1):
            yield (dz, step, 0), along_x(value, step)
        for step in (1, -1):
            moved = along_y(value, step)
            yield (dz, 0, step), moved
            if dz == 0:
                for other in (1, -1):
                    yield (0, other, step), along_x(moved, other)


SLOT = {}
for _column, _offset in enumerate(OFFSETS):
    SLOT[_offset] = (_column, 2 * _column)
    SLOT[tuple(-o for o in _offset)] = (_column, 2 * _column + 1)


def grid_kernel(extent, sizes, table, mask_in, potential_in, source_in, phi, residual,
                basis, scale, dots, weights, spare, first, second, jac,
                own_row, early, final_row, late, sends, early_recv, late_recv):
    mask, potential, source = mask_in, potential_in, source_in
    planes, rows, lanes = mask.shape
    nz, nx, ny = extent
    held = jac.shape[1]
    keep = nx + ITERS
    peers = math.prod(sizes)
    me = 0
    for axis, size in zip(AXES, sizes):
        me = me * size + lax.axis_index(axis)

    def device(index):
        return (index // (sizes[1] * sizes[2]), index // sizes[2] % sizes[1], index % sizes[2])

    def peer(k):
        return lax.rem(me + k, peers)

    barrier = pltpu.get_barrier_semaphore()

    def greet(k, carry):
        pl.semaphore_signal(
            barrier, inc=1, device_id=device(peer(k)), device_id_type=pl.DeviceIdType.MESH
        )
        return carry

    lax.fori_loop(1, peers, greet, 0)

    def spread(row, gathered, recv):
        def one(k, carry):
            pltpu.make_async_remote_copy(
                src_ref=row, dst_ref=gathered.at[me], send_sem=sends.at[k],
                recv_sem=recv.at[me], device_id=device(peer(k)),
                device_id_type=pl.DeviceIdType.MESH,
            ).start()
            return carry

        lax.fori_loop(1, peers, one, 0)

    def collect(row, gathered, recv):
        def one(k, carry):
            other = peer(k)
            copy = pltpu.make_async_remote_copy(
                src_ref=row, dst_ref=gathered.at[other], send_sem=sends.at[k],
                recv_sem=recv.at[other], device_id=device(other),
                device_id_type=pl.DeviceIdType.MESH,
            )
            copy.wait_recv()
            copy.wait_send()
            return carry

        lax.fori_loop(1, peers, one, 0)
        gathered[me] = row[...]
        return jnp.sum(gathered[...], axis=0)

    lane = lax.broadcasted_iota(jnp.int32, (1, 128), 1)

    def pick(vector, index):
        return jnp.sum(jnp.where(lane == index, vector, 0.0), axis=1, keepdims=True)

    cells = jnp.zeros((1, ny), jnp.float32)
    injected = jnp.zeros((1, ny), jnp.float32)
    for plane in range(nz):
        own_inside = jnp.where(mask_in[plane, 0:nx, 0:ny] > 0.0, 1.0, 0.0)
        cells = cells + jnp.sum(own_inside, axis=0, keepdims=True)
        injected = injected + jnp.sum(
            own_inside * source_in[plane, 0:nx, 0:ny], axis=0, keepdims=True
        )
    cells = jnp.sum(cells, axis=1, keepdims=True)
    injected = jnp.sum(injected, axis=1, keepdims=True)
    own_row[...] = jnp.where(lane == 0, cells, jnp.where(lane == 1, injected, 0.0))

    def neighbours(plane):
        above = jnp.where(plane + 1 == planes, 0, plane + 1)
        below = jnp.where(plane == 0, planes - 1, plane - 1)
        return above, below

    def store(ref, index, value):
        if held == rows:
            ref[index] = value
        else:
            ref[(*index, slice(0, keep))] = value[:keep]
            ref[(*index, slice(keep, held))] = value[rows - held + keep :]

    def setup(plane, carry):
        above, below = neighbours(plane)
        labels = mask[plane]
        tissue = jnp.where(labels == 2.0, 1.0, 0.0)
        bath = jnp.where(labels == 1.0, 1.0, 0.0)
        inside = tissue + bath
        volts = potential[plane]
        total = jnp.zeros((rows, lanes), jnp.float32)
        image = jnp.zeros((rows, lanes), jnp.float32)
        pairs = zip(
            fields_around(mask, plane, above, below, rows, lanes),
            fields_around(potential, plane, above, below, rows, lanes),
        )
        for (offset, label), (_, volt) in pairs:
            column, slot = SLOT[offset]
            beyond = {0: plane, 1: above, -1: below}[offset[0]]
            link = 0.5
            if offset[0] == 1:
                link = 0.5 * table[plane, 18]
            if offset[0] == -1:
                link = 0.5 * table[below, 18]
            their_tissue = jnp.where(label == 2.0, 1.0, 0.0)
            g_here, g_there = table[plane, column] * link, table[beyond, column] * link
            weight = tissue * g_here
            if column < 3:
                their_bath = jnp.where(label == 1.0, 1.0, 0.0)
                sigma = bath_sigma * link
                weight = inside * (
                    jnp.where(label > 0.0, weight + bath * sigma, 0.0)
                    + (their_tissue * g_there + their_bath * sigma)
                )
            else:
                weight = inside * (jnp.where(label > 0.0, weight, 0.0) + their_tissue * g_there)
            store(weights, (slot, plane), weight)
            total = total + weight
            intra = (table[plane, 9 + column] + table[beyond, 9 + column]) * link
            image = image + (tissue * their_tissue * intra) * (volts - volt)
        bounded = jnp.maximum(total, 1.0)
        jacobi = inside / bounded
        store(jac, (plane,), jacobi + jacobi)
        store(spare, (plane,), inside * (1.0 - jacobi * total))
        store(first, (plane,), jacobi * (inside * source[plane] - image))

        @pl.when(plane < nz)
        def _():
            scale[plane] = (inside * bounded)[:nx, :ny]

        return carry

    lax.fori_loop(0, planes // 2, setup, 0)
    pl.semaphore_wait(barrier, peers - 1)
    spread(own_row, early, early_recv)
    lax.fori_loop(planes // 2, planes, setup, 0)
    totals = collect(own_row, early, early_recv)
    count = pick(totals, 0)
    mean_rhs = pick(totals, 1) / count

    def centre(plane, carry):
        first[plane] = first[plane] - 0.5 * jac[plane] * mean_rhs
        return carry

    lax.fori_loop(0, planes, centre, 0)

    def record(step, now, before):
        rowsum = jnp.zeros((1, ny), jnp.float32)
        square, cross, plain = rowsum, rowsum, rowsum
        for plane in range(nz):
            value = now[plane, 0:nx, 0:ny]
            basis[step, plane] = value
            weighted = value * scale[plane]
            square = square + jnp.sum(weighted * value, axis=0, keepdims=True)
            if step:
                past = basis[step - 1, plane]
                cross = cross + jnp.sum(weighted * past, axis=0, keepdims=True)
            plain = plain + jnp.sum(value, axis=0, keepdims=True)
        if step < ITERS:
            dots[pl.ds(2 * step, 1)] = square
            dots[pl.ds(2 * ITERS + step, 1)] = plain
        if step:
            dots[pl.ds(2 * step - 1, 1)] = cross

    record(0, first, None)

    def apply(now, old, step):
        reach = ITERS - step
        if planes == nz:
            begin, span = 0, nz
        elif planes == sizes[2] * nz:
            begin = planes - lax.axis_index("gz") * reach
            span = min(planes, nz + reach)
        else:
            begin, span = planes - reach, nz + 2 * reach

        def one(index, carry):
            plane = lax.rem(begin + index, planes)
            above, below = neighbours(plane)
            total = jnp.zeros((held, lanes), jnp.float32)
            for offset, value in fields_around(now, plane, above, below, held, lanes):
                total = total + weights[SLOT[offset][1], plane] * value
            if step == 1:
                old[plane] = 0.5 * jac[plane] * total + spare[plane] * now[plane]
            else:
                old[plane] = (
                    jac[plane] * total + 2.0 * spare[plane] * now[plane] - old[plane]
                )
            return carry

        lax.fori_loop(0, span, one, 0)

    now, old = first, second
    for step in range(1, ITERS + 1):
        apply(now, old, step)
        now, old = old, now
        record(step, now, old)

    partial = jnp.sum(dots[...], axis=1, keepdims=True)
    diagonal = lax.broadcasted_iota(jnp.int32, (3 * ITERS, 128), 0) == lax.broadcasted_iota(
        jnp.int32, (3 * ITERS, 128), 1
    )
    final_row[...] = jnp.sum(jnp.where(diagonal, partial, 0.0), axis=0, keepdims=True)
    spread(final_row, late, late_recv)
    sums = collect(final_row, late, late_recv)

    def left(vector):
        return pltpu.roll(vector, 127, 1)

    def right(vector):
        return pltpu.roll(vector, 1, 1)

    mu0, mu1 = pick(sums, 0), pick(sums, 1)
    mu = jnp.where(lane < 2, sums, 2.0 * sums - jnp.where(lane % 2 == 0, mu0, mu1))
    mu = jnp.where(lane < 2 * ITERS, mu, 0.0)
    ones = pltpu.roll(sums, 128 - 2 * ITERS, 1)
    y = jnp.where(lane == 0, 1.0, 0.0)
    p = y
    m_y, m_p = mu, mu
    x = jnp.zeros((1, 128), jnp.float32)
    rz = mu0
    for step in range(ITERS):
        h_p = p - 0.5 * (left(p) + jnp.where(lane == 1, 2.0, 1.0) * right(p))
        h_p = jnp.where(lane <= ITERS, h_p, 0.0)
        before = jnp.where(lane == 0, left(m_p), right(m_p))
        m_h = m_p - 0.5 * (left(m_p) + before)
        alpha = rz / jnp.sum(jnp.where(lane < ITERS, p * m_h, 0.0), axis=1, keepdims=True)
        x = x + alpha * p
        y = y - alpha * h_p
        m_y = m_y - alpha * m_h
        if step + 1 < ITERS:
            rz_next = jnp.sum(jnp.where(lane < ITERS, y * m_y, 0.0), axis=1, keepdims=True)
            beta = rz_next / rz
            p = y + beta * p
            m_p = m_y + beta * m_p
            rz = rz_next
    mean = jnp.sum(jnp.where(lane < ITERS, x * ones, 0.0), axis=1, keepdims=True) / count
    xs = [pick(x, j) for j in range(ITERS)]
    ys = [pick(y, j) for j in range(ITERS + 1)]

    def one(plane, carry):
        weight = scale[plane]
        total = jnp.where(weight > 0.0, -mean, 0.0)
        rest = ys[ITERS] * basis[ITERS, plane]
        for j in range(ITERS):
            value = basis[j, plane]
            total = total + xs[j] * value
            rest = rest + ys[j] * value
        phi[plane] = total
        residual[plane] = weight * rest
        return carry

    lax.fori_loop(0, nz, one, 0)


def general_body(potential, tissue_mask, layer_index, source):
    extent = tissue_mask.shape
    nz = extent[0]
    labels = tissue_mask.astype(jnp.float32)
    sizes = tuple(lax.axis_size(axis) for axis in AXES)
    packed = jnp.stack([labels, potential, source], axis=1)
    packed = framed(packed, "gz", 0, 1)
    packed = framed(packed, "gx", 2, 8)
    packed = framed(packed, "gy", 3, 128)
    operands = (packed[:, 0], packed[:, 1], packed[:, 2])
    frame = operands[0].shape
    layers = framed(layer_index, "gz", 0, 1)
    planes = layers.shape[0]
    selector = (layers[:, None] == jnp.arange(LAYERS, dtype=jnp.int32)[None, :]).astype(
        jnp.float32
    )
    tables = jnp.concatenate(
        [
            tensor_table(LAYERS, bulk_long, bulk_trans),
            tensor_table(LAYERS, intra_long, intra_trans),
        ],
        axis=1,
    )
    table = jnp.dot(selector, tables, precision=lax.Precision.HIGHEST)
    size = lax.axis_size("gz")
    link = jnp.ones((planes, 1), jnp.float32)
    if planes == size * nz:
        place = (lax.axis_index("gz") * nz + jnp.arange(planes)) % planes
        link = (place + 1 < planes).astype(jnp.float32)[:, None]
    table = jnp.concatenate([table, link], axis=1)
    smem = pl.BlockSpec(memory_space=pltpu.SMEM)
    vmem = pl.BlockSpec(memory_space=pltpu.VMEM)
    compact = frame
    if extent[1] % 8 == 0 and ITERS % 8 == 0 and frame[1] > extent[1] + 2 * ITERS:
        compact = (planes, extent[1] + 2 * ITERS, frame[2])
    peers = math.prod(sizes)
    row = pltpu.VMEM((1, 128), jnp.float32)
    gathered = pltpu.VMEM((peers, 1, 128), jnp.float32)
    return tuple(
        pl.pallas_call(
            functools.partial(grid_kernel, extent, sizes),
            out_shape=(jax.ShapeDtypeStruct(extent, jnp.float32),) * 2,
            in_specs=[smem, vmem, vmem, vmem],
            out_specs=(vmem, vmem),
            scratch_shapes=[
                pltpu.VMEM((ITERS + 1,) + extent, jnp.float32),
                pltpu.VMEM(extent, jnp.float32),
                pltpu.VMEM((3 * ITERS, extent[2]), jnp.float32),
                pltpu.VMEM((18,) + compact, jnp.float32),
            ]
            + [pltpu.VMEM(compact, jnp.float32)] * 4
            + [row, gathered, row, gathered]
            + [pltpu.SemaphoreType.DMA((peers,))] * 3,
            compiler_params=pltpu.CompilerParams(
                vmem_limit_bytes=60 * 1024 * 1024, collective_id=0, has_side_effects=True
            ),
        )(table, *operands)
    )


GROUP = 16
TERMS_SAME = [(0, 1), (0, -1), (1, 0), (-1, 0), (1, 1), (1, -1), (-1, 1), (-1, -1)]
TERMS_SIDE = [(0, 0), (0, 1), (0, -1), (1, 0), (-1, 0)]
LEVEL = [0, 1, 3, 4]
STEEP = [(0, 0), (1, 0), (-1, 0), (0, 1), (0, -1)]
UPWARD = 2 * len(LEVEL)
COEFS = UPWARD + 1 + 3 * len(STEEP)


def numpy_table(longitudinal, transverse):
    depth = np.arange(LAYERS, dtype=np.float64) / (LAYERS - 1)
    helix = math.pi / 3.0 * (1.0 - 2.0 * depth)
    tilted = 0.35 * np.cos(math.pi * depth)
    fiber = (np.cos(tilted) * np.cos(helix), np.cos(tilted) * np.sin(helix), np.sin(tilted))
    spread = longitudinal - transverse
    s_xx, s_yy, s_zz = (transverse + spread * f * f for f in fiber)
    s_xy = spread * fiber[0] * fiber[1]
    s_xz = spread * fiber[0] * fiber[2]
    s_yz = spread * fiber[1] * fiber[2]
    columns = [s_xx - abs(s_xy) - abs(s_xz), s_yy - abs(s_xy) - abs(s_yz), s_zz - abs(s_xz) - abs(s_yz)]
    for value in (s_xy, s_xz, s_yz):
        columns += [np.maximum(value, 0.0), np.maximum(-value, 0.0)]
    return np.stack(columns, axis=1)


HALF_TABLE = 0.5 * np.concatenate(
    [numpy_table(bulk_long, bulk_trans), numpy_table(intra_long, intra_trans)], axis=1
)


def lane_roll(value, step):
    size = value.shape[1]
    return pltpu.roll(value, step % size if isinstance(step, int) else lax.rem(step + size, size), 1)


def row_roll(value, step):
    return pltpu.roll(value, step % value.shape[0], 0)


def tiled(value, rows):
    return jnp.concatenate([value] * (rows // value.shape[0]), axis=0)


def column_of(dz, dx, dy, side):
    same, flipped = SLOT[(dz, dx, dy)][0], SLOT[(-dz, dx, dy)][0]
    return same if same == flipped else same + side * (flipped - same)


def fast_kernel(extent, sizes, potential_in, mask_in, layers_in, source_in, phi, residual,
                fields, labels, packs, edge_send, edge_recv, from_after, from_before, strips,
                derived, weights, basis, moved, beside, jac, spare, scale, coef_lanes, dots,
                early_row, early_all, line_row, line_all, final_row, final_all,
                table, coefs, layers_own, layers_far, layers,
                loads, halo_send, halo_recv, sum_send, sum_recv, reached):
    nz, nx, ny = extent
    planes, held, deep = 2 * nz, nx + 16, nx + 32
    own = slice(8, 8 + nx)
    place = tuple(lax.axis_index(axis) for axis in AXES)
    gx, gy, side = place
    first_x, last_x = gx == 0, gx == sizes[0] - 1
    first_y, last_y = gy == 0, gy == sizes[1] - 1

    def exists(dx, dy):
        return (gx + dx >= 0) & (gx + dx < sizes[0]) & (gy + dy >= 0) & (gy + dy < sizes[1])

    def around(a, b, c):
        return tuple(
            lax.rem(here + step, size) if step else here
            for here, step, size in zip(place, (a, b, c), sizes)
        )

    slab = [(0, b, c) for b in range(sizes[1]) for c in range(sizes[2])]
    line = [(a, 0, 0) for a in range(sizes[0])]
    everyone = [(a, b, c) for a, _, _ in line for _, b, c in slab]
    corners = [(dx, dy) for dx in (1, -1) for dy in (1, -1)]

    def flip(slot, turned):
        return slot + turned * (nz - 1 - 2 * slot)

    get_layers = pltpu.make_async_copy(layers_in, layers_own, loads.at[0])
    get_mask = pltpu.make_async_copy(mask_in, labels, loads.at[1])
    get_mask.start()
    get_layers.start()
    barrier = pltpu.get_barrier_semaphore()

    def greet(target):
        pl.semaphore_signal(
            barrier, inc=1, device_id=target, device_id_type=pl.DeviceIdType.MESH
        )

    expected = len(slab) - 1
    for dx, dy in corners + [(1, 0), (-1, 0)]:
        pl.when(exists(dx, dy))(lambda: greet((gx + dx, gy + dy, side)))
        expected = expected + jnp.where(exists(dx, dy), 1, 0)
    for step in slab[1:]:
        greet(around(*step))

    whole = []
    for index, ref in ((1, potential_in), (2, source_in)):
        for plane in range(nz):
            pltpu.make_async_copy(
                ref.at[plane], fields.at[index, flip(plane, side), own], loads.at[1 + index]
            ).start()
        whole.append(pltpu.make_async_copy(ref, fields.at[index, 0:nz, own], loads.at[1 + index]))

    def clear(when, ref, index):
        @pl.when(when)
        def _():
            ref[index] = jnp.zeros(ref.at[index].shape, jnp.float32)

    every = slice(None)
    clear(first_x, fields, (every, slice(0, nz), slice(0, 8)))
    clear(last_x, fields, (every, slice(0, nz), slice(8 + nx, held)))
    for index in range(2):
        clear(first_x, edge_recv, (0, index, 0))
        clear(last_x, edge_recv, (0, index, 1))
    for ref, edge in ((from_after, last_y), (from_before, first_y)):
        clear(edge, ref, (every,))
        clear(first_x, ref, (every, slice(0, 16)))
        clear(last_x, ref, (every, slice(16 + nx, deep)))
    def lanes_of(rows):
        lane = lax.broadcasted_iota(jnp.int32, (rows, ny), 1)
        return lane, lane // GROUP, lane % GROUP

    lane = lax.broadcasted_iota(jnp.int32, (1, ny), 1)

    def pick(vector, index):
        return jnp.sum(jnp.where(lane == index, vector, 0.0), axis=1, keepdims=True)

    own_lane, _, _ = lanes_of(nx)
    later = (own_lane + 1) % ny // GROUP
    sooner = (own_lane + ny - 1) % ny // GROUP

    def pack(index):
        values = [fields[index, slot, own] for slot in range(nz)]
        turned = [lane_roll(value, GROUP * slot + 8) for slot, value in enumerate(values)]
        for toward, owner in ((0, later), (1, sooner)):
            total = turned[0]
            for slot in range(1, nz):
                total = jnp.where(owner == slot, turned[slot], total)
            packs[index, toward] = total
        if index < 2:
            for slot in range(nz):
                edge_send[index, 0, slot : slot + 1] = values[slot][8:9]
                edge_send[index, 1, slot : slot + 1] = values[slot][nx - 9 : nx - 8]

    def spread(number, row, gathered, targets):
        for index, step in enumerate(targets):
            if index:
                pltpu.make_async_remote_copy(
                    src_ref=row, dst_ref=gathered.at[index], send_sem=sum_send.at[number],
                    recv_sem=sum_recv.at[number], device_id=around(*step),
                    device_id_type=pl.DeviceIdType.MESH,
                ).start()

    def collect(number, row, gathered, targets):
        arrived = gathered.at[pl.ds(1, len(targets) - 1)]
        pltpu.make_async_copy(arrived, arrived, sum_recv.at[number]).wait()
        pltpu.make_async_copy(arrived, arrived, sum_send.at[number]).wait()
        gathered[0] = row[...]
        return jnp.sum(gathered[...], axis=0)

    def link(number, src, dst, target):
        return pltpu.make_async_remote_copy(
            src_ref=src, dst_ref=dst, send_sem=halo_send.at[number],
            recv_sem=halo_recv.at[number], device_id=target,
            device_id_type=pl.DeviceIdType.MESH,
        )

    other = (gx, gy, 1 - side)
    numbers = iter(range(64))

    def swap(src, dst):
        copy = link(next(numbers), src, dst, other)
        copy.start()
        return copy

    def exchange(picked, rows, edge):
        found = []

        def move(dx, dy, src, dst):
            copy = link(next(numbers), src, dst, (gx + dx, gy + dy, side))
            pl.when(exists(dx, dy))(copy.start)
            found.append((exists(-dx, -dy), exists(dx, dy), copy))

        for dx, dy in corners:
            into, toward = (from_before, 0) if dy == 1 else (from_after, 1)
            if dx == 1:
                move(dx, dy, packs.at[rows, toward, nx - 16 : nx], into.at[rows, 0:16])
            else:
                move(dx, dy, packs.at[rows, toward, 0:16], into.at[rows, 16 + nx : deep])
        move(0, 1, packs.at[rows, 0], from_before.at[rows, 16 : 16 + nx])
        move(0, -1, packs.at[rows, 1], from_after.at[rows, 16 : 16 + nx])
        move(1, 0, edge_send.at[edge, 1], edge_recv.at[0, edge, 0])
        move(-1, 0, edge_send.at[edge, 0], edge_recv.at[0, edge, 1])
        move(1, 0, fields.at[rows, 0:nz, nx : nx + 8], fields.at[rows, 0:nz, 0:8])
        move(-1, 0, fields.at[rows, 0:nz, 8:16], fields.at[rows, 0:nz, 8 + nx : held])
        return found

    groups = [(slice(0, 2), slice(0, 1), 0), (slice(2, 5), slice(1, 3), 1)]
    moves, relays = [], []

    def launch(picked, rows, edge):
        moves.append(exchange(picked, rows, edge))
        relays.append([swap(fields.at[rows, 0:nz, own], fields.at[rows, nz:planes, own])])

    def relay(picked, rows, edge):
        for receives, _, copy in moves[edge]:
            pl.when(receives)(copy.wait_recv)
        for index in range(rows.start, rows.stop):
            below, above = from_before[index], from_after[index]
            strips[2 * index, 0] = jnp.where(inner_deep < 8, below, above)
            if index < 2:
                strips[2 * index + 1, 0] = jnp.where(
                    inner_deep == 15, lane_roll(above, -1), lane_roll(below, 1)
                )
        relays[edge] += [
            swap(strips.at[picked, 0], strips.at[picked, 1]),
            swap(edge_recv.at[0, edge], edge_recv.at[1, edge]),
            swap(fields.at[rows, 0:nz, 0:8], fields.at[rows, nz:planes, 0:8]),
            swap(fields.at[rows, 0:nz, 8 + nx : held], fields.at[rows, nz:planes, 8 + nx : held]),
        ]

    get_mask.wait()
    get_layers.wait()
    for plane in range(nz):
        fields[0, flip(plane, side), own] = labels[plane].astype(jnp.float32)
    pack(0)
    pl.semaphore_wait(barrier, expected)
    layer_swap = swap(layers_own, layers_far)
    launch(*groups[0])
    for copy in whole:
        copy.wait()
    cells = jnp.zeros((8, ny), jnp.float32)
    injected = cells
    for slot in range(nz):
        for row in range(8, 8 + nx, 8):
            inside = jnp.where(fields[0, slot, row : row + 8] > 0.0, 1.0, 0.0)
            cells = cells + inside
            injected = injected + inside * fields[2, slot, row : row + 8]
    cells = jnp.sum(jnp.sum(cells, axis=0, keepdims=True), axis=1, keepdims=True)
    injected = jnp.sum(jnp.sum(injected, axis=0, keepdims=True), axis=1, keepdims=True)
    early_row[...] = jnp.where(lane == 0, cells, jnp.where(lane == 1, injected, 0.0))

    spread(0, early_row, early_all, slab)
    pack(1)
    pack(2)

    for layer in range(LAYERS):
        for column in range(18):
            table[layer, column] = jnp.float32(HALF_TABLE[layer, column])

    layer_swap.wait()
    for slot in range(nz):
        layers[slot] = layers_own[flip(slot, side)]
        layers[nz + slot] = layers_far[flip(slot, 1 - side)]

    def slot_of(j):
        return jnp.where(j < nz, j, 3 * nz - 1 - j)

    def coefficients(pair, carry):
        for slot in (2 * pair, 2 * pair + 1):
            j = slot_of(slot)
            layer = layers[slot]
            for n, k in enumerate(LEVEL):
                coefs[slot, 2 * n] = table[layer, k]
                coefs[slot, 2 * n + 1] = 2.0 * table[layer, 9 + k]
            near = j + 1 < planes
            there = layers[slot_of(jnp.where(near, j + 1, j))]
            open_ = jnp.where(near, 1.0, 0.0).astype(jnp.float32)
            coefs[slot, UPWARD] = 0.5 * bath_sigma * open_
            for n, (dx, dy) in enumerate(STEEP):
                k = column_of(1, dx, dy, side)
                coefs[slot, UPWARD + 1 + 3 * n] = table[layer, k] * open_
                coefs[slot, UPWARD + 2 + 3 * n] = table[there, k] * open_
                coefs[slot, UPWARD + 3 + 3 * n] = (table[layer, 9 + k] + table[there, 9 + k]) * open_
        return carry

    launch(*groups[1])
    lax.fori_loop(0, nz, coefficients, 0)
    for n in range(COEFS):
        coefs[planes, n] = jnp.float32(0.0)
    _, group8, _ = lanes_of(8)

    def at(j):
        return j if j < nz else 3 * nz - 1 - j

    def widen(block, carry):
        for n in [8 * block + m for m in range(8)]:
            for q in range(2):
                for which, shift in enumerate((0, -1)):
                    value = None
                    for g in range(nz):
                        j = at(q * nz + g) + shift
                        entry = coefs[planes if j < 0 else at(j), n]
                        if value is None:
                            value = jnp.full((8, ny), entry, jnp.float32)
                        else:
                            value = jnp.where(group8 == g, entry, value)
                    coef_lanes[which, q, n] = value
        return carry

    lax.fori_loop(0, COEFS // 8, widen, 0)

    lane_of, group_of, inner_deep = lanes_of(deep)
    relay(*groups[0])
    for dx in (1, -1):
        @pl.when(exists(dx, 0))
        def _():
            pl.semaphore_signal(
                reached, inc=1, device_id=(gx + dx, gy, side), device_id_type=pl.DeviceIdType.MESH
            )
    def ring_of(strip, g):
        return lane_roll(strip, -(GROUP * g + 8))

    def sides(value, ring):
        after = lane_roll(jnp.where(lane_of == 0, ring, value), -1)
        before = lane_roll(jnp.where(lane_of == ny - 1, ring, value), 1)
        return after, before

    def stored(index, number, slot, value):
        if index:
            derived[3 * number + 2, slot] = value
        else:
            derived[3 * number, slot] = jnp.where(value == 2.0, 1.0, 0.0)
            derived[3 * number + 1, slot] = jnp.where(value > 0.0, 1.0, 0.0)

    def framed_plane(index, q, g):
        before = jnp.broadcast_to(edge_recv[q, index, 0, pl.ds(g, 1)], (8, ny))
        after = jnp.broadcast_to(edge_recv[q, index, 1, pl.ds(g, 1)], (8, ny))
        return jnp.concatenate([before, fields[index, q * nz + g], after], axis=0)

    def derive_plane(index, q, g, mixed, ring):
        value = framed_plane(index, q, g)
        for number, part in enumerate((value,) + sides(value, ring)):
            stored(index, number, q * nz + g, part)
        return jnp.where(group_of == g, lane_roll(value, GROUP * g + 8), mixed)

    def derive_strip(index, q, mixed):
        strip, edge = strips[2 * index, q], strips[2 * index + 1, q]
        after = lane_roll(jnp.where(inner_deep == 8, mixed, strip), -1)
        before = lane_roll(jnp.where(inner_deep == 7, mixed, strip), 1)
        stored(index, 0, planes + q, strip)
        stored(index, 1, planes + q, jnp.where(inner_deep == 15, edge, after))
        stored(index, 2, planes + q, jnp.where(inner_deep == 0, edge, before))

    def derive_beside(index):
        for number in ((2, 5, 8) if index else (0, 1, 3, 4, 6, 7)):
            found = across(derived[number, planes], derived[number, planes + 1])
            for shift, value in enumerate(found):
                derived[number, planes + 2 + shift] = value

    def across(lower, upper):
        up0 = jnp.where(group_of == nz - 1, upper, lane_roll(lower, -GROUP))
        up1 = lane_roll(upper, GROUP)
        down0 = lane_roll(lower, GROUP)
        down1 = jnp.where(group_of == nz - 1, lower, lane_roll(upper, -GROUP))
        return up0, up1, down0, down1

    def level_of(coef):
        return {k: (coef(1, 2 * n), coef(1, 2 * n + 1)) for n, k in enumerate(LEVEL)}

    def steep_of(coef, dz):
        entries = {}
        for n, (dx, dy) in enumerate(STEEP):
            here, there, intra = (coef(dz, UPWARD + 1 + 3 * n + m) for m in range(3))
            if dz == 1:
                entries[(dx, dy)] = here, there, intra
            else:
                entries[(-dx, -dy)] = there, here, intra
        return coef(dz, UPWARD), entries

    middle = slice(8, 8 + held)

    def by(value, factor):
        if isinstance(factor, float) or factor.ndim == 0:
            return value * factor
        return value * tiled(factor, value.shape[0])

    def gathered_terms(edges, full):
        sums = edges(tuple(value[middle] for value in full), middle, 0, TERMS_SAME, 0)
        high = tuple(row_roll(value, 1)[8:deep] for value in full)
        part = edges(high, slice(8, deep), 1, TERMS_SIDE, 8)
        sums = sums + row_roll(part, -1)[0:held]
        low = tuple(row_roll(value, -1)[0 : 8 + held] for value in full)
        part = edges(low, slice(0, 8 + held), -1, TERMS_SIDE, 13)
        return sums + row_roll(part, 1)[middle]

    def weigh(slot, above, below, coef):
        level, slopes = level_of(coef), {1: steep_of(coef, 1), -1: steep_of(coef, -1)}
        base_bath = 0.5 * bath_sigma
        neighbour = {0: slot, 1: above, -1: below}

        def fetch(dz, dy, rows):
            number = {0: 0, 1: 1, -1: 2}[dy]
            return tuple(derived[3 * number + m, neighbour[dz], rows] for m in range(2))

        def edges(centre, rows, dx, terms, first):
            t, i = centre
            total = None
            keep = {0: slice(0, held), 1: slice(0, held), -1: slice(8, 8 + held)}[dx]
            for number, (dz, dy) in enumerate(terms):
                tn, i_n = fetch(dz, dy, rows)
                if dz == 0:
                    g_here = g_there = level[SLOT[(0, dx, dy)][0]][0]
                    bath = base_bath
                else:
                    bath, entries = slopes[dz]
                    g_here, g_there, _ = entries[(dx, dy)]
                if (dz != 0) + (dx != 0) + (dy != 0) == 1:
                    ours = by(t, g_here - bath) + by(i, bath)
                    theirs = by(tn, g_there - bath) + by(i_n, bath)
                else:
                    ours, theirs = by(t, g_here), by(tn, g_there)
                weight = i_n * ours + i * theirs
                weights[first + number, slot] = weight[keep]
                total = weight if total is None else total + weight
            return total

        full = fetch(0, 0, slice(0, deep))
        total = gathered_terms(edges, full)
        inside = full[1][middle]
        bounded = jnp.maximum(total, 1.0)
        jacobi = inside / bounded
        jac[slot] = jacobi + jacobi
        spare[slot] = 2.0 * (inside - inside * (jacobi * total))
        return (inside * bounded)[own]

    def begin(slot, above, below, coef, source):
        level, slopes = level_of(coef), {1: steep_of(coef, 1), -1: steep_of(coef, -1)}
        neighbour = {0: slot, 1: above, -1: below}

        def edges(centre, rows, dx, terms, first):
            v = centre[0]
            image = None
            for dz, dy in terms:
                number = {0: 0, 1: 1, -1: 2}[dy]
                tn = derived[3 * number, neighbour[dz], rows]
                vn = derived[3 * number + 2, neighbour[dz], rows]
                if dz == 0:
                    intra = level[SLOT[(0, dx, dy)][0]][1]
                else:
                    intra = slopes[dz][1][(dx, dy)][2]
                term = by(tn * (v - vn), intra)
                image = term if image is None else image + term
            return image

        image = gathered_terms(edges, (derived[2, slot],))
        tissue, inside = derived[0, slot, middle], derived[1, slot, middle]
        basis[0, slot] = 0.5 * jac[slot] * (inside * source - tissue * image)

    def beyond(slot):
        j = slot_of(slot)
        return slot_of(jnp.minimum(j + 1, planes - 1)), slot_of(jnp.maximum(j - 1, 0))

    def from_table(slot):
        j = slot_of(slot)
        under = jnp.where(j == 0, planes, slot_of(j - 1))
        return lambda dz, n: coefs[slot if dz == 1 else under, n]

    def from_lanes(q):
        return lambda dz, n: coef_lanes[0 if dz == 1 else 1, q, n]

    def plane_weigh(slot, carry):
        scale[slot] = weigh(slot, *beyond(slot), from_table(slot))
        return carry

    def strip_weigh(q, carry):
        slot = planes + q
        weigh(slot, slot + 2, slot + 4, from_lanes(q))
        return carry

    def label_half(q, carry):
        @pl.when(q == 1)
        def _():
            for copy in relays[0]:
                copy.wait_recv()
            line_row[...] = collect(0, early_row, early_all, slab)
            sides_x = jnp.where(exists(1, 0), 1, 0) + jnp.where(exists(-1, 0), 1, 0)
            pl.semaphore_wait(reached, sides_x)
            spread(1, line_row, line_all, line)

        mixed = strips[0, q]
        for g in range(nz):
            mixed = derive_plane(0, q, g, mixed, ring_of(strips[0, q], g))
        derive_strip(0, q, mixed)
        lax.fori_loop(q * (nz - 1), nz - 1 + q, plane_weigh, 0)
        return carry

    lax.fori_loop(0, 2, label_half, 0)
    relay(*groups[1])
    def derive_pair(q, pair, mixed):
        for g in (2 * pair, 2 * pair + 1):
            mixed = derive_plane(1, q, g, mixed, ring_of(strips[2, q], g))
        return mixed

    def far_weigh(pair, mixed):
        for m in range(2):
            plane_weigh(nz + 2 * pair + m, 0)
        return derive_pair(0, pair, mixed)

    mixed = lax.fori_loop(0, nz // 2, far_weigh, strips[2, 0])
    derive_strip(1, 0, mixed)
    derive_beside(0)
    lax.fori_loop(0, 2, strip_weigh, 0)
    for copy in relays[1]:
        copy.wait_recv()

    def plane_begin(slot, carry):
        begin(slot, *beyond(slot), from_table(slot), fields[2, slot])
        return carry

    def own_begin(pair, mixed):
        plane_begin(2 * pair, 0)
        plane_begin(jnp.minimum(2 * pair + 1, nz - 2), 0)
        return derive_pair(1, pair, mixed)

    def strip_begin(q, carry):
        slot = planes + q
        begin(slot, slot + 2, slot + 4, from_lanes(q), strips[4, q, middle])
        return carry

    mixed = lax.fori_loop(0, nz // 2, own_begin, strips[2, 1])
    derive_strip(1, 1, mixed)
    derive_beside(1)
    lax.fori_loop(nz - 1, planes, plane_begin, 0)
    lax.fori_loop(0, 2, strip_begin, 0)

    def folded(value):
        total = value[0:8]
        for row in range(8, value.shape[0], 8):
            total = total + value[row : row + 8]
        return total

    zero8 = jnp.zeros((8, ny), jnp.float32)

    def record(step, sums):
        for kind, value in enumerate(sums):
            dots[kind * (ITERS + 1) + step] = value

    totals = collect(1, line_row, line_all, line)
    count = pick(totals, 0)
    mean_rhs = pick(totals, 1) / count

    half_mean = 0.5 * mean_rhs
    sums = [zero8, zero8, zero8]
    for slot in range(planes + 2):
        value = basis[0, slot] - half_mean * jac[slot]
        basis[0, slot] = value
        if slot < nz:
            value = value[own]
            sums[0] = sums[0] + folded(value * value * scale[slot])
            sums[2] = sums[2] + folded(value)
    record(0, sums)

    lane_of, group_of, inner_held = lanes_of(held)

    tiles = held // 8

    def advance(step, slot, near, rows, first):
        kept = range(rows.start // 8, rows.stop // 8)
        same, plus, minus = [None] * tiles, [None] * tiles, [None] * tiles
        for t in range(max(kept.start - 1, 0), min(kept.stop + 1, tiles)):
            spot = slice(8 * t, 8 * t + 8)
            values = {}
            for key in TERMS_SIDE + TERMS_SAME:
                ref = near(*key)
                if ref is not None:
                    values[key] = ref[spot]
            for found, terms, begin_at, wanted in (
                (same, TERMS_SAME, 0, t in kept),
                (plus, TERMS_SIDE, 8, t >= kept.start),
                (minus, TERMS_SIDE, 13, t < kept.stop),
            ):
                for number, key in enumerate(terms):
                    if wanted and key in values:
                        term = weights[begin_at + number, slot, spot] * values[key]
                        found[t] = term if found[t] is None else found[t] + term

        def shifted_rows(found, step_by):
            filler = next(value for value in found if value is not None)
            whole = jnp.concatenate([filler if value is None else value for value in found], axis=0)
            return row_roll(whole, step_by)[rows]

        total = jnp.concatenate([same[t] for t in kept], axis=0)
        total = total + shifted_rows(plus, -1) + shifted_rows(minus, 1)
        value = basis[step - 1, slot, rows]
        fresh = jac[slot, rows] * total + spare[slot, rows] * value
        if first:
            factor = jnp.where(step == 1, 0.5, 1.0).astype(jnp.float32)
            back = jnp.where(step == 1, 0.0, 1.0).astype(jnp.float32)
            fresh = factor * fresh - back * basis[jnp.maximum(step - 2, 0), slot, rows]
        else:
            fresh = fresh - basis[step - 2, slot, rows]
        basis[step, slot, rows] = fresh
        return fresh, value

    LEAD = 3

    def roll_plane(field, j, ring):
        slot = at(j)
        moved[0, slot], moved[1, slot] = sides(field[slot], ring)

    def ring_plane(field, j):
        slot = at(j)
        return ring_of(field[planes + slot // nz], slot % nz)

    def one_step(step, last, first=False, final=False):
        now = basis.at[step - 1]
        entering = min(last + 1, planes)
        rings = {}

        def turn(j):
            if LEAD <= j < entering:
                rings[j] = ring_plane(now, j)

        def roll(j):
            if LEAD <= j < entering:
                roll_plane(now, j, rings.pop(j))

        mixed, triples = {}, {}

        def insert(q):
            total = now[planes + q]
            for g in range(nz):
                slot = q * nz + g
                j = slot if q == 0 else 3 * nz - 1 - slot
                if j <= last:
                    total = jnp.where(group_of == g, lane_roll(now[slot], GROUP * g + 8), total)
            mixed[q] = total

        def shift_strip(q):
            strip = now[planes + q]
            after = lane_roll(jnp.where(inner_held == 8, mixed[q], strip), -1)
            before = lane_roll(jnp.where(inner_held == 7, mixed[q], strip), 1)
            moved[0, planes + q], moved[1, planes + q] = after, before

        def cross(number):
            if number:
                found = across(moved[number - 1, planes], moved[number - 1, planes + 1])
            else:
                found = across(now[planes], now[planes + 1])
            for which, value in enumerate(found):
                beside[which, number] = value

        def advance_strip(q):
            slot = planes + q

            def near(dz, dy):
                number = {0: 0, 1: 1, -1: 2}[dy]
                if dz:
                    return beside.at[q if dz == 1 else 2 + q, number]
                return now.at[slot] if dy == 0 else moved.at[number - 1, slot]

            advance(step, slot, near, slice(0, held), first)

        coming = basis.at[step]
        plan = {
            0: [lambda: insert(0)],
            1: [lambda: shift_strip(0), lambda: insert(1)],
            2: [lambda: shift_strip(1), lambda: cross(0)],
            3: [lambda: cross(1)],
            4: [lambda: cross(2)],
            6: [lambda: advance_strip(0), lambda: advance_strip(1)],
            8: [lambda: rings.update({-1 - j: ring_plane(coming, j) for j in (0, 1)})],
            9: [
                lambda: roll_plane(coming, 0, rings[-1]),
                lambda: roll_plane(coming, 1, rings[-2]),
                lambda: rings.update({-3: ring_plane(coming, 2)}),
            ],
            10: [lambda: roll_plane(coming, 2, rings[-3])],
        }
        sums = [zero8, zero8, zero8]
        turn(LEAD)
        for j in range(last):
            turn(j + LEAD + 1)
            roll(j + LEAD)
            if not final:
                for work in plan.get(j, []):
                    work()
            slot = at(j)

            def near(dz, dy):
                if j + dz < 0:
                    return None
                spot = at(j + dz)
                return now.at[spot] if dy == 0 else moved.at[0 if dy == 1 else 1, spot]

            rows = own if final else slice(0, held)
            fresh, value = advance(step, slot, near, rows, first)
            if j < nz:
                if not final:
                    fresh, value = fresh[own], value[own]
                weighted = fresh * scale[slot]
                sums[0] = sums[0] + folded(weighted * fresh)
                sums[1] = sums[1] + folded(weighted * value)
                sums[2] = sums[2] + folded(fresh)
        record(step, sums)

    def early_steps(step, carry):
        one_step(step, planes - 1, first=True)
        return carry

    def later_steps(step, carry):
        one_step(step, planes - 4)
        return carry

    for j in range(LEAD):
        roll_plane(basis.at[0], j, ring_plane(basis.at[0], j))
    lax.fori_loop(1, 4, early_steps, 0)
    lax.fori_loop(4, ITERS, later_steps, 0)
    one_step(ITERS, nz, final=True)
    partial = jnp.sum(jnp.sum(dots[...], axis=1), axis=1, keepdims=True)
    entry = lax.broadcasted_iota(jnp.int32, (3 * (ITERS + 1), ny), 0)
    kind, index = entry // (ITERS + 1), entry % (ITERS + 1)
    place_of = jnp.where(kind == 0, 2 * index, jnp.where(kind == 1, 2 * index - 1, 2 * ITERS + 1 + index))
    wanted = place_of == lax.broadcasted_iota(jnp.int32, entry.shape, 1)
    final_row[...] = jnp.sum(jnp.where(wanted, partial, 0.0), axis=0, keepdims=True)
    spread(2, final_row, final_all, everyone)
    for group in moves:
        for _, sends, copy in group:
            pl.when(sends)(copy.wait_send)
    for group in relays:
        for copy in group:
            copy.wait_send()
    sums = collect(2, final_row, final_all, everyone)

    mu = [pick(sums, n) for n in range(2 * ITERS)]
    ones = [pick(sums, 2 * ITERS + 1 + n) for n in range(ITERS)]
    for n in range(2, 2 * ITERS):
        mu[n] = 2.0 * mu[n] - mu[n % 2]
    one = jnp.ones((1, 1), jnp.float32)
    y, p = [one], [one]
    m_y, m_p = list(mu), list(mu)
    x = []
    rz = mu[0]

    def plus(first, second):
        if first is None or second is None:
            return second if first is None else first
        return first + second

    def get(values, n):
        return values[n] if 0 <= n < len(values) else None

    for step in range(ITERS):
        h_p = []
        for n in range(step + 2):
            right = get(p, n - 1)
            if n == 1:
                right = right + right
            around_n = plus(get(p, n + 1), right)
            here = get(p, n)
            drop = None if around_n is None else -0.5 * around_n
            h_p.append(plus(here, drop))
        m_h = [m_p[0] - m_p[1]]
        for n in range(1, 2 * ITERS - 1 - step):
            m_h.append(m_p[n] - 0.5 * (m_p[n + 1] + m_p[n - 1]))
        bottom = p[0] * m_h[0]
        for n in range(1, step + 1):
            bottom = bottom + p[n] * m_h[n]
        alpha = rz / bottom
        x = [plus(get(x, n), alpha * p[n]) for n in range(step + 1)]
        y = [plus(get(y, n), -(alpha * h_p[n])) for n in range(step + 2)]
        if step + 1 < ITERS:
            m_y = [m_y[n] - alpha * m_h[n] for n in range(len(m_h))]
            rz_next = y[0] * m_y[0]
            for n in range(1, step + 2):
                rz_next = rz_next + y[n] * m_y[n]
            beta = rz_next / rz
            p = [plus(y[n], None if n > step else beta * p[n]) for n in range(step + 2)]
            m_p = [m_y[n] + beta * m_p[n] for n in range(len(m_y))]
            rz = rz_next
    mean = x[0] * ones[0]
    for n in range(1, ITERS):
        mean = mean + x[n] * ones[n]
    mean = mean / count
    xs = [jnp.broadcast_to(value, (8, ny)) for value in x]
    ys = [jnp.broadcast_to(value, (8, ny)) for value in y]
    mean = jnp.broadcast_to(mean, (8, ny))
    for slot in range(nz):
        target = flip(slot, side)
        for row in range(0, nx, 8):
            spot = slice(8 + row, 16 + row)
            weight = scale[slot, row : row + 8]
            total = jnp.where(weight > 0.0, -mean, 0.0)
            rest = ys[ITERS] * basis[ITERS, slot, spot]
            for n in range(ITERS):
                value = basis[n, slot, spot]
                total = total + xs[n] * value
                rest = rest + ys[n] * value
            phi[target, row : row + 8] = total
            residual[target, row : row + 8] = weight * rest


def hand_out(phi, residual, phi_out, residual_out, sems):
    copies = [
        pltpu.make_async_copy(phi, phi_out, sems.at[0]),
        pltpu.make_async_copy(residual, residual_out, sems.at[1]),
    ]
    for copy in copies:
        copy.start()
    for copy in copies:
        copy.wait()


def fast_body(potential, tissue_mask, layer_index, source):
    extent = tissue_mask.shape
    nz, nx, ny = extent
    sizes = tuple(lax.axis_size(axis) for axis in AXES)
    planes, held, deep = 2 * nz, nx + 16, nx + 32
    peers = math.prod(sizes)
    vmem = pl.BlockSpec(memory_space=pltpu.VMEM)
    hbm = pl.BlockSpec(memory_space=pltpu.HBM)

    def real(*shape):
        return pltpu.VMEM(shape + (ny,), jnp.float32)

    moves = 40
    inputs = (potential, tissue_mask, layer_index, source)
    scratch = [
        real(3, planes, held), pltpu.VMEM(extent, jnp.int32), real(3, 2, nx), real(2, 2, nz),
        real(2, 2, 2, nz), real(3, deep), real(3, deep), real(5, 2, deep),
        real(9, planes + 6, deep), real(18, planes + 2, held), real(ITERS + 1, planes + 2, held),
        real(2, planes + 2, held), real(4, 3, held), real(planes + 2, held),
        real(planes + 2, held), real(planes, nx), real(2, 2, COEFS, 8), real(3 * (ITERS + 1), 8),
        real(1), real(sizes[1] * sizes[2], 1), real(1), real(sizes[0], 1), real(1), real(peers, 1),
        pltpu.SMEM((LAYERS, 18), jnp.float32), pltpu.SMEM((planes + 1, COEFS), jnp.float32),
        pltpu.SMEM((nz,), jnp.int32), pltpu.SMEM((nz,), jnp.int32), pltpu.SMEM((planes,), jnp.int32),
        pltpu.SemaphoreType.DMA((4,)), pltpu.SemaphoreType.DMA((moves,)),
        pltpu.SemaphoreType.DMA((moves,)), pltpu.SemaphoreType.DMA((3,)),
        pltpu.SemaphoreType.DMA((3,)), pltpu.SemaphoreType.REGULAR,
    ]
    shapes = (jax.ShapeDtypeStruct(extent, jnp.float32),) * 2
    found = pl.pallas_call(
        functools.partial(fast_kernel, extent, sizes),
        out_shape=shapes,
        in_specs=[hbm] * 4,
        out_specs=(vmem, vmem),
        scratch_shapes=scratch,
        compiler_params=pltpu.CompilerParams(
            vmem_limit_bytes=32 * 1024 * 1024, collective_id=0, has_side_effects=True
        ),
    )(*(pltpu.with_memory_space_constraint(ref, pltpu.HBM) for ref in inputs))
    return tuple(
        pl.pallas_call(
            hand_out,
            out_shape=shapes,
            in_specs=[vmem] * 2,
            out_specs=(hbm, hbm),
            scratch_shapes=[pltpu.SemaphoreType.DMA((2,))],
            compiler_params=pltpu.CompilerParams(vmem_limit_bytes=4 * 1024 * 1024),
        )(*found)
    )


def body(potential, tissue_mask, layer_index, source):
    nz, nx, ny = tissue_mask.shape
    fits = (
        lax.axis_size("gz") == 2 and nz == 8 and ITERS == 8 and nx % 8 == 0 and nx >= 16
        and ny == nz * GROUP and 1 < lax.axis_size("gx") <= 4 and lax.axis_size("gy") > 1
    )
    return (fast_body if fits else general_body)(potential, tissue_mask, layer_index, source)


def solution(mesh):
    placed = (P("gz", "gx", "gy"), P("gz", "gx", "gy"), P("gz"), P("gz", "gx", "gy"))
    return jax.shard_map(
        body,
        mesh=mesh,
        in_specs=placed,
        out_specs=(P("gz", "gx", "gy"), P("gz", "gx", "gy")),
        check_vma=False,
    )
```

```python
import functools
import math

import jax
import jax.numpy as jnp
from jax import lax
from jax.experimental import pallas as pl
from jax.experimental.pallas import tpu as pltpu
from jax.sharding import PartitionSpec as P
import numpy as np

ITERS = 8
DEPTH = ITERS + 1
LAYERS = 16
AXES = ("gx", "gy", "gz")

OFFSETS = [
    (0, 1, 0),
    (0, 0, 1),
    (1, 0, 0),
    (0, 1, 1),
    (0, 1, -1),
    (1, 1, 0),
    (-1, 1, 0),
    (1, 0, 1),
    (-1, 0, 1),
]
bulk_long = 7.99
bulk_trans = 2.55
intra_long = 1.74
intra_trans = 0.19
bath_sigma = 5.0


def tensor_table(layers, longitudinal, transverse):
    depth = jnp.arange(layers, dtype=jnp.float32) / (layers - 1)
    helix = math.pi / 3.0 * (1.0 - 2.0 * depth)
    tilted = 0.35 * jnp.cos(math.pi * depth)
    fiber_x = jnp.cos(tilted) * jnp.cos(helix)
    fiber_y = jnp.cos(tilted) * jnp.sin(helix)
    fiber_z = jnp.sin(tilted)
    spread = longitudinal - transverse
    s_xx = transverse + spread * fiber_x * fiber_x
    s_yy = transverse + spread * fiber_y * fiber_y
    s_zz = transverse + spread * fiber_z * fiber_z
    s_xy = spread * fiber_x * fiber_y
    s_xz = spread * fiber_x * fiber_z
    s_yz = spread * fiber_y * fiber_z
    columns = [
        s_xx - jnp.abs(s_xy) - jnp.abs(s_xz),
        s_yy - jnp.abs(s_xy) - jnp.abs(s_yz),
        s_zz - jnp.abs(s_xz) - jnp.abs(s_yz),
        jnp.maximum(s_xy, 0.0),
        jnp.maximum(-s_xy, 0.0),
        jnp.maximum(s_xz, 0.0),
        jnp.maximum(-s_xz, 0.0),
        jnp.maximum(s_yz, 0.0),
        jnp.maximum(-s_yz, 0.0),
    ]
    return jnp.stack(columns, axis=1)


def shifted(value, axis, hop):
    count = lax.axis_size(axis)
    pairs = [(i + hop, i) for i in range(count) if 0 <= i + hop < count]
    return lax.ppermute(value, axis, pairs)


def framed(value, axis, dim, multiple):
    count, length = lax.axis_size(axis), value.shape[dim]
    if count == 1:
        return value
    if count == 2 and 2 * length <= length + 2 * DEPTH and multiple == 1:
        other = lax.ppermute(value, axis, [(0, 1), (1, 0)])
        return jnp.concatenate([value, other], axis=dim)
    after, before = [], []
    left, hop = DEPTH, 1
    while left > 0:
        width = min(left, length)
        if hop < count:
            after.append(
                shifted(lax.slice_in_dim(value, 0, width, axis=dim), axis, hop)
            )
            before.insert(
                0, shifted(lax.slice_in_dim(value, length - width, length, axis=dim), axis, -hop)
            )
        else:
            shape = list(value.shape)
            shape[dim] = width
            after.append(jnp.zeros(shape, value.dtype))
            before.insert(0, jnp.zeros(shape, value.dtype))
        left, hop = left - width, hop + 1
    gap = -(length + 2 * DEPTH) % multiple
    shape = list(value.shape)
    shape[dim] = gap
    middle = [jnp.zeros(shape, value.dtype)] if gap else []
    return jnp.concatenate([value] + after + middle + before, axis=dim)


def fields_around(ref, here, above, below, rows, lanes):
    def along_x(value, step):
        return pltpu.roll(value, (-step) % rows, 0)

    def along_y(value, step):
        return pltpu.roll(value, (-step) % lanes, 1)

    for dz, plane in ((0, here), (1, above), (-1, below)):
        value = ref[plane]
        if dz:
            yield (dz, 0, 0), value
        for step in (1, -1):
            yield (dz, step, 0), along_x(value, step)
        for step in (1, -1):
            moved = along_y(value, step)
            yield (dz, 0, step), moved
            if dz == 0:
                for other in (1, -1):
                    yield (0, other, step), along_x(moved, other)


SLOT = {}
for _column, _offset in enumerate(OFFSETS):
    SLOT[_offset] = (_column, 2 * _column)
    SLOT[tuple(-o for o in _offset)] = (_column, 2 * _column + 1)


def grid_kernel(extent, sizes, table, mask_in, potential_in, source_in, phi, residual,
                basis, scale, dots, weights, spare, first, second, jac,
                own_row, early, final_row, late, sends, early_recv, late_recv):
    mask, potential, source = mask_in, potential_in, source_in
    planes, rows, lanes = mask.shape
    nz, nx, ny = extent
    held = jac.shape[1]
    keep = nx + ITERS
    peers = math.prod(sizes)
    me = 0
    for axis, size in zip(AXES, sizes):
        me = me * size + lax.axis_index(axis)

    def device(index):
        return (index // (sizes[1] * sizes[2]), index // sizes[2] % sizes[1], index % sizes[2])

    def peer(k):
        return lax.rem(me + k, peers)

    barrier = pltpu.get_barrier_semaphore()

    def greet(k, carry):
        pl.semaphore_signal(
            barrier, inc=1, device_id=device(peer(k)), device_id_type=pl.DeviceIdType.MESH
        )
        return carry

    lax.fori_loop(1, peers, greet, 0)

    def spread(row, gathered, recv):
        def one(k, carry):
            pltpu.make_async_remote_copy(
                src_ref=row, dst_ref=gathered.at[me], send_sem=sends.at[k],
                recv_sem=recv.at[me], device_id=device(peer(k)),
                device_id_type=pl.DeviceIdType.MESH,
            ).start()
            return carry

        lax.fori_loop(1, peers, one, 0)

    def collect(row, gathered, recv):
        def one(k, carry):
            other = peer(k)
            copy = pltpu.make_async_remote_copy(
                src_ref=row, dst_ref=gathered.at[other], send_sem=sends.at[k],
                recv_sem=recv.at[other], device_id=device(other),
                device_id_type=pl.DeviceIdType.MESH,
            )
            copy.wait_recv()
            copy.wait_send()
            return carry

        lax.fori_loop(1, peers, one, 0)
        gathered[me] = row[...]
        return jnp.sum(gathered[...], axis=0)

    lane = lax.broadcasted_iota(jnp.int32, (1, 128), 1)

    def pick(vector, index):
        return jnp.sum(jnp.where(lane == index, vector, 0.0), axis=1, keepdims=True)

    cells = jnp.zeros((1, ny), jnp.float32)
    injected = jnp.zeros((1, ny), jnp.float32)
    for plane in range(nz):
        own_inside = jnp.where(mask_in[plane, 0:nx, 0:ny] > 0.0, 1.0, 0.0)
        cells = cells + jnp.sum(own_inside, axis=0, keepdims=True)
        injected = injected + jnp.sum(
            own_inside * source_in[plane, 0:nx, 0:ny], axis=0, keepdims=True
        )
    cells = jnp.sum(cells, axis=1, keepdims=True)
    injected = jnp.sum(injected, axis=1, keepdims=True)
    own_row[...] = jnp.where(lane == 0, cells, jnp.where(lane == 1, injected, 0.0))

    def neighbours(plane):
        above = jnp.where(plane + 1 == planes, 0, plane + 1)
        below = jnp.where(plane == 0, planes - 1, plane - 1)
        return above, below

    def store(ref, index, value):
        if held == rows:
            ref[index] = value
        else:
            ref[(*index, slice(0, keep))] = value[:keep]
            ref[(*index, slice(keep, held))] = value[rows - held + keep :]

    def setup(plane, carry):
        above, below = neighbours(plane)
        labels = mask[plane]
        tissue = jnp.where(labels == 2.0, 1.0, 0.0)
        bath = jnp.where(labels == 1.0, 1.0, 0.0)
        inside = tissue + bath
        volts = potential[plane]
        total = jnp.zeros((rows, lanes), jnp.float32)
        image = jnp.zeros((rows, lanes), jnp.float32)
        pairs = zip(
            fields_around(mask, plane, above, below, rows, lanes),
            fields_around(potential, plane, above, below, rows, lanes),
        )
        for (offset, label), (_, volt) in pairs:
            column, slot = SLOT[offset]
            beyond = {0: plane, 1: above, -1: below}[offset[0]]
            link = 0.5
            if offset[0] == 1:
                link = 0.5 * table[plane, 18]
            if offset[0] == -1:
                link = 0.5 * table[below, 18]
            their_tissue = jnp.where(label == 2.0, 1.0, 0.0)
            g_here, g_there = table[plane, column] * link, table[beyond, column] * link
            weight = tissue * g_here
            if column < 3:
                their_bath = jnp.where(label == 1.0, 1.0, 0.0)
                sigma = bath_sigma * link
                weight = inside * (
                    jnp.where(label > 0.0, weight + bath * sigma, 0.0)
                    + (their_tissue * g_there + their_bath * sigma)
                )
            else:
                weight = inside * (jnp.where(label > 0.0, weight, 0.0) + their_tissue * g_there)
            store(weights, (slot, plane), weight)
            total = total + weight
            intra = (table[plane, 9 + column] + table[beyond, 9 + column]) * link
            image = image + (tissue * their_tissue * intra) * (volts - volt)
        bounded = jnp.maximum(total, 1.0)
        jacobi = inside / bounded
        store(jac, (plane,), jacobi + jacobi)
        store(spare, (plane,), inside * (1.0 - jacobi * total))
        store(first, (plane,), jacobi * (inside * source[plane] - image))

        @pl.when(plane < nz)
        def _():
            scale[plane] = (inside * bounded)[:nx, :ny]

        return carry

    lax.fori_loop(0, planes // 2, setup, 0)
    pl.semaphore_wait(barrier, peers - 1)
    spread(own_row, early, early_recv)
    lax.fori_loop(planes // 2, planes, setup, 0)
    totals = collect(own_row, early, early_recv)
    count = pick(totals, 0)
    mean_rhs = pick(totals, 1) / count

    def centre(plane, carry):
        first[plane] = first[plane] - 0.5 * jac[plane] * mean_rhs
        return carry

    lax.fori_loop(0, planes, centre, 0)

    def record(step, now, before):
        rowsum = jnp.zeros((1, ny), jnp.float32)
        square, cross, plain = rowsum, rowsum, rowsum
        for plane in range(nz):
            value = now[plane, 0:nx, 0:ny]
            basis[step, plane] = value
            weighted = value * scale[plane]
            square = square + jnp.sum(weighted * value, axis=0, keepdims=True)
            if step:
                past = basis[step - 1, plane]
                cross = cross + jnp.sum(weighted * past, axis=0, keepdims=True)
            plain = plain + jnp.sum(value, axis=0, keepdims=True)
        if step < ITERS:
            dots[pl.ds(2 * step, 1)] = square
            dots[pl.ds(2 * ITERS + step, 1)] = plain
        if step:
            dots[pl.ds(2 * step - 1, 1)] = cross

    record(0, first, None)

    def apply(now, old, step):
        reach = ITERS - step
        if planes == nz:
            begin, span = 0, nz
        elif planes == sizes[2] * nz:
            begin = planes - lax.axis_index("gz") * reach
            span = min(planes, nz + reach)
        else:
            begin, span = planes - reach, nz + 2 * reach

        def one(index, carry):
            plane = lax.rem(begin + index, planes)
            above, below = neighbours(plane)
            total = jnp.zeros((held, lanes), jnp.float32)
            for offset, value in fields_around(now, plane, above, below, held, lanes):
                total = total + weights[SLOT[offset][1], plane] * value
            if step == 1:
                old[plane] = 0.5 * jac[plane] * total + spare[plane] * now[plane]
            else:
                old[plane] = (
                    jac[plane] * total + 2.0 * spare[plane] * now[plane] - old[plane]
                )
            return carry

        lax.fori_loop(0, span, one, 0)

    now, old = first, second
    for step in range(1, ITERS + 1):
        apply(now, old, step)
        now, old = old, now
        record(step, now, old)

    partial = jnp.sum(dots[...], axis=1, keepdims=True)
    diagonal = lax.broadcasted_iota(jnp.int32, (3 * ITERS, 128), 0) == lax.broadcasted_iota(
        jnp.int32, (3 * ITERS, 128), 1
    )
    final_row[...] = jnp.sum(jnp.where(diagonal, partial, 0.0), axis=0, keepdims=True)
    spread(final_row, late, late_recv)
    sums = collect(final_row, late, late_recv)

    def left(vector):
        return pltpu.roll(vector, 127, 1)

    def right(vector):
        return pltpu.roll(vector, 1, 1)

    mu0, mu1 = pick(sums, 0), pick(sums, 1)
    mu = jnp.where(lane < 2, sums, 2.0 * sums - jnp.where(lane % 2 == 0, mu0, mu1))
    mu = jnp.where(lane < 2 * ITERS, mu, 0.0)
    ones = pltpu.roll(sums, 128 - 2 * ITERS, 1)
    y = jnp.where(lane == 0, 1.0, 0.0)
    p = y
    m_y, m_p = mu, mu
    x = jnp.zeros((1, 128), jnp.float32)
    rz = mu0
    for step in range(ITERS):
        h_p = p - 0.5 * (left(p) + jnp.where(lane == 1, 2.0, 1.0) * right(p))
        h_p = jnp.where(lane <= ITERS, h_p, 0.0)
        before = jnp.where(lane == 0, left(m_p), right(m_p))
        m_h = m_p - 0.5 * (left(m_p) + before)
        alpha = rz / jnp.sum(jnp.where(lane < ITERS, p * m_h, 0.0), axis=1, keepdims=True)
        x = x + alpha * p
        y = y - alpha * h_p
        m_y = m_y - alpha * m_h
        if step + 1 < ITERS:
            rz_next = jnp.sum(jnp.where(lane < ITERS, y * m_y, 0.0), axis=1, keepdims=True)
            beta = rz_next / rz
            p = y + beta * p
            m_p = m_y + beta * m_p
            rz = rz_next
    mean = jnp.sum(jnp.where(lane < ITERS, x * ones, 0.0), axis=1, keepdims=True) / count
    xs = [pick(x, j) for j in range(ITERS)]
    ys = [pick(y, j) for j in range(ITERS + 1)]

    def one(plane, carry):
        weight = scale[plane]
        total = jnp.where(weight > 0.0, -mean, 0.0)
        rest = ys[ITERS] * basis[ITERS, plane]
        for j in range(ITERS):
            value = basis[j, plane]
            total = total + xs[j] * value
            rest = rest + ys[j] * value
        phi[plane] = total
        residual[plane] = weight * rest
        return carry

    lax.fori_loop(0, nz, one, 0)


def general_body(potential, tissue_mask, layer_index, source):
    extent = tissue_mask.shape
    nz = extent[0]
    labels = tissue_mask.astype(jnp.float32)
    sizes = tuple(lax.axis_size(axis) for axis in AXES)
    packed = jnp.stack([labels, potential, source], axis=1)
    packed = framed(packed, "gz", 0, 1)
    packed = framed(packed, "gx", 2, 8)
    packed = framed(packed, "gy", 3, 128)
    operands = (packed[:, 0], packed[:, 1], packed[:, 2])
    frame = operands[0].shape
    layers = framed(layer_index, "gz", 0, 1)
    planes = layers.shape[0]
    selector = (layers[:, None] == jnp.arange(LAYERS, dtype=jnp.int32)[None, :]).astype(
        jnp.float32
    )
    tables = jnp.concatenate(
        [
            tensor_table(LAYERS, bulk_long, bulk_trans),
            tensor_table(LAYERS, intra_long, intra_trans),
        ],
        axis=1,
    )
    table = jnp.dot(selector, tables, precision=lax.Precision.HIGHEST)
    size = lax.axis_size("gz")
    link = jnp.ones((planes, 1), jnp.float32)
    if planes == size * nz:
        place = (lax.axis_index("gz") * nz + jnp.arange(planes)) % planes
        link = (place + 1 < planes).astype(jnp.float32)[:, None]
    table = jnp.concatenate([table, link], axis=1)
    smem = pl.BlockSpec(memory_space=pltpu.SMEM)
    vmem = pl.BlockSpec(memory_space=pltpu.VMEM)
    compact = frame
    if extent[1] % 8 == 0 and ITERS % 8 == 0 and frame[1] > extent[1] + 2 * ITERS:
        compact = (planes, extent[1] + 2 * ITERS, frame[2])
    peers = math.prod(sizes)
    row = pltpu.VMEM((1, 128), jnp.float32)
    gathered = pltpu.VMEM((peers, 1, 128), jnp.float32)
    return tuple(
        pl.pallas_call(
            functools.partial(grid_kernel, extent, sizes),
            out_shape=(jax.ShapeDtypeStruct(extent, jnp.float32),) * 2,
            in_specs=[smem, vmem, vmem, vmem],
            out_specs=(vmem, vmem),
            scratch_shapes=[
                pltpu.VMEM((ITERS + 1,) + extent, jnp.float32),
                pltpu.VMEM(extent, jnp.float32),
                pltpu.VMEM((3 * ITERS, extent[2]), jnp.float32),
                pltpu.VMEM((18,) + compact, jnp.float32),
            ]
            + [pltpu.VMEM(compact, jnp.float32)] * 4
            + [row, gathered, row, gathered]
            + [pltpu.SemaphoreType.DMA((peers,))] * 3,
            compiler_params=pltpu.CompilerParams(
                vmem_limit_bytes=60 * 1024 * 1024, collective_id=0, has_side_effects=True
            ),
        )(table, *operands)
    )


GROUP = 16
TERMS_SAME = [(0, 1), (0, -1), (1, 0), (-1, 0), (1, 1), (1, -1), (-1, 1), (-1, -1)]
TERMS_SIDE = [(0, 0), (0, 1), (0, -1), (1, 0), (-1, 0)]
LEVEL = [0, 1, 3, 4]
STEEP = [(0, 0), (1, 0), (-1, 0), (0, 1), (0, -1)]
UPWARD = 2 * len(LEVEL)
COEFS = UPWARD + 1 + 3 * len(STEEP)


def numpy_table(longitudinal, transverse):
    depth = np.arange(LAYERS, dtype=np.float64) / (LAYERS - 1)
    helix = math.pi / 3.0 * (1.0 - 2.0 * depth)
    tilted = 0.35 * np.cos(math.pi * depth)
    fiber = (np.cos(tilted) * np.cos(helix), np.cos(tilted) * np.sin(helix), np.sin(tilted))
    spread = longitudinal - transverse
    s_xx, s_yy, s_zz = (transverse + spread * f * f for f in fiber)
    s_xy = spread * fiber[0] * fiber[1]
    s_xz = spread * fiber[0] * fiber[2]
    s_yz = spread * fiber[1] * fiber[2]
    columns = [s_xx - abs(s_xy) - abs(s_xz), s_yy - abs(s_xy) - abs(s_yz), s_zz - abs(s_xz) - abs(s_yz)]
    for value in (s_xy, s_xz, s_yz):
        columns += [np.maximum(value, 0.0), np.maximum(-value, 0.0)]
    return np.stack(columns, axis=1)


HALF_TABLE = 0.5 * np.concatenate(
    [numpy_table(bulk_long, bulk_trans), numpy_table(intra_long, intra_trans)], axis=1
)


def lane_roll(value, step):
    size = value.shape[1]
    return pltpu.roll(value, step % size if isinstance(step, int) else lax.rem(step + size, size), 1)


def row_roll(value, step):
    return pltpu.roll(value, step % value.shape[0], 0)


def tiled(value, rows):
    return jnp.concatenate([value] * (rows // value.shape[0]), axis=0)


def column_of(dz, dx, dy, side):
    same, flipped = SLOT[(dz, dx, dy)][0], SLOT[(-dz, dx, dy)][0]
    return same if same == flipped else same + side * (flipped - same)


def fast_kernel(extent, sizes, potential_in, mask_in, layers_in, source_in, phi, residual,
                fields, labels, packs, edge_send, edge_recv, from_after, from_before, strips,
                derived, weights, basis, moved, beside, jac, spare, scale, coef_lanes, dots,
                early_row, early_all, line_row, line_all, final_row, final_all,
                table, coefs, layers_own, layers_far, layers,
                loads, halo_send, halo_recv, sum_send, sum_recv, reached):
    nz, nx, ny = extent
    planes, held, deep = 2 * nz, nx + 16, nx + 32
    own = slice(8, 8 + nx)
    place = tuple(lax.axis_index(axis) for axis in AXES)
    gx, gy, side = place
    first_x, last_x = gx == 0, gx == sizes[0] - 1
    first_y, last_y = gy == 0, gy == sizes[1] - 1

    def exists(dx, dy):
        return (gx + dx >= 0) & (gx + dx < sizes[0]) & (gy + dy >= 0) & (gy + dy < sizes[1])

    def around(a, b, c):
        return tuple(
            lax.rem(here + step, size) if step else here
            for here, step, size in zip(place, (a, b, c), sizes)
        )

    slab = [(0, b, c) for b in range(sizes[1]) for c in range(sizes[2])]
    line = [(a, 0, 0) for a in range(sizes[0])]
    everyone = [(a, b, c) for a, _, _ in line for _, b, c in slab]
    corners = [(dx, dy) for dx in (1, -1) for dy in (1, -1)]

    def flip(slot, turned):
        return slot + turned * (nz - 1 - 2 * slot)

    get_layers = pltpu.make_async_copy(layers_in, layers_own, loads.at[0])
    get_mask = pltpu.make_async_copy(mask_in, labels, loads.at[1])
    get_mask.start()
    get_layers.start()
    barrier = pltpu.get_barrier_semaphore()

    def greet(target):
        pl.semaphore_signal(
            barrier, inc=1, device_id=target, device_id_type=pl.DeviceIdType.MESH
        )

    expected = len(slab) - 1
    for dx, dy in corners + [(1, 0), (-1, 0)]:
        pl.when(exists(dx, dy))(lambda: greet((gx + dx, gy + dy, side)))
        expected = expected + jnp.where(exists(dx, dy), 1, 0)
    for step in slab[1:]:
        greet(around(*step))

    whole = []
    for index, ref in ((1, potential_in), (2, source_in)):
        for plane in range(nz):
            pltpu.make_async_copy(
                ref.at[plane], fields.at[index, flip(plane, side), own], loads.at[1 + index]
            ).start()
        whole.append(pltpu.make_async_copy(ref, fields.at[index, 0:nz, own], loads.at[1 + index]))

    def clear(when, ref, index):
        @pl.when(when)
        def _():
            ref[index] = jnp.zeros(ref.at[index].shape, jnp.float32)

    every = slice(None)
    clear(first_x, fields, (every, slice(0, nz), slice(0, 8)))
    clear(last_x, fields, (every, slice(0, nz), slice(8 + nx, held)))
    for index in range(2):
        clear(first_x, edge_recv, (0, index, 0))
        clear(last_x, edge_recv, (0, index, 1))
    for ref, edge in ((from_after, last_y), (from_before, first_y)):
        clear(edge, ref, (every,))
        clear(first_x, ref, (every, slice(0, 16)))
        clear(last_x, ref, (every, slice(16 + nx, deep)))
    def lanes_of(rows):
        lane = lax.broadcasted_iota(jnp.int32, (rows, ny), 1)
        return lane, lane // GROUP, lane % GROUP

    lane = lax.broadcasted_iota(jnp.int32, (1, ny), 1)

    def pick(vector, index):
        return jnp.sum(jnp.where(lane == index, vector, 0.0), axis=1, keepdims=True)

    own_lane, _, _ = lanes_of(nx)
    later = (own_lane + 1) % ny // GROUP
    sooner = (own_lane + ny - 1) % ny // GROUP

    def pack(index):
        values = [fields[index, slot, own] for slot in range(nz)]
        turned = [lane_roll(value, GROUP * slot + 8) for slot, value in enumerate(values)]
        for toward, owner in ((0, later), (1, sooner)):
            total = turned[0]
            for slot in range(1, nz):
                total = jnp.where(owner == slot, turned[slot], total)
            packs[index, toward] = total
        if index < 2:
            for slot in range(nz):
                edge_send[index, 0, slot : slot + 1] = values[slot][8:9]
                edge_send[index, 1, slot : slot + 1] = values[slot][nx - 9 : nx - 8]

    def spread(number, row, gathered, targets):
        for index, step in enumerate(targets):
            if index:
                pltpu.make_async_remote_copy(
                    src_ref=row, dst_ref=gathered.at[index], send_sem=sum_send.at[number],
                    recv_sem=sum_recv.at[number], device_id=around(*step),
                    device_id_type=pl.DeviceIdType.MESH,
                ).start()

    def collect(number, row, gathered, targets):
        arrived = gathered.at[pl.ds(1, len(targets) - 1)]
        pltpu.make_async_copy(arrived, arrived, sum_recv.at[number]).wait()
        pltpu.make_async_copy(arrived, arrived, sum_send.at[number]).wait()
        gathered[0] = row[...]
        return jnp.sum(gathered[...], axis=0)

    def link(number, src, dst, target):
        return pltpu.make_async_remote_copy(
            src_ref=src, dst_ref=dst, send_sem=halo_send.at[number],
            recv_sem=halo_recv.at[number], device_id=target,
            device_id_type=pl.DeviceIdType.MESH,
        )

    other = (gx, gy, 1 - side)
    numbers = iter(range(64))

    def swap(src, dst):
        copy = link(next(numbers), src, dst, other)
        copy.start()
        return copy

    def exchange(picked, rows, edge):
        found = []

        def move(dx, dy, src, dst):
            copy = link(next(numbers), src, dst, (gx + dx, gy + dy, side))
            pl.when(exists(dx, dy))(copy.start)
            found.append((exists(-dx, -dy), exists(dx, dy), copy))

        for dx, dy in corners:
            into, toward = (from_before, 0) if dy == 1 else (from_after, 1)
            if dx == 1:
                move(dx, dy, packs.at[rows, toward, nx - 16 : nx], into.at[rows, 0:16])
            else:
                move(dx, dy, packs.at[rows, toward, 0:16], into.at[rows, 16 + nx : deep])
        move(0, 1, packs.at[rows, 0], from_before.at[rows, 16 : 16 + nx])
        move(0, -1, packs.at[rows, 1], from_after.at[rows, 16 : 16 + nx])
        move(1, 0, edge_send.at[edge, 1], edge_recv.at[0, edge, 0])
        move(-1, 0, edge_send.at[edge, 0], edge_recv.at[0, edge, 1])
        move(1, 0, fields.at[rows, 0:nz, nx : nx + 8], fields.at[rows, 0:nz, 0:8])
        move(-1, 0, fields.at[rows, 0:nz, 8:16], fields.at[rows, 0:nz, 8 + nx : held])
        return found

    groups = [(slice(0, 2), slice(0, 1), 0), (slice(2, 5), slice(1, 3), 1)]
    moves, relays = [], []

    def launch(picked, rows, edge):
        moves.append(exchange(picked, rows, edge))
        relays.append([swap(fields.at[rows, 0:nz, own], fields.at[rows, nz:planes, own])])

    def relay(picked, rows, edge):
        for receives, _, copy in moves[edge]:
            pl.when(receives)(copy.wait_recv)
        for index in range(rows.start, rows.stop):
            below, above = from_before[index], from_after[index]
            strips[2 * index, 0] = jnp.where(inner_deep < 8, below, above)
            if index < 2:
                strips[2 * index + 1, 0] = jnp.where(
                    inner_deep == 15, lane_roll(above, -1), lane_roll(below, 1)
                )
        relays[edge] += [
            swap(strips.at[picked, 0], strips.at[picked, 1]),
            swap(edge_recv.at[0, edge], edge_recv.at[1, edge]),
            swap(fields.at[rows, 0:nz, 0:8], fields.at[rows, nz:planes, 0:8]),
            swap(fields.at[rows, 0:nz, 8 + nx : held], fields.at[rows, nz:planes, 8 + nx : held]),
        ]

    get_mask.wait()
    get_layers.wait()
    for plane in range(nz):
        fields[0, flip(plane, side), own] = labels[plane].astype(jnp.float32)
    pack(0)
    pl.semaphore_wait(barrier, expected)
    layer_swap = swap(layers_own, layers_far)
    launch(*groups[0])
    for copy in whole:
        copy.wait()
    cells = jnp.zeros((8, ny), jnp.float32)
    injected = cells
    for slot in range(nz):
        for row in range(8, 8 + nx, 8):
            inside = jnp.where(fields[0, slot, row : row + 8] > 0.0, 1.0, 0.0)
            cells = cells + inside
            injected = injected + inside * fields[2, slot, row : row + 8]
    cells = jnp.sum(jnp.sum(cells, axis=0, keepdims=True), axis=1, keepdims=True)
    injected = jnp.sum(jnp.sum(injected, axis=0, keepdims=True), axis=1, keepdims=True)
    early_row[...] = jnp.where(lane == 0, cells, jnp.where(lane == 1, injected, 0.0))

    spread(0, early_row, early_all, slab)
    pack(1)
    pack(2)

    for layer in range(LAYERS):
        for column in range(18):
            table[layer, column] = jnp.float32(HALF_TABLE[layer, column])

    layer_swap.wait()
    for slot in range(nz):
        layers[slot] = layers_own[flip(slot, side)]
        layers[nz + slot] = layers_far[flip(slot, 1 - side)]

    def slot_of(j):
        return jnp.where(j < nz, j, 3 * nz - 1 - j)

    def coefficients(pair, carry):
        for slot in (2 * pair, 2 * pair + 1):
            j = slot_of(slot)
            layer = layers[slot]
            for n, k in enumerate(LEVEL):
                coefs[slot, 2 * n] = table[layer, k]
                coefs[slot, 2 * n + 1] = 2.0 * table[layer, 9 + k]
            near = j + 1 < planes
            there = layers[slot_of(jnp.where(near, j + 1, j))]
            open_ = jnp.where(near, 1.0, 0.0).astype(jnp.float32)
            coefs[slot, UPWARD] = 0.5 * bath_sigma * open_
            for n, (dx, dy) in enumerate(STEEP):
                k = column_of(1, dx, dy, side)
                coefs[slot, UPWARD + 1 + 3 * n] = table[layer, k] * open_
                coefs[slot, UPWARD + 2 + 3 * n] = table[there, k] * open_
                coefs[slot, UPWARD + 3 + 3 * n] = (table[layer, 9 + k] + table[there, 9 + k]) * open_
        return carry

    launch(*groups[1])
    lax.fori_loop(0, nz, coefficients, 0)
    for n in range(COEFS):
        coefs[planes, n] = jnp.float32(0.0)
    _, group8, _ = lanes_of(8)

    def at(j):
        return j if j < nz else 3 * nz - 1 - j

    def widen(block, carry):
        for n in [8 * block + m for m in range(8)]:
            for q in range(2):
                for which, shift in enumerate((0, -1)):
                    value = None
                    for g in range(nz):
                        j = at(q * nz + g) + shift
                        entry = coefs[planes if j < 0 else at(j), n]
                        if value is None:
                            value = jnp.full((8, ny), entry, jnp.float32)
                        else:
                            value = jnp.where(group8 == g, entry, value)
                    coef_lanes[which, q, n] = value
        return carry

    lax.fori_loop(0, COEFS // 8, widen, 0)

    lane_of, group_of, inner_deep = lanes_of(deep)
    relay(*groups[0])
    for dx in (1, -1):
        @pl.when(exists(dx, 0))
        def _():
            pl.semaphore_signal(
                reached, inc=1, device_id=(gx + dx, gy, side), device_id_type=pl.DeviceIdType.MESH
            )
    def ring_of(strip, g):
        return lane_roll(strip, -(GROUP * g + 8))

    def sides(value, ring):
        after = lane_roll(jnp.where(lane_of == 0, ring, value), -1)
        before = lane_roll(jnp.where(lane_of == ny - 1, ring, value), 1)
        return after, before

    def stored(index, number, slot, value):
        if index:
            derived[3 * number + 2, slot] = value
        else:
            derived[3 * number, slot] = jnp.where(value == 2.0, 1.0, 0.0)
            derived[3 * number + 1, slot] = jnp.where(value > 0.0, 1.0, 0.0)

    def framed_plane(index, q, g):
        before = jnp.broadcast_to(edge_recv[q, index, 0, pl.ds(g, 1)], (8, ny))
        after = jnp.broadcast_to(edge_recv[q, index, 1, pl.ds(g, 1)], (8, ny))
        return jnp.concatenate([before, fields[index, q * nz + g], after], axis=0)

    def derive_plane(index, q, g, mixed, ring):
        value = framed_plane(index, q, g)
        for number, part in enumerate((value,) + sides(value, ring)):
            stored(index, number, q * nz + g, part)
        return jnp.where(group_of == g, lane_roll(value, GROUP * g + 8), mixed)

    def derive_strip(index, q, mixed):
        strip, edge = strips[2 * index, q], strips[2 * index + 1, q]
        after = lane_roll(jnp.where(inner_deep == 8, mixed, strip), -1)
        before = lane_roll(jnp.where(inner_deep == 7, mixed, strip), 1)
        stored(index, 0, planes + q, strip)
        stored(index, 1, planes + q, jnp.where(inner_deep == 15, edge, after))
        stored(index, 2, planes + q, jnp.where(inner_deep == 0, edge, before))

    def derive_beside(index):
        for number in ((2, 5, 8) if index else (0, 1, 3, 4, 6, 7)):
            found = across(derived[number, planes], derived[number, planes + 1])
            for shift, value in enumerate(found):
                derived[number, planes + 2 + shift] = value

    def across(lower, upper):
        up0 = jnp.where(group_of == nz - 1, upper, lane_roll(lower, -GROUP))
        up1 = lane_roll(upper, GROUP)
        down0 = lane_roll(lower, GROUP)
        down1 = jnp.where(group_of == nz - 1, lower, lane_roll(upper, -GROUP))
        return up0, up1, down0, down1

    def level_of(coef):
        return {k: (coef(1, 2 * n), coef(1, 2 * n + 1)) for n, k in enumerate(LEVEL)}

    def steep_of(coef, dz):
        entries = {}
        for n, (dx, dy) in enumerate(STEEP):
            here, there, intra = (coef(dz, UPWARD + 1 + 3 * n + m) for m in range(3))
            if dz == 1:
                entries[(dx, dy)] = here, there, intra
            else:
                entries[(-dx, -dy)] = there, here, intra
        return coef(dz, UPWARD), entries

    middle = slice(8, 8 + held)

    def by(value, factor):
        if isinstance(factor, float) or factor.ndim == 0:
            return value * factor
        return value * tiled(factor, value.shape[0])

    def gathered_terms(edges, full):
        sums = edges(tuple(value[middle] for value in full), middle, 0, TERMS_SAME, 0)
        high = tuple(row_roll(value, 1)[8:deep] for value in full)
        part = edges(high, slice(8, deep), 1, TERMS_SIDE, 8)
        sums = sums + row_roll(part, -1)[0:held]
        low = tuple(row_roll(value, -1)[0 : 8 + held] for value in full)
        part = edges(low, slice(0, 8 + held), -1, TERMS_SIDE, 13)
        return sums + row_roll(part, 1)[middle]

    def weigh(slot, above, below, coef):
        level, slopes = level_of(coef), {1: steep_of(coef, 1), -1: steep_of(coef, -1)}
        base_bath = 0.5 * bath_sigma
        neighbour = {0: slot, 1: above, -1: below}

        def fetch(dz, dy, rows):
            number = {0: 0, 1: 1, -1: 2}[dy]
            return tuple(derived[3 * number + m, neighbour[dz], rows] for m in range(2))

        def edges(centre, rows, dx, terms, first):
            t, i = centre
            total = None
            keep = {0: slice(0, held), 1: slice(0, held), -1: slice(8, 8 + held)}[dx]
            for number, (dz, dy) in enumerate(terms):
                tn, i_n = fetch(dz, dy, rows)
                if dz == 0:
                    g_here = g_there = level[SLOT[(0, dx, dy)][0]][0]
                    bath = base_bath
                else:
                    bath, entries = slopes[dz]
                    g_here, g_there, _ = entries[(dx, dy)]
                if (dz != 0) + (dx != 0) + (dy != 0) == 1:
                    ours = by(t, g_here - bath) + by(i, bath)
                    theirs = by(tn, g_there - bath) + by(i_n, bath)
                else:
                    ours, theirs = by(t, g_here), by(tn, g_there)
                weight = i_n * ours + i * theirs
                weights[first + number, slot] = weight[keep]
                total = weight if total is None else total + weight
            return total

        full = fetch(0, 0, slice(0, deep))
        total = gathered_terms(edges, full)
        inside = full[1][middle]
        bounded = jnp.maximum(total, 1.0)
        jacobi = inside / bounded
        jac[slot] = jacobi + jacobi
        spare[slot] = 2.0 * (inside - inside * (jacobi * total))
        return (inside * bounded)[own]

    def begin(slot, above, below, coef, source):
        level, slopes = level_of(coef), {1: steep_of(coef, 1), -1: steep_of(coef, -1)}
        neighbour = {0: slot, 1: above, -1: below}

        def edges(centre, rows, dx, terms, first):
            v = centre[0]
            image = None
            for dz, dy in terms:
                number = {0: 0, 1: 1, -1: 2}[dy]
                tn = derived[3 * number, neighbour[dz], rows]
                vn = derived[3 * number + 2, neighbour[dz], rows]
                if dz == 0:
                    intra = level[SLOT[(0, dx, dy)][0]][1]
                else:
                    intra = slopes[dz][1][(dx, dy)][2]
                term = by(tn * (v - vn), intra)
                image = term if image is None else image + term
            return image

        image = gathered_terms(edges, (derived[2, slot],))
        tissue, inside = derived[0, slot, middle], derived[1, slot, middle]
        basis[0, slot] = 0.5 * jac[slot] * (inside * source - tissue * image)

    def beyond(slot):
        j = slot_of(slot)
        return slot_of(jnp.minimum(j + 1, planes - 1)), slot_of(jnp.maximum(j - 1, 0))

    def from_table(slot):
        j = slot_of(slot)
        under = jnp.where(j == 0, planes, slot_of(j - 1))
        return lambda dz, n: coefs[slot if dz == 1 else under, n]

    def from_lanes(q):
        return lambda dz, n: coef_lanes[0 if dz == 1 else 1, q, n]

    def plane_weigh(slot, carry):
        scale[slot] = weigh(slot, *beyond(slot), from_table(slot))
        return carry

    def strip_weigh(q, carry):
        slot = planes + q
        weigh(slot, slot + 2, slot + 4, from_lanes(q))
        return carry

    def label_half(q, carry):
        @pl.when(q == 1)
        def _():
            for copy in relays[0]:
                copy.wait_recv()
            line_row[...] = collect(0, early_row, early_all, slab)
            sides_x = jnp.where(exists(1, 0), 1, 0) + jnp.where(exists(-1, 0), 1, 0)
            pl.semaphore_wait(reached, sides_x)
            spread(1, line_row, line_all, line)

        mixed = strips[0, q]
        for g in range(nz):
            mixed = derive_plane(0, q, g, mixed, ring_of(strips[0, q], g))
        derive_strip(0, q, mixed)
        lax.fori_loop(q * (nz - 1), nz - 1 + q, plane_weigh, 0)
        return carry

    lax.fori_loop(0, 2, label_half, 0)
    relay(*groups[1])
    def derive_pair(q, pair, mixed):
        for g in (2 * pair, 2 * pair + 1):
            mixed = derive_plane(1, q, g, mixed, ring_of(strips[2, q], g))
        return mixed

    def far_weigh(pair, mixed):
        for m in range(2):
            plane_weigh(nz + 2 * pair + m, 0)
        return derive_pair(0, pair, mixed)

    mixed = lax.fori_loop(0, nz // 2, far_weigh, strips[2, 0])
    derive_strip(1, 0, mixed)
    derive_beside(0)
    lax.fori_loop(0, 2, strip_weigh, 0)
    for copy in relays[1]:
        copy.wait_recv()

    def plane_begin(slot, carry):
        begin(slot, *beyond(slot), from_table(slot), fields[2, slot])
        return carry

    def own_begin(pair, mixed):
        plane_begin(2 * pair, 0)
        plane_begin(jnp.minimum(2 * pair + 1, nz - 2), 0)
        return derive_pair(1, pair, mixed)

    def strip_begin(q, carry):
        slot = planes + q
        begin(slot, slot + 2, slot + 4, from_lanes(q), strips[4, q, middle])
        return carry

    mixed = lax.fori_loop(0, nz // 2, own_begin, strips[2, 1])
    derive_strip(1, 1, mixed)
    derive_beside(1)
    def three_begin(block, carry):
        for m in range(3):
            plane_begin(nz - 1 + 3 * block + m, 0)
        return carry

    lax.fori_loop(0, (nz + 1) // 3, three_begin, 0)
    lax.fori_loop(0, 2, strip_begin, 0)

    def folded(value):
        total = value[0:8]
        for row in range(8, value.shape[0], 8):
            total = total + value[row : row + 8]
        return total

    zero8 = jnp.zeros((8, ny), jnp.float32)

    def record(step, sums):
        for kind, value in enumerate(sums):
            dots[kind * (ITERS + 1) + step] = value

    totals = collect(1, line_row, line_all, line)
    count = pick(totals, 0)
    mean_rhs = pick(totals, 1) / count

    half_mean = 0.5 * mean_rhs
    sums = [zero8, zero8, zero8]
    for slot in range(planes + 2):
        value = basis[0, slot] - half_mean * jac[slot]
        basis[0, slot] = value
        if slot < nz:
            value = value[own]
            sums[0] = sums[0] + folded(value * value * scale[slot])
            sums[2] = sums[2] + folded(value)
    record(0, sums)

    lane_of, group_of, inner_held = lanes_of(held)

    tiles = held // 8

    def advance(step, slot, near, rows, first):
        kept = range(rows.start // 8, rows.stop // 8)
        same, plus, minus = [None] * tiles, [None] * tiles, [None] * tiles
        for t in range(max(kept.start - 1, 0), min(kept.stop + 1, tiles)):
            spot = slice(8 * t, 8 * t + 8)
            values = {}
            for key in TERMS_SIDE + TERMS_SAME:
                ref = near(*key)
                if ref is not None:
                    values[key] = ref[spot]
            for found, terms, begin_at, wanted in (
                (same, TERMS_SAME, 0, t in kept),
                (plus, TERMS_SIDE, 8, t >= kept.start),
                (minus, TERMS_SIDE, 13, t < kept.stop),
            ):
                for number, key in enumerate(terms):
                    if wanted and key in values:
                        term = weights[begin_at + number, slot, spot] * values[key]
                        found[t] = term if found[t] is None else found[t] + term

        def shifted_rows(found, step_by):
            filler = next(value for value in found if value is not None)
            whole = jnp.concatenate([filler if value is None else value for value in found], axis=0)
            return row_roll(whole, step_by)[rows]

        total = jnp.concatenate([same[t] for t in kept], axis=0)
        total = total + shifted_rows(plus, -1) + shifted_rows(minus, 1)
        value = basis[step - 1, slot, rows]
        fresh = jac[slot, rows] * total + spare[slot, rows] * value
        if first:
            factor = jnp.where(step == 1, 0.5, 1.0).astype(jnp.float32)
            back = jnp.where(step == 1, 0.0, 1.0).astype(jnp.float32)
            fresh = factor * fresh - back * basis[jnp.maximum(step - 2, 0), slot, rows]
        else:
            fresh = fresh - basis[step - 2, slot, rows]
        basis[step, slot, rows] = fresh
        return fresh, value

    LEAD = 3

    def roll_plane(field, j, ring):
        slot = at(j)
        moved[0, slot], moved[1, slot] = sides(field[slot], ring)

    def ring_plane(field, j):
        slot = at(j)
        return ring_of(field[planes + slot // nz], slot % nz)

    def one_step(step, last, first=False, final=False):
        now = basis.at[step - 1]
        entering = min(last + 1, planes)
        rings = {}

        def turn(j):
            if LEAD <= j < entering:
                rings[j] = ring_plane(now, j)

        def roll(j):
            if LEAD <= j < entering:
                roll_plane(now, j, rings.pop(j))

        mixed, triples = {}, {}

        def insert(q):
            total = now[planes + q]
            for g in range(nz):
                slot = q * nz + g
                j = slot if q == 0 else 3 * nz - 1 - slot
                if j <= last:
                    total = jnp.where(group_of == g, lane_roll(now[slot], GROUP * g + 8), total)
            mixed[q] = total

        def shift_strip(q):
            strip = now[planes + q]
            after = lane_roll(jnp.where(inner_held == 8, mixed[q], strip), -1)
            before = lane_roll(jnp.where(inner_held == 7, mixed[q], strip), 1)
            moved[0, planes + q], moved[1, planes + q] = after, before

        def cross(number):
            if number:
                found = across(moved[number - 1, planes], moved[number - 1, planes + 1])
            else:
                found = across(now[planes], now[planes + 1])
            for which, value in enumerate(found):
                beside[which, number] = value

        def advance_strip(q):
            slot = planes + q

            def near(dz, dy):
                number = {0: 0, 1: 1, -1: 2}[dy]
                if dz:
                    return beside.at[q if dz == 1 else 2 + q, number]
                return now.at[slot] if dy == 0 else moved.at[number - 1, slot]

            advance(step, slot, near, slice(0, held), first)

        coming = basis.at[step]
        plan = {
            0: [lambda: insert(0)],
            1: [lambda: shift_strip(0), lambda: insert(1)],
            2: [lambda: shift_strip(1), lambda: cross(0)],
            3: [lambda: cross(1)],
            4: [lambda: cross(2)],
            6: [lambda: advance_strip(0), lambda: advance_strip(1)],
            8: [lambda: rings.update({-1 - j: ring_plane(coming, j) for j in (0, 1)})],
            9: [
                lambda: roll_plane(coming, 0, rings[-1]),
                lambda: roll_plane(coming, 1, rings[-2]),
                lambda: rings.update({-3: ring_plane(coming, 2)}),
            ],
            10: [lambda: roll_plane(coming, 2, rings[-3])],
        }
        sums = [zero8, zero8, zero8]
        turn(LEAD)
        for j in range(last):
            turn(j + LEAD + 1)
            roll(j + LEAD)
            slot = at(j)

            def near(dz, dy):
                if j + dz < 0:
                    return None
                spot = at(j + dz)
                return now.at[spot] if dy == 0 else moved.at[0 if dy == 1 else 1, spot]

            rows = own if final else slice(0, held)
            fresh, value = advance(step, slot, near, rows, first)
            if j < nz:
                if not final:
                    fresh, value = fresh[own], value[own]
                weighted = fresh * scale[slot]
                sums[0] = sums[0] + folded(weighted * fresh)
                sums[1] = sums[1] + folded(weighted * value)
                sums[2] = sums[2] + folded(fresh)
            if not final:
                for work in plan.get(j, []):
                    work()
        record(step, sums)

    def early_steps(step, carry):
        one_step(step, planes - 1, first=True)
        return carry

    def later_steps(step, carry):
        one_step(step, planes - 4)
        return carry

    for j in range(LEAD):
        roll_plane(basis.at[0], j, ring_plane(basis.at[0], j))
    lax.fori_loop(1, 4, early_steps, 0)
    lax.fori_loop(4, ITERS, later_steps, 0)
    one_step(ITERS, nz, final=True)
    partial = jnp.sum(jnp.sum(dots[...], axis=1), axis=1, keepdims=True)
    entry = lax.broadcasted_iota(jnp.int32, (3 * (ITERS + 1), ny), 0)
    kind, index = entry // (ITERS + 1), entry % (ITERS + 1)
    place_of = jnp.where(kind == 0, 2 * index, jnp.where(kind == 1, 2 * index - 1, 2 * ITERS + 1 + index))
    wanted = place_of == lax.broadcasted_iota(jnp.int32, entry.shape, 1)
    final_row[...] = jnp.sum(jnp.where(wanted, partial, 0.0), axis=0, keepdims=True)
    spread(2, final_row, final_all, everyone)
    for group in moves:
        for _, sends, copy in group:
            pl.when(sends)(copy.wait_send)
    for group in relays:
        for copy in group:
            copy.wait_send()
    sums = collect(2, final_row, final_all, everyone)

    mu = [pick(sums, n) for n in range(2 * ITERS)]
    ones = [pick(sums, 2 * ITERS + 1 + n) for n in range(ITERS)]
    for n in range(2, 2 * ITERS):
        mu[n] = 2.0 * mu[n] - mu[n % 2]
    one = jnp.ones((1, 1), jnp.float32)
    y, p = [one], [one]
    m_y, m_p = list(mu), list(mu)
    x = []
    rz = mu[0]

    def plus(first, second):
        if first is None or second is None:
            return second if first is None else first
        return first + second

    def get(values, n):
        return values[n] if 0 <= n < len(values) else None

    for step in range(ITERS):
        h_p = []
        for n in range(step + 2):
            right = get(p, n - 1)
            if n == 1:
                right = right + right
            around_n = plus(get(p, n + 1), right)
            here = get(p, n)
            drop = None if around_n is None else -0.5 * around_n
            h_p.append(plus(here, drop))
        m_h = [m_p[0] - m_p[1]]
        for n in range(1, 2 * ITERS - 1 - step):
            m_h.append(m_p[n] - 0.5 * (m_p[n + 1] + m_p[n - 1]))
        bottom = p[0] * m_h[0]
        for n in range(1, step + 1):
            bottom = bottom + p[n] * m_h[n]
        alpha = rz / bottom
        x = [plus(get(x, n), alpha * p[n]) for n in range(step + 1)]
        y = [plus(get(y, n), -(alpha * h_p[n])) for n in range(step + 2)]
        if step + 1 < ITERS:
            m_y = [m_y[n] - alpha * m_h[n] for n in range(len(m_h))]
            rz_next = y[0] * m_y[0]
            for n in range(1, step + 2):
                rz_next = rz_next + y[n] * m_y[n]
            beta = rz_next / rz
            p = [plus(y[n], None if n > step else beta * p[n]) for n in range(step + 2)]
            m_p = [m_y[n] + beta * m_p[n] for n in range(len(m_y))]
            rz = rz_next
    mean = x[0] * ones[0]
    for n in range(1, ITERS):
        mean = mean + x[n] * ones[n]
    mean = mean / count
    xs = [jnp.broadcast_to(value, (8, ny)) for value in x]
    ys = [jnp.broadcast_to(value, (8, ny)) for value in y]
    mean = jnp.broadcast_to(mean, (8, ny))
    for slot in range(nz):
        target = flip(slot, side)
        for row in range(0, nx, 8):
            spot = slice(8 + row, 16 + row)
            weight = scale[slot, row : row + 8]
            total = jnp.where(weight > 0.0, -mean, 0.0)
            rest = ys[ITERS] * basis[ITERS, slot, spot]
            for n in range(ITERS):
                value = basis[n, slot, spot]
                total = total + xs[n] * value
                rest = rest + ys[n] * value
            phi[target, row : row + 8] = total
            residual[target, row : row + 8] = weight * rest


def hand_out(phi, residual, phi_out, residual_out, sems):
    copies = [
        pltpu.make_async_copy(phi, phi_out, sems.at[0]),
        pltpu.make_async_copy(residual, residual_out, sems.at[1]),
    ]
    for copy in copies:
        copy.start()
    for copy in copies:
        copy.wait()


def fast_body(potential, tissue_mask, layer_index, source):
    extent = tissue_mask.shape
    nz, nx, ny = extent
    sizes = tuple(lax.axis_size(axis) for axis in AXES)
    planes, held, deep = 2 * nz, nx + 16, nx + 32
    peers = math.prod(sizes)
    vmem = pl.BlockSpec(memory_space=pltpu.VMEM)
    hbm = pl.BlockSpec(memory_space=pltpu.HBM)

    def real(*shape):
        return pltpu.VMEM(shape + (ny,), jnp.float32)

    moves = 40
    inputs = (potential, tissue_mask, layer_index, source)
    scratch = [
        real(3, planes, held), pltpu.VMEM(extent, jnp.int32), real(3, 2, nx), real(2, 2, nz),
        real(2, 2, 2, nz), real(3, deep), real(3, deep), real(5, 2, deep),
        real(9, planes + 6, deep), real(18, planes + 2, held), real(ITERS + 1, planes + 2, held),
        real(2, planes + 2, held), real(4, 3, held), real(planes + 2, held),
        real(planes + 2, held), real(planes, nx), real(2, 2, COEFS, 8), real(3 * (ITERS + 1), 8),
        real(1), real(sizes[1] * sizes[2], 1), real(1), real(sizes[0], 1), real(1), real(peers, 1),
        pltpu.SMEM((LAYERS, 18), jnp.float32), pltpu.SMEM((planes + 1, COEFS), jnp.float32),
        pltpu.SMEM((nz,), jnp.int32), pltpu.SMEM((nz,), jnp.int32), pltpu.SMEM((planes,), jnp.int32),
        pltpu.SemaphoreType.DMA((4,)), pltpu.SemaphoreType.DMA((moves,)),
        pltpu.SemaphoreType.DMA((moves,)), pltpu.SemaphoreType.DMA((3,)),
        pltpu.SemaphoreType.DMA((3,)), pltpu.SemaphoreType.REGULAR,
    ]
    shapes = (jax.ShapeDtypeStruct(extent, jnp.float32),) * 2
    found = pl.pallas_call(
        functools.partial(fast_kernel, extent, sizes),
        out_shape=shapes,
        in_specs=[hbm] * 4,
        out_specs=(vmem, vmem),
        scratch_shapes=scratch,
        compiler_params=pltpu.CompilerParams(
            vmem_limit_bytes=32 * 1024 * 1024, collective_id=0, has_side_effects=True
        ),
    )(*(pltpu.with_memory_space_constraint(ref, pltpu.HBM) for ref in inputs))
    return tuple(
        pl.pallas_call(
            hand_out,
            out_shape=shapes,
            in_specs=[vmem] * 2,
            out_specs=(hbm, hbm),
            scratch_shapes=[pltpu.SemaphoreType.DMA((2,))],
            compiler_params=pltpu.CompilerParams(vmem_limit_bytes=4 * 1024 * 1024),
        )(*found)
    )


def body(potential, tissue_mask, layer_index, source):
    nz, nx, ny = tissue_mask.shape
    fits = (
        lax.axis_size("gz") == 2 and nz == 8 and ITERS == 8 and nx % 8 == 0 and nx >= 16
        and ny == nz * GROUP and 1 < lax.axis_size("gx") <= 4 and lax.axis_size("gy") > 1
    )
    return (fast_body if fits else general_body)(potential, tissue_mask, layer_index, source)


def solution(mesh):
    placed = (P("gz", "gx", "gy"), P("gz", "gx", "gy"), P("gz"), P("gz", "gx", "gy"))
    return jax.shard_map(
        body,
        mesh=mesh,
        in_specs=placed,
        out_specs=(P("gz", "gx", "gy"), P("gz", "gx", "gy")),
        check_vma=False,
    )
```
